32 devices in a mesh: task: 16 (over z, x, core), tensor: 2 (over y).
Axes of the slice: x: 2, y: 2, z: 4, core: 2. Of those that a mesh axis runs over, the one named last changes fastest.
Arguments:
- inputs: bfloat16 [2048, 4096], P('task', 'tensor'), may hold values from -6 to 6
- targets: bfloat16 [2048, 4096], P('task', 'tensor'), may hold values from -6 to 6
- queries: bfloat16 [2048, 2048], P('task', 'tensor'), may hold values from -120 to 120
- key_rows: bfloat16 [2048, 2048], P('task', 'tensor'), may hold values from -4 to 4
- value_weight: bfloat16 [4096, 2048], P(None, 'tensor'), may hold values from -0.09375 to 0.09375
- output_weight: bfloat16 [2048, 4096], P('tensor'), may hold values from -0.125 to 0.125
- splits: int32 [16], P('task'), may hold values from 32 to 96
Outputs:
- meta_value: float32 [4096, 2048], P('task', 'tensor')
- meta_output: float32 [2048, 4096], P('tensor', 'task')
The draws below stay inside these ranges and needn't reach their ends.
Inputs may be any that keep to these rules, and one draw needn't show every extreme that they name: `splits`: support and query parts of every task are both nonempty.
All inputs are finite; a program needn't handle non-finite values.
Results may differ from the reference program's by a relative error of at most 0.025.
Values may be sent and summed in bfloat16 or wider, within the bound.
A program may use at most 128 MiB of HBM per device.

```python
import jax
import jax.numpy as jnp
from jax import lax

D = 4096
HD = 128
HEADS = 16
INNER = 1
TASKS_DEV = 1
TASK_LEN = 128
TOKENS = 2048
N_TASK = 16
N_TENSOR = 2


def paired(key):
    first, second = jax.random.split(jax.random.fold_in(key, 7), 2)
    query_base = jnp.clip(jax.random.normal(first, (TOKENS, HEADS * HD), jnp.float32), -4.0, 4.0)
    key_base = jnp.clip(jax.random.normal(second, (TOKENS, HEADS * HD), jnp.float32), -4.0, 4.0)
    return (query_base, key_base)


def draw_queries(key, part):
    return paired(key)[0].astype(jnp.bfloat16)


def draw_key_rows(key, part):
    return paired(key)[1].astype(jnp.bfloat16)


def touch_ends(values, own_key, smallest, high):
    extent = values.shape
    place = [jax.random.randint(jax.random.fold_in(own_key, axis), (), 0, extent[axis]) for axis in range(len(extent))]
    values = values.at[tuple(place)].set(smallest)
    longest = extent.index(max(extent))
    place[longest] = (place[longest] + 1) % extent[longest]
    return values.at[tuple(place)].set(high)


def spiked(drawn, stream_key, source, target, blocks, factor):
    def block_of(dim):
        return (jnp.arange(drawn.shape[dim]) // (drawn.shape[dim] // blocks)).reshape((-1,) + (1,) * (drawn.ndim - 1 - dim))

    one_side = jax.random.permutation(stream_key, blocks)[block_of(target)]
    second = (block_of(target) + blocks // 2) % blocks
    return jnp.where((block_of(source) == one_side) | (block_of(source) == second), factor * drawn, drawn)


def steps_of(own_key, shape, cuts, low, top_value):
    level, own = 1.0, jax.random.fold_in(own_key, 6)
    for dim, blocks in cuts:
        heights = jnp.exp(jax.random.uniform(jax.random.fold_in(own, dim), (blocks,), jnp.float32, low / len(cuts), top_value / len(cuts)))
        level = level * jnp.repeat(heights, shape[dim] // blocks).reshape([-1 if axis == dim else 1 for axis in range(len(shape))])
    return level


def bell_draw(own_key, extent, scale, reach, pieces=(), kind=jnp.bfloat16):
    array = jax.random.normal(own_key, extent, jnp.float32) * scale
    if len(pieces) > 0:
        array = steps_of(own_key, extent, pieces, -0.22, 0.18) * array
    return jnp.clip(array, min=-reach, max=reach).astype(kind)


def gaussian_with(stream_key, shape, scale, most, shards, heavy, held_as=jnp.bfloat16):
    entries = scale * jax.random.normal(stream_key, shape, jnp.float32)
    if shards:
        entries = entries * steps_of(stream_key, shape, shards, -0.22, 0.18)
    return jnp.clip(spiked(entries, jax.random.fold_in(stream_key, 3), *heavy), -most, most).astype(held_as)


def setup_inputs(seed: int = 0) -> dict:
    streams_of = jax.random.split(jax.random.key(seed), 8)
    return {
        "inputs": gaussian_with(streams_of[0], (TOKENS, D), 1.0, 6.0, ((0, 16), (1, 2)), (0, 1, 16, 2.0)),
        "targets": bell_draw(streams_of[1], (TOKENS, D), 1.0, 6.0, ((0, 16), (1, 2))),
        "queries": draw_queries(jax.random.fold_in(streams_of[7], 71), 0),
        "key_rows": draw_key_rows(jax.random.fold_in(streams_of[7], 71), 0),
        "value_weight": bell_draw(streams_of[4], (D, HEADS * HD), D ** -0.5, 0.09375, ((1, 2),)),
        "output_weight": bell_draw(streams_of[5], (HEADS * HD, D), (HEADS * HD) ** -0.5, 0.125, ((0, 2),)),
        "splits": touch_ends(jax.random.randint(streams_of[6], (TASKS_DEV * N_TASK,), TASK_LEN // 4, 3 * TASK_LEN // 4 + 1), jax.random.fold_in(streams_of[6], 1), TASK_LEN // 4, (3 * TASK_LEN // 4 + 1) - 1).astype(jnp.int32),
    }


step_rate = 0.25

def normed_rows(inputs):
    values = inputs.astype(jnp.float32)
    scale = lax.rsqrt(lax.optimization_barrier(jnp.mean(values * values, axis=-1, keepdims=True)) + 1e-05)
    return (values * scale).astype(jnp.bfloat16)

def attention_probs(queries, key_rows, heads):
    length = queries.shape[0]
    query_f = queries.astype(jnp.float32).reshape(length, heads, -1)
    key_f = key_rows.astype(jnp.float32).reshape(length, heads, -1)
    scores = jnp.einsum('ihd,jhd->hij', query_f, key_f) / jnp.sqrt(jnp.float32(query_f.shape[2]))
    position = jnp.arange(length)
    causal = position[:, None] >= position[None, :]
    scores = jnp.where(causal[None], scores, jnp.float32(-1e+30))
    scores = scores - lax.optimization_barrier(jnp.max(scores, axis=-1, keepdims=True))
    expo = jnp.exp(scores)
    return (expo / lax.optimization_barrier(jnp.sum(expo, axis=-1, keepdims=True))).astype(jnp.bfloat16)

def local_out(value_mat, output_mat, normed, probs):
    heads = probs.shape[0]
    length = normed.shape[0]
    upper = jnp.dot(normed, value_mat.astype(jnp.bfloat16), preferred_element_type=jnp.float32).astype(jnp.bfloat16)
    mixed = jnp.einsum('hij,jhd->ihd', probs.astype(jnp.float32), upper.astype(jnp.float32).reshape(length, heads, -1))
    mixed = mixed.reshape(length, -1).astype(jnp.bfloat16)
    return jnp.dot(mixed, output_mat.astype(jnp.bfloat16), preferred_element_type=jnp.float32).astype(jnp.bfloat16)

def task_meta(value_mat, output_mat, inputs, targets, queries, key_rows, split):
    cols = HEADS * HD // N_TENSOR
    group = HEADS // N_TENSOR
    normed = normed_rows(inputs)
    probs = attention_probs(queries, key_rows, HEADS)
    position = jnp.arange(TASK_LEN)
    support = (position < split).astype(jnp.float32)[:, None]
    query_mask = 1.0 - support
    count_s = split.astype(jnp.float32)
    count_q = jnp.float32(TASK_LEN) - count_s
    input_f = inputs.astype(jnp.float32)
    target_f = targets.astype(jnp.float32)

    def total(value_now, output_now):
        result = input_f
        for index in range(N_TENSOR):
            result = result + local_out(value_now[:, index * cols:(index + 1) * cols], output_now[index * cols:(index + 1) * cols], normed, probs[index * group:(index + 1) * group]).astype(jnp.float32)
        return result

    def loss(value_now, output_now, mask, count):
        error = total(value_now, output_now) - target_f
        return 0.5 * jnp.sum(mask * error * error) / count

    def meta_loss(value_now, output_now):
        for inner in range(INNER):
            grad_value, grad_output = jax.grad(loss, argnums=(0, 1))(value_now, output_now, support, count_s)
            value_now = value_now - step_rate * grad_value
            output_now = output_now - step_rate * grad_output
        return loss(value_now, output_now, query_mask, count_q)
    return jax.grad(meta_loss, argnums=(0, 1))(value_mat, output_mat)

def reference(inputs, targets, queries, key_rows, value_weight, output_weight, splits):
    count = N_TASK * TASKS_DEV
    value_f = value_weight.astype(jnp.float32)
    output_f = output_weight.astype(jnp.float32)
    items = (inputs.reshape(count, TASK_LEN, D), targets.reshape(count, TASK_LEN, D), queries.reshape(count, TASK_LEN, HEADS * HD), key_rows.reshape(count, TASK_LEN, HEADS * HD), splits.astype(jnp.int32))

    def accumulate(carry, item):
        grad_value, grad_output = task_meta(value_f, output_f, item[0], item[1], item[2], item[3], item[4])
        return ((carry[0] + grad_value, carry[1] + grad_output), None)
    start = (jnp.zeros((D, HEADS * HD), jnp.float32), jnp.zeros((HEADS * HD, D), jnp.float32))
    result, unused = lax.scan(accumulate, start, items)
    return (result[0], result[1])
```

```python
import functools

import jax
import jax.numpy as jnp
from jax import lax
from jax.experimental import pallas as pl
from jax.experimental.pallas import tpu as pltpu
from jax.sharding import PartitionSpec as P

HD = 128
BF = jnp.bfloat16
F32 = jnp.float32

step_rate = 0.25


def normed_rows(inputs):
    values = inputs.astype(F32)
    scale = lax.rsqrt(jnp.mean(values * values, axis=-1, keepdims=True) + 1e-05)
    return (values * scale).astype(BF)


def attention_probs(queries, key_rows, heads):
    length = queries.shape[0]
    query_h = queries.reshape(length, heads, -1)
    key_h = key_rows.reshape(length, heads, -1)
    scores = jnp.einsum("ihd,jhd->hij", query_h, key_h, preferred_element_type=F32)
    scores = scores / jnp.sqrt(F32(query_h.shape[2]))
    position = jnp.arange(length)
    causal = position[:, None] >= position[None, :]
    scores = jnp.where(causal[None], scores, F32(-1e30))
    scores = scores - jnp.max(scores, axis=-1, keepdims=True)
    expo = jnp.exp(scores)
    return (expo / jnp.sum(expo, axis=-1, keepdims=True)).astype(BF)


def mm(left, right):
    return jnp.dot(left, right, preferred_element_type=F32)


def mm_nt(left, right):
    return lax.dot_general(left, right, (((1,), (1,)), ((), ())), preferred_element_type=F32)


def mm_tn(left, right):
    return lax.dot_general(left, right, (((0,), (0,)), ((), ())), preferred_element_type=F32)


def mix(probs, rows):
    heads = probs.shape[0]
    split = rows.reshape(rows.shape[0], heads, -1)
    out = jnp.einsum("hij,jhd->ihd", probs, split, preferred_element_type=F32)
    return out.reshape(out.shape[0], -1)


def mix_back(probs, rows):
    heads = probs.shape[0]
    split = rows.reshape(rows.shape[0], heads, -1)
    out = jnp.einsum("hij,ihd->jhd", probs, split, preferred_element_type=F32)
    return out.reshape(out.shape[0], -1)


def group_sum(term, count):
    term = term.astype(BF)
    if count == 1:
        return term.astype(F32)
    if count == 2:
        other = lax.ppermute(term, "tensor", ((0, 1), (1, 0)))
        return term.astype(F32) + other.astype(F32)
    share = lax.psum_scatter(term, "tensor", scatter_dimension=1, tiled=True)
    return lax.all_gather(share, "tensor", axis=1, tiled=True).astype(F32)


def full_rows(inputs, count, index):
    if count != 2:
        return lax.all_gather(inputs, "tensor", axis=1, tiled=True)
    other = lax.ppermute(inputs, "tensor", ((0, 1), (1, 0)))
    low = jnp.where(index == 0, inputs, other)
    high = jnp.where(index == 0, other, inputs)
    return jnp.concatenate([low, high], axis=1)


def gather_kernel(lines, src_ref, out_ref, own_sem, send_sem, line_sem, side_sem, core_sem):
    me = lax.axis_index("task")
    core, side, line = lax.rem(me, 2), lax.rem(me // 2, 2), me // 4

    def place(back, over_side, over_core):
        line_from = lax.rem(line + lines - back, lines)
        side_from = 1 - side if over_side else side
        core_from = 1 - core if over_core else core
        return (line_from * 2 + side_from) * 2 + core_from

    side_peer, core_peer = place(0, True, False), place(0, False, True)
    peers = [place(lines - step, False, False) for step in range(1, lines)] + [side_peer, core_peer]
    barrier = pltpu.get_barrier_semaphore()
    for peer in peers:
        pl.semaphore_signal(
            barrier, inc=1, device_id={"task": peer}, device_id_type=pl.DeviceIdType.MESH
        )
    pl.semaphore_wait(barrier, len(peers))

    started = []

    def send(source, slot, arrival, peer):
        copy = pltpu.make_async_remote_copy(
            src_ref=source,
            dst_ref=out_ref.at[slot],
            send_sem=send_sem.at[len(started)],
            recv_sem=arrival,
            device_id={"task": peer},
            device_id_type=pl.DeviceIdType.MESH,
        )
        copy.start()
        started.append(copy)

    def arrived(slot, arrival, peer):
        pltpu.make_async_remote_copy(
            src_ref=out_ref.at[slot],
            dst_ref=out_ref.at[slot],
            send_sem=send_sem.at[0],
            recv_sem=arrival,
            device_id={"task": peer},
            device_id_type=pl.DeviceIdType.MESH,
        ).wait_recv()

    for step in sorted(range(1, lines), key=lambda step: -min(step, lines - step)):
        send(src_ref, me, line_sem.at[step], peers[step - 1])
    send(src_ref, me, side_sem.at[0], side_peer)
    send(src_ref, me, core_sem.at[0, 0], core_peer)
    own = pltpu.make_async_copy(src_ref, out_ref.at[me], own_sem)
    own.start()
    order = sorted(range(1, lines), key=lambda step: min(step, lines - step))
    for step in order:
        slot = place(step, False, False)
        arrived(slot, line_sem.at[step], side_peer)
        send(out_ref.at[slot], slot, side_sem.at[step], side_peer)
        send(out_ref.at[slot], slot, core_sem.at[step, 0], core_peer)
    for step in [0] + order:
        slot = place(step, True, False)
        arrived(slot, side_sem.at[step], side_peer)
        send(out_ref.at[slot], slot, core_sem.at[step, 1], core_peer)
    for step in [0] + order:
        for over in range(2):
            arrived(place(step, over == 1, True), core_sem.at[step, over], core_peer)
    own.wait()
    for copy in started:
        copy.wait_send()


def gather_by_copies(rows, number):
    count = lax.axis_size("task")
    if count % 4:
        return gather_tokens(rows)
    lines = count // 4
    sends = (lines + 1) + 2 * (lines - 1) + lines
    gathered = pl.pallas_call(
        functools.partial(gather_kernel, lines),
        out_shape=jax.ShapeDtypeStruct((count,) + rows.shape, rows.dtype),
        in_specs=[pl.BlockSpec(memory_space=pltpu.VMEM)],
        out_specs=pl.BlockSpec(memory_space=pltpu.VMEM),
        scratch_shapes=[
            pltpu.SemaphoreType.DMA,
            pltpu.SemaphoreType.DMA((sends,)),
            pltpu.SemaphoreType.DMA((lines,)),
            pltpu.SemaphoreType.DMA((lines,)),
            pltpu.SemaphoreType.DMA((lines, 2)),
        ],
        compiler_params=pltpu.CompilerParams(collective_id=number, has_side_effects=True),
        cost_estimate=pl.CostEstimate(
            flops=0, bytes_accessed=16 * rows.size * rows.dtype.itemsize * count, transcendentals=0
        ),
    )(rows)
    return gathered.reshape(count * rows.shape[0], rows.shape[1])


def gather_tokens(rows):
    return lax.all_gather(rows, "task", axis=0, tiled=True)


def my_columns(rows):
    return lax.all_to_all(rows, "task", split_axis=1, concat_axis=0, tiled=True)


def below(rows, length):
    return jnp.pad(rows, ((0, length - rows.shape[0]), (0, 0)))


def above(rows, length):
    return jnp.pad(rows, ((length - rows.shape[0], 0), (0, 0)))


MESH = pl.DeviceIdType.MESH


def dot_of(left, right, dims):
    return lax.dot_general(left, right, (dims, ((), ())), preferred_element_type=F32)


def step_kernel(
    lines,
    x_in, t_in, q_in, k_in, v_in, o_in, split_ref,
    dv_ref, do_ref,
    xf, tg, qs, ks, vw, ow, probs, probs_t, upper, mixq, second, acc, half_acc,
    part_0, part_1, part_2, got_0, got_1, got_2, err_1, err_2, err_3, both,
    back, gram_b, cross, pairs, value_now, z_all, left_all, rows_all, x_cols, both_cols, err_cols,
    load_sem, x_sem, part_sem, part_got,
    a2a_send, a2a_got, g_send, g_line, g_side, g_core,
):
    count = lines * 4
    length, depth = xf.shape
    half = depth // 2
    width = upper.shape[1]
    heads = width // HD
    low, high = length // 4, 3 * length // 4
    piece = depth // count
    chunks = 8
    cut = depth // chunks
    near = chunks // 2

    me = lax.axis_index("task")
    mine = lax.axis_index("tensor")
    core, side, line = lax.rem(me, 2), lax.rem(me // 2, 2), me // 4
    pair = {"tensor": 1 - mine}

    def place(back_by, over_side, over_core):
        line_from = lax.rem(line + lines - back_by, lines)
        side_from = 1 - side if over_side else side
        core_from = 1 - core if over_core else core
        return (line_from * 2 + side_from) * 2 + core_from

    def lanes(start, size):
        return pl.ds(pl.multiple_of(start, 128), size)

    own_half = lanes(mine * half, half)
    loads = [
        pltpu.make_async_copy(x_in, xf.at[:, own_half], load_sem.at[0]),
        pltpu.make_async_copy(q_in, qs, load_sem.at[1]),
        pltpu.make_async_copy(k_in, ks, load_sem.at[2]),
        pltpu.make_async_copy(v_in, vw, load_sem.at[3]),
        pltpu.make_async_copy(t_in, tg, load_sem.at[4]),
        pltpu.make_async_copy(o_in, ow, load_sem.at[5]),
    ]
    for load in loads:
        load.start()

    barrier = pltpu.get_barrier_semaphore()
    for step in range(1, count):
        pl.semaphore_signal(
            barrier, inc=1, device_id={"task": lax.rem(me + step, count)}, device_id_type=MESH
        )
    pl.semaphore_signal(barrier, inc=1, device_id=pair, device_id_type=MESH)
    pl.semaphore_wait(barrier, count)

    def remote(src, dst, send, got, peer):
        return pltpu.make_async_remote_copy(
            src_ref=src, dst_ref=dst, send_sem=send, recv_sem=got, device_id=peer, device_id_type=MESH
        )

    def x_copy(k, owner):
        part = xf.at[:, lanes(owner * half + k * cut, cut)]
        return remote(part, part, x_sem.at[0, k], x_sem.at[1, k], pair)

    loads[0].wait()
    for k in range(near):
        x_copy(k, mine).start()

    def a2a_copy(number, src, dst, step):
        peer = lax.rem(me + step, count)
        return remote(
            src.at[:, lanes(peer * piece, piece)],
            dst.at[me],
            a2a_send.at[number, step],
            a2a_got.at[number, step],
            {"task": peer},
        )

    def a2a_start(number, src, dst):
        def one(step, carry):
            a2a_copy(number, src, dst, step).start()
            return carry
        lax.fori_loop(1, count, one, 0)

    def a2a_wait(number, src, dst):
        def one(step, carry):
            a2a_copy(number, src, dst, step).wait()
            return carry
        lax.fori_loop(1, count, one, 0)

    def x_spread(own):
        def one(step, carry):
            peer = lax.rem(me + step, count)
            here = (peer // (count // 2)) == mine
            @pl.when(here if own else jnp.logical_not(here))
            def _():
                a2a_copy(0, xf, x_cols, step).start()
            return carry
        lax.fori_loop(1, count, one, 0)

    x_spread(True)

    def gather_copy(number, src, dst, peer, index, got):
        return remote(src, dst, g_send.at[number, index], got, {"task": peer})

    def gather_start(number, array):
        src = array.at[me]
        index = 0
        for step in range(1, lines):
            gather_copy(number, src, src, place(lines - step, False, False), index, g_line.at[number, step]).start()
            index += 1
        gather_copy(number, src, src, place(0, True, False), index, g_side.at[number, 0]).start()
        gather_copy(number, src, src, place(0, False, True), index + 1, g_core.at[number, 0, 0]).start()

    def gather_relay_line(number, array):
        index = lines + 1
        for step in range(1, lines):
            slot = array.at[place(step, False, False)]
            gather_copy(number, slot, slot, place(0, True, False), index, g_line.at[number, step]).wait_recv()
            gather_copy(number, slot, slot, place(0, True, False), index, g_side.at[number, step]).start()
            gather_copy(number, slot, slot, place(0, False, True), index + 1, g_core.at[number, step, 0]).start()
            index += 2

    def gather_relay_side(number, array):
        index = lines + 1 + 2 * (lines - 1)
        for step in range(lines):
            slot = array.at[place(step, True, False)]
            gather_copy(number, slot, slot, place(0, False, True), index, g_side.at[number, step]).wait_recv()
            gather_copy(number, slot, slot, place(0, False, True), index, g_core.at[number, step, 1]).start()
            index += 1

    def gather_finish(number, array):
        for step in range(lines):
            for over in range(2):
                slot = array.at[place(step, over == 1, True)]
                gather_copy(number, slot, slot, place(0, False, True), 0, g_core.at[number, step, over]).wait_recv()

    def gather_sent(number, array):
        for index in range(lines + 1 + 2 * (lines - 1) + lines):
            gather_copy(number, array.at[me], array.at[me], place(0, False, True), index, g_core.at[number, 0, 0]).wait_send()

    def head(h):
        return slice(h * HD, (h + 1) * HD)

    row = lax.broadcasted_iota(jnp.int32, (length, length), 0)
    col = lax.broadcasted_iota(jnp.int32, (length, length), 1)
    causal = row >= col
    loads[1].wait()
    loads[2].wait()
    root = jnp.sqrt(F32(HD))
    for h in range(heads):
        scores = dot_of(qs[:, head(h)], ks[:, head(h)], ((1,), (1,))) / root
        scores = jnp.where(causal, scores, F32(-1e30))
        scores = scores - jnp.max(scores, axis=-1, keepdims=True)
        expo = jnp.exp(scores)
        prob = expo / jnp.sum(expo, axis=-1, keepdims=True)
        probs[:, head(h)] = prob.astype(BF)
        probs_t[:, head(h)] = prob.T.astype(BF)

    err_1[high:, :] = jnp.zeros((length - high, depth), BF)
    err_2[:low, :] = jnp.zeros((low, depth), BF)
    err_3[high:, :] = jnp.zeros((length - high, depth), BF)
    position = lax.broadcasted_iota(jnp.int32, (length, 1), 0)
    split = jnp.full((length, 1), split_ref[0], jnp.int32)
    is_support = position < split
    support = is_support.astype(F32)
    count_s = split.astype(F32)
    weight_s = support / count_s
    weight_q = (1.0 - support) / (F32(length) - count_s)

    loads[3].wait()

    def take(k, owner, first):
        at = lanes(owner * half + k * cut, cut)
        x_part = xf[:, at]
        new = dot_of(x_part, vw[pl.ds(pl.multiple_of(owner * half + k * cut, 128), cut), :], ((1,), (0,)))
        gram = dot_of(x_part, x_part, ((1,), (1,)))
        if first:
            acc[...] = new
            half_acc[...] = gram
        else:
            acc[...] += new
            half_acc[...] += gram

    take(0, mine, True)
    def own_take(k, carry):
        take(k, mine, False)
        return carry
    lax.fori_loop(1, near, own_take, 0)
    def other_take(k, carry):
        x_copy(k, 1 - mine).wait_recv()
        take(k, 1 - mine, False)
        return carry
    lax.fori_loop(0, near, other_take, 0)
    x_spread(False)

    gram_raw = half_acc[...]
    diagonal = jnp.where(row == col, gram_raw, F32(0.0))
    scale_row = lax.rsqrt(jnp.sum(diagonal, axis=1, keepdims=True) / F32(depth) + 1e-05)
    scale_col = lax.rsqrt(jnp.sum(diagonal, axis=0, keepdims=True) / F32(depth) + 1e-05)
    gram_b[...] = (gram_raw * scale_row * scale_col).astype(BF)
    upper[...] = (acc[...] * scale_row).astype(BF)

    z_mine = z_all.at[me]
    for h in range(heads):
        mixed = dot_of(probs[:, head(h)], upper[:, head(h)], ((1,), (0,)))
        z_mine[:, head(h)] = mixed[:high].astype(BF)
    loads[4].wait()
    loads[5].wait()

    def part_copy(number, send, got, k, owner):
        at = lanes(lax.rem(owner * near + k, chunks) * cut, cut)
        return remote(send.at[:, at], got.at[:, at], part_sem.at[number, k], part_got.at[number, k], pair)

    def own_columns(k):
        return lanes(lax.rem(mine * near + k, chunks) * cut, cut)

    def other_columns(k):
        return lanes(lax.rem((1 - mine) * near + k, chunks) * cut, cut)

    def offset(k, rows):
        there = lanes(k * cut, cut)
        return xf[rows, own_columns(k)].astype(F32) - tg[rows, there].astype(F32)

    def send_parts(number, value, rows, send, got, with_offset):
        def one(k, near_half):
            at = own_columns(k)
            part = value(at)
            if near_half and with_offset:
                part = part + offset(k, rows)
            send[:, at] = part.astype(BF)
            part_copy(number, send, got, k, mine).start()
        def first(k, carry):
            one(k, True)
            return carry
        def later(k, carry):
            one(k, False)
            return carry
        lax.fori_loop(0, near, first, 0)
        lax.fori_loop(near, chunks, later, 0)

    def take_parts(number, send, got, rows, weight, error, also):
        def one(k, carry):
            at = other_columns(k)
            part_copy(number, send, got, k, 1 - mine).wait_recv()
            total = send[:, at].astype(F32) + got[:, at].astype(F32)
            error[rows, at] = (weight[rows] * total).astype(BF)
            part = error[:, at]
            acc[...] += dot_of(part, ow[:, at], ((1,), (1,)))
            also(at, part)
            return carry
        lax.fori_loop(0, chunks, one, 0)

    support_rows, query_rows = slice(0, high), slice(low, length)
    nothing = lambda at, part: None

    def value_0(at):
        return dot_of(z_mine[...], ow[:, at], ((1,), (0,)))

    acc[...] = jnp.zeros_like(acc)
    send_parts(0, value_0, support_rows, part_0, got_0, True)
    gather_start(0, z_all)
    take_parts(0, part_0, got_0, support_rows, weight_s, err_1, nothing)

    back[...] = acc[...].astype(BF)
    for h in range(heads):
        up = dot_of(probs_t[:, head(h)], back[:, head(h)], ((1,), (0,))).astype(BF)
        new = (upper[:, head(h)].astype(F32) - step_rate * dot_of(gram_b[...], up, ((1,), (0,)))).astype(BF)
        mixq[:, head(h)] = dot_of(probs[:, head(h)], new, ((1,), (0,))).astype(BF)
    cross[:, :high] = (-step_rate * dot_of(mixq[...], z_mine[...], ((1,), (1,)))).astype(BF)

    def value_1(at):
        part = dot_of(mixq[...], ow[:, at], ((1,), (0,))) + dot_of(cross[:, :high], err_1[:high, at], ((1,), (0,)))
        return part[low:]

    half_acc[...] = jnp.zeros_like(half_acc)
    acc[...] = jnp.zeros_like(acc)

    def pairs_of(at, part):
        half_acc[...] += dot_of(part, err_1[:, at], ((1,), (1,)))

    send_parts(1, value_1, query_rows, part_1, got_1, True)
    gather_relay_line(0, z_all)
    take_parts(1, part_1, got_1, query_rows, weight_q, err_2, pairs_of)
    gather_relay_side(0, z_all)

    pairs[...] = (-step_rate * half_acc[...]).astype(BF)
    back[...] = (acc[...] + dot_of(pairs[:, :high], z_mine[...], ((1,), (0,)))).astype(BF)
    left_mine = left_all.at[me]
    for h in range(heads):
        up = dot_of(probs_t[:, head(h)], back[:, head(h)], ((1,), (0,)))
        value_now[:, head(h)] = up
        flow = (-step_rate * dot_of(gram_b[...], up.astype(BF), ((1,), (0,)))).astype(BF)
        again = dot_of(probs[:, head(h)], flow, ((1,), (0,))).astype(BF)
        second[:, head(h)] = again
        left_mine[:, head(h)] = jnp.where(is_support, again, mixq[:, head(h)])

    def value_2(at):
        part = dot_of(second[...], ow[:, at], ((1,), (0,))) + dot_of(cross[...], err_2[:, at], ((0,), (0,)))
        return part[:high]

    acc[...] = jnp.zeros_like(acc)
    cross[:, high:] = jnp.zeros((length, length - high), BF)
    send_parts(2, value_2, support_rows, part_2, got_2, False)

    def join(k, carry):
        at = own_columns(k)
        both[:, at] = jnp.where(is_support, err_1[:, at], err_2[:, at])
        return carry
    lax.fori_loop(0, chunks, join, 0)
    a2a_start(1, both, both_cols)
    gather_start(1, left_all)
    take_parts(2, part_2, got_2, support_rows, weight_s, err_3, nothing)
    a2a_start(2, err_3.at[:high], err_cols)

    back[...] = (acc[...] + dot_of(pairs[...], mixq[...], ((0,), (0,)))).astype(BF)
    rows_mine = rows_all.at[me]
    for h in range(heads):
        late = dot_of(probs_t[:, head(h)], back[:, head(h)], ((1,), (0,)))
        rows_mine[:, head(h)] = ((value_now[:, head(h)] + late) * scale_row).astype(BF)
    gather_relay_line(1, left_all)
    gather_start(2, rows_all)
    gather_relay_side(1, left_all)

    x_cols[me] = xf[:, lanes(me * piece, piece)]
    both_cols[me] = both[:, lanes(me * piece, piece)]
    err_cols[me] = err_3[:high, lanes(me * piece, piece)]

    a2a_wait(0, xf, x_cols)
    a2a_wait(1, both, both_cols)
    gather_finish(0, z_all)
    gather_relay_line(2, rows_all)
    gather_finish(1, left_all)

    tile = 256

    def early(i, carry):
        at = lanes(i * tile, tile)
        do_ref[at, :] = dot_of(
            left_all[:, :, at].reshape(count * length, tile), both_cols[...].reshape(count * length, piece), ((0,), (0,))
        )
        return carry
    lax.fori_loop(0, width // tile, early, 0)
    gather_relay_side(2, rows_all)
    a2a_wait(2, err_3.at[:high], err_cols)

    def late_part(i, carry):
        at = lanes(i * tile, tile)
        do_ref[at, :] += dot_of(
            z_all[:, :, at].reshape(count * high, tile), err_cols[...].reshape(count * high, piece), ((0,), (0,))
        )
        return carry
    lax.fori_loop(0, width // tile, late_part, 0)
    gather_finish(2, rows_all)

    def last(i, carry):
        at = lanes(i * tile, tile)
        dv_ref[:, at] = dot_of(
            x_cols[...].reshape(count * length, piece), rows_all[:, :, at].reshape(count * length, tile), ((0,), (0,))
        )
        return carry
    lax.fori_loop(0, width // tile, last, 0)

    for k in range(near):
        x_copy(k, mine).wait_send()
    for number, (send, got) in enumerate(((part_0, got_0), (part_1, got_1), (part_2, got_2))):
        for k in range(chunks):
            part_copy(number, send, got, k, mine).wait_send()
    for number, array in enumerate((z_all, left_all, rows_all)):
        gather_sent(number, array)


def one_kernel(inputs, targets, queries, key_rows, value_weight, output_weight, splits):
    count = lax.axis_size("task")
    lines = count // 4
    length, half = inputs.shape
    depth = 2 * half
    width = queries.shape[1]
    high = 3 * length // 4
    piece = depth // count
    sends = (lines + 1) + 2 * (lines - 1) + lines
    vm = pltpu.VMEM
    dma = pltpu.SemaphoreType.DMA
    anywhere = pl.BlockSpec(memory_space=pl.ANY)
    chunks = 8
    return pl.pallas_call(
        functools.partial(step_kernel, lines),
        out_shape=(
            jax.ShapeDtypeStruct((piece, width), F32),
            jax.ShapeDtypeStruct((width, piece), F32),
        ),
        in_specs=[anywhere] * 6 + [pl.BlockSpec(memory_space=pltpu.SMEM)],
        out_specs=(pl.BlockSpec(memory_space=pltpu.VMEM), pl.BlockSpec(memory_space=pltpu.VMEM)),
        scratch_shapes=[
            vm((length, depth), BF),
            vm((length, half), BF),
            vm((length, width), BF),
            vm((length, width), BF),
            vm((depth, width), BF),
            vm((width, depth), BF),
            vm((length, width), BF),
            vm((length, width), BF),
            vm((length, width), BF),
            vm((length, width), BF),
            vm((length, width), BF),
            vm((length, width), F32),
            vm((length, length), F32),
            vm((high, depth), BF),
            vm((high, depth), BF),
            vm((high, depth), BF),
            vm((high, depth), BF),
            vm((high, depth), BF),
            vm((high, depth), BF),
            vm((length, depth), BF),
            vm((length, depth), BF),
            vm((length, depth), BF),
            vm((length, depth), BF),
            vm((length, width), BF),
            vm((length, length), BF),
            vm((length, length), BF),
            vm((length, length), BF),
            vm((length, width), F32),
            vm((count, high, width), BF),
            vm((count, length, width), BF),
            vm((count, length, width), BF),
            vm((count, length, piece), BF),
            vm((count, length, piece), BF),
            vm((count, high, piece), BF),
            dma((6,)),
            dma((2, chunks // 2)),
            dma((3, chunks)),
            dma((3, chunks)),
            dma((3, count)),
            dma((3, count)),
            dma((3, sends)),
            dma((3, lines)),
            dma((3, lines)),
            dma((3, lines, 2)),
        ],
        compiler_params=pltpu.CompilerParams(
            collective_id=1, has_side_effects=True, vmem_limit_bytes=60 * 2**20
        ),
    )(inputs, targets, queries, key_rows, value_weight, output_weight, splits)


def make_device(tensor_count):
    def per_device(inputs, targets, queries, key_rows, value_weight, output_weight, splits):
        length = inputs.shape[0]
        low, high = length // 4, 3 * length // 4
        heads = queries.shape[1] // HD
        index = lax.axis_index("tensor")
        normed = normed_rows(full_rows(inputs, tensor_count, index))
        offset_here = inputs.astype(F32) - targets.astype(F32)
        offset = jnp.concatenate(
            [jnp.where(index == block, offset_here, F32(0.0)) for block in range(tensor_count)],
            axis=1,
        )
        probs = attention_probs(queries, key_rows, heads)
        probs_s = probs[:, :high, :high]
        probs_q = probs[:, low:, :]
        split = splits[0]
        count_s = split.astype(F32)
        position = jnp.arange(length)
        support = (position < split).astype(F32)[:, None]
        weight_s = (support / count_s)[:high]
        weight_q = ((1.0 - support) / (F32(length) - count_s))[low:]

        upper = mm(normed, value_weight).astype(BF)
        mixed_s = mix(probs_s, upper[:high]).astype(BF)
        gram = mm_nt(normed, normed).astype(BF)
        mixed_s_all = gather_tokens(mixed_s)
        part_0 = (mm(mixed_s, output_weight) + offset[:high]).astype(BF)
        part_0, normed_sent = lax.optimization_barrier((part_0, normed))
        normed_cols = my_columns(normed_sent)
        error_1 = (weight_s * group_sum(part_0, tensor_count)).astype(BF)

        back_u = mix_back(probs_s, mm_nt(error_1, output_weight).astype(BF)).astype(BF)
        upper_1 = (upper.astype(F32) - step_rate * mm(gram[:, :high], back_u)).astype(BF)
        mixed_q = mix(probs_q, upper_1).astype(BF)
        cross = (-step_rate * mm_nt(mixed_q, mixed_s)).astype(BF)
        part_1 = mm(mixed_q, output_weight) + mm(cross, error_1)
        part_1 = (part_1 + offset[low:]).astype(BF)
        error_2 = (weight_q * group_sum(part_1, tensor_count)).astype(BF)

        errors = (-step_rate * mm_nt(error_2, error_1)).astype(BF)
        back_z1 = (mm_nt(error_2, output_weight) + mm(errors, mixed_s)).astype(BF)
        back_u1 = mix_back(probs_q, back_z1)
        back_u1_b = back_u1.astype(BF)
        back_gram = (-step_rate * mm(gram[:high], back_u1_b)).astype(BF)
        second = mix(probs_s, back_gram).astype(BF)
        error_back = (mm(second, output_weight) + mm_tn(cross, error_2)).astype(BF)
        is_support = (position < split)[:, None]
        left = jnp.where(is_support, below(second, length), above(mixed_q, length))
        errors_both = jnp.where(is_support, below(error_1, length), above(error_2, length))
        error_back, normed_cols, errors_both, left = lax.optimization_barrier(
            (error_back, normed_cols, errors_both, left)
        )
        both_cols = my_columns(errors_both)
        left, mixed_s_all = lax.optimization_barrier((left, mixed_s_all))
        left_all = gather_tokens(left)
        error_sum = group_sum(error_back, tensor_count)
        error_3 = (weight_s * error_sum).astype(BF)
        error_3_cols = my_columns(error_3)

        back_z0 = (mm_nt(error_3, output_weight) + mm_tn(errors, mixed_q)).astype(BF)
        late = mix_back(probs_s, back_z0)
        value_rows = (back_u1 + jnp.pad(late, ((0, length - high), (0, 0)))).astype(BF)
        value_rows_all = gather_by_copies(value_rows, 1)
        total_output = (
            mm_tn(left_all, both_cols)
            + mm_tn(mixed_s_all, error_3_cols)
        )
        total_value = mm_tn(normed_cols, value_rows_all)
        return (total_value, total_output)

    return per_device


def solution(mesh):
    whole_step = mesh.shape["tensor"] == 2 and mesh.shape["task"] % 4 == 0
    return jax.shard_map(
        one_kernel if whole_step else make_device(mesh.shape["tensor"]),
        mesh=mesh,
        in_specs=(
            P("task", "tensor"),
            P("task", "tensor"),
            P("task", "tensor"),
            P("task", "tensor"),
            P(None, "tensor"),
            P("tensor", None),
            P("task"),
        ),
        out_specs=(P("task", "tensor"), P("tensor", "task")),
        check_vma=False,
    )
```

```python
import functools

import jax
import jax.numpy as jnp
from jax import lax
from jax.experimental import pallas as pl
from jax.experimental.pallas import tpu as pltpu
from jax.sharding import PartitionSpec as P

HD = 128
BF = jnp.bfloat16
F32 = jnp.float32

step_rate = 0.25


def normed_rows(inputs):
    values = inputs.astype(F32)
    scale = lax.rsqrt(jnp.mean(values * values, axis=-1, keepdims=True) + 1e-05)
    return (values * scale).astype(BF)


def attention_probs(queries, key_rows, heads):
    length = queries.shape[0]
    query_h = queries.reshape(length, heads, -1)
    key_h = key_rows.reshape(length, heads, -1)
    scores = jnp.einsum("ihd,jhd->hij", query_h, key_h, preferred_element_type=F32)
    scores = scores / jnp.sqrt(F32(query_h.shape[2]))
    position = jnp.arange(length)
    causal = position[:, None] >= position[None, :]
    scores = jnp.where(causal[None], scores, F32(-1e30))
    scores = scores - jnp.max(scores, axis=-1, keepdims=True)
    expo = jnp.exp(scores)
    return (expo / jnp.sum(expo, axis=-1, keepdims=True)).astype(BF)


def mm(left, right):
    return jnp.dot(left, right, preferred_element_type=F32)


def mm_nt(left, right):
    return lax.dot_general(left, right, (((1,), (1,)), ((), ())), preferred_element_type=F32)


def mm_tn(left, right):
    return lax.dot_general(left, right, (((0,), (0,)), ((), ())), preferred_element_type=F32)


def mix(probs, rows):
    heads = probs.shape[0]
    split = rows.reshape(rows.shape[0], heads, -1)
    out = jnp.einsum("hij,jhd->ihd", probs, split, preferred_element_type=F32)
    return out.reshape(out.shape[0], -1)


def mix_back(probs, rows):
    heads = probs.shape[0]
    split = rows.reshape(rows.shape[0], heads, -1)
    out = jnp.einsum("hij,ihd->jhd", probs, split, preferred_element_type=F32)
    return out.reshape(out.shape[0], -1)


def group_sum(term, count):
    term = term.astype(BF)
    if count == 1:
        return term.astype(F32)
    if count == 2:
        other = lax.ppermute(term, "tensor", ((0, 1), (1, 0)))
        return term.astype(F32) + other.astype(F32)
    share = lax.psum_scatter(term, "tensor", scatter_dimension=1, tiled=True)
    return lax.all_gather(share, "tensor", axis=1, tiled=True).astype(F32)


def full_rows(inputs, count, index):
    if count != 2:
        return lax.all_gather(inputs, "tensor", axis=1, tiled=True)
    other = lax.ppermute(inputs, "tensor", ((0, 1), (1, 0)))
    low = jnp.where(index == 0, inputs, other)
    high = jnp.where(index == 0, other, inputs)
    return jnp.concatenate([low, high], axis=1)


def gather_kernel(lines, src_ref, out_ref, own_sem, send_sem, line_sem, side_sem, core_sem):
    me = lax.axis_index("task")
    core, side, line = lax.rem(me, 2), lax.rem(me // 2, 2), me // 4

    def place(back, over_side, over_core):
        line_from = lax.rem(line + lines - back, lines)
        side_from = 1 - side if over_side else side
        core_from = 1 - core if over_core else core
        return (line_from * 2 + side_from) * 2 + core_from

    side_peer, core_peer = place(0, True, False), place(0, False, True)
    peers = [place(lines - step, False, False) for step in range(1, lines)] + [side_peer, core_peer]
    barrier = pltpu.get_barrier_semaphore()
    for peer in peers:
        pl.semaphore_signal(
            barrier, inc=1, device_id={"task": peer}, device_id_type=pl.DeviceIdType.MESH
        )
    pl.semaphore_wait(barrier, len(peers))

    started = []

    def send(source, slot, arrival, peer):
        copy = pltpu.make_async_remote_copy(
            src_ref=source,
            dst_ref=out_ref.at[slot],
            send_sem=send_sem.at[len(started)],
            recv_sem=arrival,
            device_id={"task": peer},
            device_id_type=pl.DeviceIdType.MESH,
        )
        copy.start()
        started.append(copy)

    def arrived(slot, arrival, peer):
        pltpu.make_async_remote_copy(
            src_ref=out_ref.at[slot],
            dst_ref=out_ref.at[slot],
            send_sem=send_sem.at[0],
            recv_sem=arrival,
            device_id={"task": peer},
            device_id_type=pl.DeviceIdType.MESH,
        ).wait_recv()

    for step in sorted(range(1, lines), key=lambda step: -min(step, lines - step)):
        send(src_ref, me, line_sem.at[step], peers[step - 1])
    send(src_ref, me, side_sem.at[0], side_peer)
    send(src_ref, me, core_sem.at[0, 0], core_peer)
    own = pltpu.make_async_copy(src_ref, out_ref.at[me], own_sem)
    own.start()
    order = sorted(range(1, lines), key=lambda step: min(step, lines - step))
    for step in order:
        slot = place(step, False, False)
        arrived(slot, line_sem.at[step], side_peer)
        send(out_ref.at[slot], slot, side_sem.at[step], side_peer)
        send(out_ref.at[slot], slot, core_sem.at[step, 0], core_peer)
    for step in [0] + order:
        slot = place(step, True, False)
        arrived(slot, side_sem.at[step], side_peer)
        send(out_ref.at[slot], slot, core_sem.at[step, 1], core_peer)
    for step in [0] + order:
        for over in range(2):
            arrived(place(step, over == 1, True), core_sem.at[step, over], core_peer)
    own.wait()
    for copy in started:
        copy.wait_send()


def gather_by_copies(rows, number):
    count = lax.axis_size("task")
    if count % 4:
        return gather_tokens(rows)
    lines = count // 4
    sends = (lines + 1) + 2 * (lines - 1) + lines
    gathered = pl.pallas_call(
        functools.partial(gather_kernel, lines),
        out_shape=jax.ShapeDtypeStruct((count,) + rows.shape, rows.dtype),
        in_specs=[pl.BlockSpec(memory_space=pltpu.VMEM)],
        out_specs=pl.BlockSpec(memory_space=pltpu.VMEM),
        scratch_shapes=[
            pltpu.SemaphoreType.DMA,
            pltpu.SemaphoreType.DMA((sends,)),
            pltpu.SemaphoreType.DMA((lines,)),
            pltpu.SemaphoreType.DMA((lines,)),
            pltpu.SemaphoreType.DMA((lines, 2)),
        ],
        compiler_params=pltpu.CompilerParams(collective_id=number, has_side_effects=True),
        cost_estimate=pl.CostEstimate(
            flops=0, bytes_accessed=16 * rows.size * rows.dtype.itemsize * count, transcendentals=0
        ),
    )(rows)
    return gathered.reshape(count * rows.shape[0], rows.shape[1])


def gather_tokens(rows):
    return lax.all_gather(rows, "task", axis=0, tiled=True)


def my_columns(rows):
    return lax.all_to_all(rows, "task", split_axis=1, concat_axis=0, tiled=True)


def below(rows, length):
    return jnp.pad(rows, ((0, length - rows.shape[0]), (0, 0)))


def above(rows, length):
    return jnp.pad(rows, ((length - rows.shape[0], 0), (0, 0)))


MESH = pl.DeviceIdType.MESH


def dot_of(left, right, dims):
    return lax.dot_general(left, right, (dims, ((), ())), preferred_element_type=F32)


def step_kernel(
    lines,
    x_in, t_in, q_in, k_in, v_in, o_in, split_ref,
    dv_ref, do_ref,
    xf, tg, qs, ks, vw, ow, probs, probs_t, upper, mixq, second, left, acc, half_acc,
    part_0, part_1, part_2, got_0, got_1, got_2, err_1, err_2, err_3, both,
    back, gram_b, cross, cross_got, pairs, value_now, z_mine, a_all, left_all, rows_all,
    x_cols, both_cols, right_a, swap, swap_got,
    load_sem, x_sem, part_sem, part_got, cross_sem, swap_sem,
    a2a_send, a2a_got, g_send, g_line, g_side, g_core,
):
    count = lines * 4
    length, depth = xf.shape
    half = depth // 2
    width = upper.shape[1]
    heads = width // HD
    low, high = length // 4, 3 * length // 4
    piece = depth // count
    chunks = 8
    cut = depth // chunks
    near = chunks // 2

    me = lax.axis_index("task")
    mine = lax.axis_index("tensor")
    core, side, line = lax.rem(me, 2), lax.rem(me // 2, 2), me // 4
    pair = {"tensor": 1 - mine}

    def place(line_at, side_at, core_at):
        return (line_at * 2 + side_at) * 2 + core_at

    def lanes(start, size):
        return pl.ds(pl.multiple_of(start, 128), size)

    own_half = lanes(mine * half, half)
    loads = [
        pltpu.make_async_copy(x_in, xf.at[:, own_half], load_sem.at[0]),
        pltpu.make_async_copy(q_in, qs, load_sem.at[1]),
        pltpu.make_async_copy(k_in, ks, load_sem.at[2]),
        pltpu.make_async_copy(v_in, vw, load_sem.at[3]),
        pltpu.make_async_copy(t_in, tg, load_sem.at[4]),
        pltpu.make_async_copy(o_in, ow, load_sem.at[5]),
    ]
    for load in loads:
        load.start()

    barrier = pltpu.get_barrier_semaphore()
    for step in range(1, count):
        pl.semaphore_signal(
            barrier, inc=1, device_id={"task": lax.rem(me + step, count)}, device_id_type=MESH
        )
    pl.semaphore_signal(barrier, inc=1, device_id=pair, device_id_type=MESH)
    pl.semaphore_wait(barrier, count)

    def remote(src, dst, send, got, peer):
        return pltpu.make_async_remote_copy(
            src_ref=src, dst_ref=dst, send_sem=send, recv_sem=got, device_id=peer, device_id_type=MESH
        )

    def x_copy(k, owner):
        part = xf.at[:, lanes(owner * half + k * cut, cut)]
        return remote(part, part, x_sem.at[0, k], x_sem.at[1, k], pair)

    loads[0].wait()
    for k in range(near):
        x_copy(k, mine).start()

    def a2a_copy(number, src, dst, rows, step):
        peer = lax.rem(me + step, count)
        return remote(
            src.at[rows, lanes(peer * piece, piece)],
            dst.at[me, rows],
            a2a_send.at[number, step],
            a2a_got.at[number, step],
            {"task": peer},
        )

    def a2a_start(number, src, dst, rows, first=1, last=count):
        def one(step, carry):
            a2a_copy(number, src, dst, rows, step).start()
            return carry
        lax.fori_loop(first, last, one, 0)

    def a2a_wait(number, src, dst, rows):
        def one(step, carry):
            a2a_copy(number, src, dst, rows, step).wait()
            return carry
        lax.fori_loop(1, count, one, 0)

    all_rows = pl.ds(0, length)

    def x_spread(own):
        def one(step, carry):
            peer = lax.rem(me + step, count)
            here = (peer // (count // 2)) == mine
            @pl.when(here if own else jnp.logical_not(here))
            def _():
                a2a_copy(0, xf, x_cols, all_rows, step).start()
            return carry
        lax.fori_loop(1, count, one, 0)

    x_spread(True)

    def gather_copy(number, array, slot, kind, source, got, peer):
        block = array.at[slot]
        return remote(block, block, g_send.at[number, kind, source], got, {"task": peer})

    up_peer, down_peer = me + 4, me - 4
    side_peer, core_peer = place(line, 1 - side, core), place(line, side, 1 - core)

    def pass_on(number, array, source):
        slot = place(source, side, core)
        @pl.when(jnp.logical_and(source <= line, line < lines - 1))
        def _():
            gather_copy(number, array, slot, 0, source, g_line.at[number, source], up_peer).start()
        @pl.when(jnp.logical_and(source >= line, line > 0))
        def _():
            gather_copy(number, array, slot, 1, source, g_line.at[number, source], down_peer).start()
        gather_copy(number, array, slot, 2, source, g_side.at[number, source], side_peer).start()
        gather_copy(number, array, slot, 3, source, g_core.at[number, source, 0], core_peer).start()

    def gather_start(number, array):
        pass_on(number, array, line)

    def gather_line(number, array, away):
        def take(source):
            slot = place(source, side, core)
            gather_copy(number, array, slot, 2, source, g_line.at[number, source], side_peer).wait_recv()
            pass_on(number, array, source)
        @pl.when(line >= away)
        def _():
            take(line - away)
        @pl.when(line + away < lines)
        def _():
            take(line + away)

    def gather_side(number, array):
        for source in range(lines):
            slot = place(source, 1 - side, core)
            gather_copy(number, array, slot, 4, source, g_side.at[number, source], core_peer).wait_recv()
            gather_copy(number, array, slot, 4, source, g_core.at[number, source, 1], core_peer).start()

    def gather_finish(number, array):
        for source in range(lines):
            for over in range(2):
                slot = place(source, side if over == 0 else 1 - side, 1 - core)
                gather_copy(number, array, slot, 3, source, g_core.at[number, source, over], core_peer).wait_recv()

    def gather_sent(number, array):
        def sent(kind, source):
            gather_copy(number, array, me, kind, source, g_core.at[number, source, 0], core_peer).wait_send()
        for source in range(lines):
            @pl.when(jnp.logical_and(source <= line, line < lines - 1))
            def _():
                sent(0, source)
            @pl.when(jnp.logical_and(source >= line, line > 0))
            def _():
                sent(1, source)
            for kind in range(2, 5):
                sent(kind, source)

    def head(h):
        return slice(h * HD, (h + 1) * HD)

    row = lax.broadcasted_iota(jnp.int32, (length, length), 0)
    col = lax.broadcasted_iota(jnp.int32, (length, length), 1)
    causal = row >= col
    loads[1].wait()
    loads[2].wait()
    root = jnp.sqrt(F32(HD))
    for h in range(heads):
        scores = dot_of(qs[:, head(h)], ks[:, head(h)], ((1,), (1,))) / root
        scores = jnp.where(causal, scores, F32(-1e30))
        scores = scores - jnp.max(scores, axis=-1, keepdims=True)
        expo = jnp.exp(scores)
        prob = expo / jnp.sum(expo, axis=-1, keepdims=True)
        probs[:, head(h)] = prob.astype(BF)
        probs_t[:, head(h)] = prob.T.astype(BF)

    err_1[high:, :] = jnp.zeros((length - high, depth), BF)
    err_2[:low, :] = jnp.zeros((low, depth), BF)
    err_3[high:, :] = jnp.zeros((length - high, depth), BF)
    position = lax.broadcasted_iota(jnp.int32, (length, 1), 0)
    split = jnp.full((length, 1), split_ref[0], jnp.int32)
    is_support = position < split
    support = is_support.astype(F32)
    count_s = split.astype(F32)
    weight_s = support / count_s
    weight_q = (1.0 - support) / (F32(length) - count_s)

    loads[3].wait()

    def take(k, owner, first):
        at = lanes(owner * half + k * cut, cut)
        x_part = xf[:, at]
        new = dot_of(x_part, vw[pl.ds(pl.multiple_of(owner * half + k * cut, 128), cut), :], ((1,), (0,)))
        gram = dot_of(x_part, x_part, ((1,), (1,)))
        if first:
            acc[...] = new
            half_acc[...] = gram
        else:
            acc[...] += new
            half_acc[...] += gram

    take(0, mine, True)
    def own_take(k, carry):
        take(k, mine, False)
        return carry
    lax.fori_loop(1, near, own_take, 0)
    def other_take(k, carry):
        x_copy(k, 1 - mine).wait_recv()
        take(k, 1 - mine, False)
        return carry
    lax.fori_loop(0, near, other_take, 0)
    x_spread(False)

    gram_raw = half_acc[...]
    diagonal = jnp.where(row == col, gram_raw, F32(0.0))
    scale_row = lax.rsqrt(jnp.sum(diagonal, axis=1, keepdims=True) / F32(depth) + 1e-05)
    scale_col = lax.rsqrt(jnp.sum(diagonal, axis=0, keepdims=True) / F32(depth) + 1e-05)
    gram_b[...] = (gram_raw * scale_row * scale_col).astype(BF)
    upper[...] = (acc[...] * scale_row).astype(BF)

    a_mine = a_all.at[me]
    for h in range(heads):
        mixed = dot_of(probs[:, head(h)], upper[:, head(h)], ((1,), (0,)))
        z_mine[:, head(h)] = mixed[:high].astype(BF)
    a_mine[:high, :] = (weight_s[:high] * z_mine[...].astype(F32)).astype(BF)
    loads[4].wait()
    loads[5].wait()

    def part_copy(number, send, got, k, owner):
        at = lanes(lax.rem(owner * near + k, chunks) * cut, cut)
        return remote(send.at[:, at], got.at[:, at], part_sem.at[number, k], part_got.at[number, k], pair)

    def own_columns(k):
        return lanes(lax.rem(mine * near + k, chunks) * cut, cut)

    def other_columns(k):
        return lanes(lax.rem((1 - mine) * near + k, chunks) * cut, cut)

    def offset(k, rows):
        there = lanes(k * cut, cut)
        return xf[rows, own_columns(k)].astype(F32) - tg[rows, there].astype(F32)

    def send_parts(number, value, rows, send, got, with_offset):
        def one(k, near_half):
            at = own_columns(k)
            part = value(at)
            if near_half and with_offset:
                part = part + offset(k, rows)
            send[:, at] = part.astype(BF)
            part_copy(number, send, got, k, mine).start()
        def first(k, carry):
            one(k, True)
            return carry
        def later(k, carry):
            one(k, False)
            return carry
        lax.fori_loop(0, near, first, 0)
        lax.fori_loop(near, chunks, later, 0)

    def take_parts(number, send, got, rows, weight, error, also, first=0, last=chunks):
        def one(k, carry):
            at = other_columns(k)
            part_copy(number, send, got, k, 1 - mine).wait_recv()
            total = send[:, at].astype(F32) + got[:, at].astype(F32)
            error[rows, at] = (weight[rows] * total).astype(BF)
            part = error[:, at]
            acc[...] += dot_of(part, ow[:, at], ((1,), (1,)))
            also(at, part)
            return carry
        lax.fori_loop(first, last, one, 0)

    support_rows, query_rows = slice(0, high), slice(low, length)
    nothing = lambda at, part: None

    def value_0(at):
        return dot_of(z_mine[...], ow[:, at], ((1,), (0,)))

    early_rows, middle_rows, late_rows = pl.ds(0, low), pl.ds(low, high - low), pl.ds(high, length - high)
    acc[...] = jnp.zeros_like(acc)
    send_parts(0, value_0, support_rows, part_0, got_0, True)
    take_parts(0, part_0, got_0, support_rows, weight_s, err_1, nothing)
    a2a_start(1, err_1, both_cols, early_rows)

    back[...] = acc[...].astype(BF)
    for h in range(heads):
        up = dot_of(probs_t[:, head(h)], back[:, head(h)], ((1,), (0,))).astype(BF)
        new = (upper[:, head(h)].astype(F32) - step_rate * dot_of(gram_b[...], up, ((1,), (0,)))).astype(BF)
        mixq[:, head(h)] = dot_of(probs[:, head(h)], new, ((1,), (0,))).astype(BF)
    cross[:, high:] = jnp.zeros((length, length - high), BF)
    product = -step_rate * dot_of(mixq[...], z_mine[...], ((1,), (1,)))
    cross[:, :high] = jnp.where(is_support, F32(0.0), product).astype(BF)
    cross_copy = remote(cross, cross_got, cross_sem.at[0], cross_sem.at[1], pair)
    cross_copy.start()

    def value_1(at):
        part = dot_of(mixq[...], ow[:, at], ((1,), (0,))) + dot_of(cross[:, :high], err_1[:high, at], ((1,), (0,)))
        return part[low:]

    half_acc[...] = jnp.zeros_like(half_acc)
    acc[...] = jnp.zeros_like(acc)

    def pairs_of(at, part):
        half_acc[...] += dot_of(part, err_1[:, at], ((1,), (1,)))

    send_parts(1, value_1, query_rows, part_1, got_1, True)
    cross_copy.wait_recv()
    cross_sum = (cross[...].astype(F32) + cross_got[...].astype(F32)).astype(BF)
    left[...] = (mixq[...].astype(F32) + dot_of(cross_sum[:, :high], a_mine[:high], ((1,), (0,)))).astype(BF)
    a_mine[high:, :] = left[high:, :]
    gather_start(0, a_all)
    take_parts(1, part_1, got_1, query_rows, weight_q, err_2, pairs_of, 0, 5)
    gather_line(0, a_all, 1)
    take_parts(1, part_1, got_1, query_rows, weight_q, err_2, pairs_of, 5, chunks)

    pairs[...] = (-step_rate * half_acc[...]).astype(BF)
    back[...] = (acc[...] + dot_of(pairs[:, :high], z_mine[...], ((1,), (0,)))).astype(BF)
    left_mine = left_all.at[me]
    for h in range(heads):
        up = dot_of(probs_t[:, head(h)], back[:, head(h)], ((1,), (0,)))
        value_now[:, head(h)] = up
        flow = (-step_rate * dot_of(gram_b[...], up.astype(BF), ((1,), (0,)))).astype(BF)
        again = dot_of(probs[:, head(h)], flow, ((1,), (0,))).astype(BF)
        second[:, head(h)] = again
        left_mine[:, head(h)] = jnp.where(is_support, again, left[:, head(h)])[:high]

    def value_2(at):
        part = dot_of(second[...], ow[:, at], ((1,), (0,))) + dot_of(cross[...], err_2[:, at], ((0,), (0,)))
        return part[:high]

    acc[...] = jnp.zeros_like(acc)
    gather_start(1, left_all)
    send_parts(2, value_2, support_rows, part_2, got_2, False)

    def join(k, carry):
        at = own_columns(k)
        both[:, at] = jnp.where(is_support, err_1[:, at], err_2[:, at])
        return carry
    lax.fori_loop(0, chunks, join, 0)
    gather_line(0, a_all, 2)
    take_parts(2, part_2, got_2, support_rows, weight_s, err_3, nothing, 0, 3)
    for away in range(3, lines):
        gather_line(0, a_all, away)
    gather_line(1, left_all, 1)
    a2a_start(2, both, both_cols, middle_rows, 1, count // 2)
    a2a_start(3, both, right_a, late_rows, 1, count // 2)
    take_parts(2, part_2, got_2, support_rows, weight_s, err_3, nothing, 3, 6)
    gather_line(1, left_all, 2)
    gather_side(0, a_all)
    a2a_start(2, both, both_cols, middle_rows, count // 2, count)
    a2a_start(3, both, right_a, late_rows, count // 2, count)
    take_parts(2, part_2, got_2, support_rows, weight_s, err_3, nothing, 6, chunks)

    back[...] = (acc[...] + dot_of(pairs[...], mixq[...], ((0,), (0,)))).astype(BF)
    rows_mine = rows_all.at[me]
    for h in range(heads):
        late = dot_of(probs_t[:, head(h)], back[:, head(h)], ((1,), (0,)))
        rows_mine[:, head(h)] = ((value_now[:, head(h)] + late) * scale_row).astype(BF)
    gather_start(2, rows_all)
    for away in range(3, lines):
        gather_line(1, left_all, away)
    gather_side(1, left_all)

    x_cols[me] = xf[:, lanes(me * piece, piece)]
    both_cols[me] = both[:high, lanes(me * piece, piece)]
    right_a[me, late_rows] = both[high:, lanes(me * piece, piece)]

    def swap_copy(slot):
        return remote(swap.at[slot], swap_got.at[slot], swap_sem.at[0, slot], swap_sem.at[1, slot], pair)

    def swap_one(slot):
        swap[slot] = dot_of(left_all[slot], ow[:, lanes(me * piece, piece)], ((1,), (0,))).astype(BF)
        swap_copy(slot).start()

    def swap_core(source, carry):
        swap_one(place(source // 2, lax.rem(source, 2), core))
        return carry

    def swap_other(source, carry):
        swap_one(place(source // 2, lax.rem(source, 2), 1 - core))
        return carry

    lax.fori_loop(0, count // 2, swap_core, 0)
    gather_line(2, rows_all, 1)
    gather_finish(1, left_all)
    lax.fori_loop(0, count // 2, swap_other, 0)
    gather_line(2, rows_all, 2)
    a2a_wait(0, xf, x_cols, all_rows)
    a2a_wait(1, err_1, both_cols, early_rows)
    a2a_wait(2, both, both_cols, middle_rows)

    tile = 256

    def early(i, carry):
        at = lanes(i * tile, tile)
        do_ref[at, :] = dot_of(
            left_all[:, :, at].reshape(count * high, tile), both_cols[...].reshape(count * high, piece), ((0,), (0,))
        )
        return carry
    lax.fori_loop(0, width // tile, early, 0)
    for away in range(3, lines):
        gather_line(2, rows_all, away)
    a2a_wait(3, both, right_a, late_rows)
    gather_finish(0, a_all)
    gather_side(2, rows_all)

    def swapped(slot, carry):
        swap_copy(slot).wait()
        right_a[slot, :high] = (swap[slot].astype(F32) + swap_got[slot].astype(F32)).astype(BF)
        return carry
    lax.fori_loop(0, count, swapped, 0)

    def late_part(i, carry):
        at = lanes(i * tile, tile)
        do_ref[at, :] += dot_of(
            a_all[:, :, at].reshape(count * length, tile), right_a[...].reshape(count * length, piece), ((0,), (0,))
        )
        return carry
    lax.fori_loop(0, width // tile, late_part, 0)
    gather_finish(2, rows_all)

    def last(i, carry):
        at = lanes(i * tile, tile)
        dv_ref[:, at] = dot_of(
            x_cols[...].reshape(count * length, piece), rows_all[:, :, at].reshape(count * length, tile), ((0,), (0,))
        )
        return carry
    lax.fori_loop(0, width // tile, last, 0)

    cross_copy.wait_send()
    for k in range(near):
        x_copy(k, mine).wait_send()
    for number, (send, got) in enumerate(((part_0, got_0), (part_1, got_1), (part_2, got_2))):
        for k in range(chunks):
            part_copy(number, send, got, k, mine).wait_send()
    for number, array in enumerate((a_all, left_all, rows_all)):
        gather_sent(number, array)


def one_kernel(inputs, targets, queries, key_rows, value_weight, output_weight, splits):
    count = lax.axis_size("task")
    lines = count // 4
    length, half = inputs.shape
    depth = 2 * half
    width = queries.shape[1]
    high = 3 * length // 4
    piece = depth // count
    vm = pltpu.VMEM
    dma = pltpu.SemaphoreType.DMA
    anywhere = pl.BlockSpec(memory_space=pl.ANY)
    chunks = 8
    return pl.pallas_call(
        functools.partial(step_kernel, lines),
        out_shape=(
            jax.ShapeDtypeStruct((piece, width), F32),
            jax.ShapeDtypeStruct((width, piece), F32),
        ),
        in_specs=[anywhere] * 6 + [pl.BlockSpec(memory_space=pltpu.SMEM)],
        out_specs=(pl.BlockSpec(memory_space=pltpu.VMEM), pl.BlockSpec(memory_space=pltpu.VMEM)),
        scratch_shapes=[
            vm((length, depth), BF),
            vm((length, half), BF),
            vm((length, width), BF),
            vm((length, width), BF),
            vm((depth, width), BF),
            vm((width, depth), BF),
        ]
        + [vm((length, width), BF)] * 6
        + [vm((length, width), F32), vm((length, length), F32)]
        + [vm((high, depth), BF)] * 6
        + [vm((length, depth), BF)] * 4
        + [vm((length, width), BF)]
        + [vm((length, length), BF)] * 4
        + [
            vm((length, width), F32),
            vm((high, width), BF),
            vm((count, length, width), BF),
            vm((count, high, width), BF),
            vm((count, length, width), BF),
            vm((count, length, piece), BF),
            vm((count, high, piece), BF),
            vm((count, length, piece), BF),
            vm((count, high, piece), BF),
            vm((count, high, piece), BF),
            dma((6,)),
            dma((2, chunks // 2)),
            dma((3, chunks)),
            dma((3, chunks)),
            dma((2,)),
            dma((2, count)),
            dma((4, count)),
            dma((4, count)),
            dma((3, 5, lines)),
            dma((3, lines)),
            dma((3, lines)),
            dma((3, lines, 2)),
        ],
        compiler_params=pltpu.CompilerParams(
            collective_id=1, has_side_effects=True, vmem_limit_bytes=60 * 2**20
        ),
    )(inputs, targets, queries, key_rows, value_weight, output_weight, splits)


def make_device(tensor_count):
    def per_device(inputs, targets, queries, key_rows, value_weight, output_weight, splits):
        length = inputs.shape[0]
        low, high = length // 4, 3 * length // 4
        heads = queries.shape[1] // HD
        index = lax.axis_index("tensor")
        normed = normed_rows(full_rows(inputs, tensor_count, index))
        offset_here = inputs.astype(F32) - targets.astype(F32)
        offset = jnp.concatenate(
            [jnp.where(index == block, offset_here, F32(0.0)) for block in range(tensor_count)],
            axis=1,
        )
        probs = attention_probs(queries, key_rows, heads)
        probs_s = probs[:, :high, :high]
        probs_q = probs[:, low:, :]
        split = splits[0]
        count_s = split.astype(F32)
        position = jnp.arange(length)
        support = (position < split).astype(F32)[:, None]
        weight_s = (support / count_s)[:high]
        weight_q = ((1.0 - support) / (F32(length) - count_s))[low:]

        upper = mm(normed, value_weight).astype(BF)
        mixed_s = mix(probs_s, upper[:high]).astype(BF)
        gram = mm_nt(normed, normed).astype(BF)
        mixed_s_all = gather_tokens(mixed_s)
        part_0 = (mm(mixed_s, output_weight) + offset[:high]).astype(BF)
        part_0, normed_sent = lax.optimization_barrier((part_0, normed))
        normed_cols = my_columns(normed_sent)
        error_1 = (weight_s * group_sum(part_0, tensor_count)).astype(BF)

        back_u = mix_back(probs_s, mm_nt(error_1, output_weight).astype(BF)).astype(BF)
        upper_1 = (upper.astype(F32) - step_rate * mm(gram[:, :high], back_u)).astype(BF)
        mixed_q = mix(probs_q, upper_1).astype(BF)
        cross = (-step_rate * mm_nt(mixed_q, mixed_s)).astype(BF)
        part_1 = mm(mixed_q, output_weight) + mm(cross, error_1)
        part_1 = (part_1 + offset[low:]).astype(BF)
        error_2 = (weight_q * group_sum(part_1, tensor_count)).astype(BF)

        errors = (-step_rate * mm_nt(error_2, error_1)).astype(BF)
        back_z1 = (mm_nt(error_2, output_weight) + mm(errors, mixed_s)).astype(BF)
        back_u1 = mix_back(probs_q, back_z1)
        back_u1_b = back_u1.astype(BF)
        back_gram = (-step_rate * mm(gram[:high], back_u1_b)).astype(BF)
        second = mix(probs_s, back_gram).astype(BF)
        error_back = (mm(second, output_weight) + mm_tn(cross, error_2)).astype(BF)
        is_support = (position < split)[:, None]
        left = jnp.where(is_support, below(second, length), above(mixed_q, length))
        errors_both = jnp.where(is_support, below(error_1, length), above(error_2, length))
        error_back, normed_cols, errors_both, left = lax.optimization_barrier(
            (error_back, normed_cols, errors_both, left)
        )
        both_cols = my_columns(errors_both)
        left, mixed_s_all = lax.optimization_barrier((left, mixed_s_all))
        left_all = gather_tokens(left)
        error_sum = group_sum(error_back, tensor_count)
        error_3 = (weight_s * error_sum).astype(BF)
        error_3_cols = my_columns(error_3)

        back_z0 = (mm_nt(error_3, output_weight) + mm_tn(errors, mixed_q)).astype(BF)
        late = mix_back(probs_s, back_z0)
        value_rows = (back_u1 + jnp.pad(late, ((0, length - high), (0, 0)))).astype(BF)
        value_rows_all = gather_by_copies(value_rows, 1)
        total_output = (
            mm_tn(left_all, both_cols)
            + mm_tn(mixed_s_all, error_3_cols)
        )
        total_value = mm_tn(normed_cols, value_rows_all)
        return (total_value, total_output)

    return per_device


def solution(mesh):
    whole_step = mesh.shape["tensor"] == 2 and mesh.shape["task"] % 4 == 0
    return jax.shard_map(
        one_kernel if whole_step else make_device(mesh.shape["tensor"]),
        mesh=mesh,
        in_specs=(
            P("task", "tensor"),
            P("task", "tensor"),
            P("task", "tensor"),
            P("task", "tensor"),
            P(None, "tensor"),
            P("tensor", None),
            P("task"),
        ),
        out_specs=(P("task", "tensor"), P("tensor", "task")),
        check_vma=False,
    )
```

```python
import functools

import jax
import jax.numpy as jnp
from jax import lax
from jax.experimental import pallas as pl
from jax.experimental.pallas import tpu as pltpu
from jax.sharding import PartitionSpec as P

HD = 128
BF = jnp.bfloat16
F32 = jnp.float32

step_rate = 0.25


def normed_rows(inputs):
    values = inputs.astype(F32)
    scale = lax.rsqrt(jnp.mean(values * values, axis=-1, keepdims=True) + 1e-05)
    return (values * scale).astype(BF)


def attention_probs(queries, key_rows, heads):
    length = queries.shape[0]
    query_h = queries.reshape(length, heads, -1)
    key_h = key_rows.reshape(length, heads, -1)
    scores = jnp.einsum("ihd,jhd->hij", query_h, key_h, preferred_element_type=F32)
    scores = scores / jnp.sqrt(F32(query_h.shape[2]))
    position = jnp.arange(length)
    causal = position[:, None] >= position[None, :]
    scores = jnp.where(causal[None], scores, F32(-1e30))
    scores = scores - jnp.max(scores, axis=-1, keepdims=True)
    expo = jnp.exp(scores)
    return (expo / jnp.sum(expo, axis=-1, keepdims=True)).astype(BF)


def mm(left, right):
    return jnp.dot(left, right, preferred_element_type=F32)


def mm_nt(left, right):
    return lax.dot_general(left, right, (((1,), (1,)), ((), ())), preferred_element_type=F32)


def mm_tn(left, right):
    return lax.dot_general(left, right, (((0,), (0,)), ((), ())), preferred_element_type=F32)


def mix(probs, rows):
    heads = probs.shape[0]
    split = rows.reshape(rows.shape[0], heads, -1)
    out = jnp.einsum("hij,jhd->ihd", probs, split, preferred_element_type=F32)
    return out.reshape(out.shape[0], -1)


def mix_back(probs, rows):
    heads = probs.shape[0]
    split = rows.reshape(rows.shape[0], heads, -1)
    out = jnp.einsum("hij,ihd->jhd", probs, split, preferred_element_type=F32)
    return out.reshape(out.shape[0], -1)


def group_sum(term, count):
    term = term.astype(BF)
    if count == 1:
        return term.astype(F32)
    if count == 2:
        other = lax.ppermute(term, "tensor", ((0, 1), (1, 0)))
        return term.astype(F32) + other.astype(F32)
    share = lax.psum_scatter(term, "tensor", scatter_dimension=1, tiled=True)
    return lax.all_gather(share, "tensor", axis=1, tiled=True).astype(F32)


def full_rows(inputs, count, index):
    if count != 2:
        return lax.all_gather(inputs, "tensor", axis=1, tiled=True)
    other = lax.ppermute(inputs, "tensor", ((0, 1), (1, 0)))
    low = jnp.where(index == 0, inputs, other)
    high = jnp.where(index == 0, other, inputs)
    return jnp.concatenate([low, high], axis=1)


def gather_kernel(lines, src_ref, out_ref, own_sem, send_sem, line_sem, side_sem, core_sem):
    me = lax.axis_index("task")
    core, side, line = lax.rem(me, 2), lax.rem(me // 2, 2), me // 4

    def place(back, over_side, over_core):
        line_from = lax.rem(line + lines - back, lines)
        side_from = 1 - side if over_side else side
        core_from = 1 - core if over_core else core
        return (line_from * 2 + side_from) * 2 + core_from

    side_peer, core_peer = place(0, True, False), place(0, False, True)
    peers = [place(lines - step, False, False) for step in range(1, lines)] + [side_peer, core_peer]
    barrier = pltpu.get_barrier_semaphore()
    for peer in peers:
        pl.semaphore_signal(
            barrier, inc=1, device_id={"task": peer}, device_id_type=pl.DeviceIdType.MESH
        )
    pl.semaphore_wait(barrier, len(peers))

    started = []

    def send(source, slot, arrival, peer):
        copy = pltpu.make_async_remote_copy(
            src_ref=source,
            dst_ref=out_ref.at[slot],
            send_sem=send_sem.at[len(started)],
            recv_sem=arrival,
            device_id={"task": peer},
            device_id_type=pl.DeviceIdType.MESH,
        )
        copy.start()
        started.append(copy)

    def arrived(slot, arrival, peer):
        pltpu.make_async_remote_copy(
            src_ref=out_ref.at[slot],
            dst_ref=out_ref.at[slot],
            send_sem=send_sem.at[0],
            recv_sem=arrival,
            device_id={"task": peer},
            device_id_type=pl.DeviceIdType.MESH,
        ).wait_recv()

    for step in sorted(range(1, lines), key=lambda step: -min(step, lines - step)):
        send(src_ref, me, line_sem.at[step], peers[step - 1])
    send(src_ref, me, side_sem.at[0], side_peer)
    send(src_ref, me, core_sem.at[0, 0], core_peer)
    own = pltpu.make_async_copy(src_ref, out_ref.at[me], own_sem)
    own.start()
    order = sorted(range(1, lines), key=lambda step: min(step, lines - step))
    for step in order:
        slot = place(step, False, False)
        arrived(slot, line_sem.at[step], side_peer)
        send(out_ref.at[slot], slot, side_sem.at[step], side_peer)
        send(out_ref.at[slot], slot, core_sem.at[step, 0], core_peer)
    for step in [0] + order:
        slot = place(step, True, False)
        arrived(slot, side_sem.at[step], side_peer)
        send(out_ref.at[slot], slot, core_sem.at[step, 1], core_peer)
    for step in [0] + order:
        for over in range(2):
            arrived(place(step, over == 1, True), core_sem.at[step, over], core_peer)
    own.wait()
    for copy in started:
        copy.wait_send()


def gather_by_copies(rows, number):
    count = lax.axis_size("task")
    if count % 4:
        return gather_tokens(rows)
    lines = count // 4
    sends = (lines + 1) + 2 * (lines - 1) + lines
    gathered = pl.pallas_call(
        functools.partial(gather_kernel, lines),
        out_shape=jax.ShapeDtypeStruct((count,) + rows.shape, rows.dtype),
        in_specs=[pl.BlockSpec(memory_space=pltpu.VMEM)],
        out_specs=pl.BlockSpec(memory_space=pltpu.VMEM),
        scratch_shapes=[
            pltpu.SemaphoreType.DMA,
            pltpu.SemaphoreType.DMA((sends,)),
            pltpu.SemaphoreType.DMA((lines,)),
            pltpu.SemaphoreType.DMA((lines,)),
            pltpu.SemaphoreType.DMA((lines, 2)),
        ],
        compiler_params=pltpu.CompilerParams(collective_id=number, has_side_effects=True),
        cost_estimate=pl.CostEstimate(
            flops=0, bytes_accessed=16 * rows.size * rows.dtype.itemsize * count, transcendentals=0
        ),
    )(rows)
    return gathered.reshape(count * rows.shape[0], rows.shape[1])


def gather_tokens(rows):
    return lax.all_gather(rows, "task", axis=0, tiled=True)


def my_columns(rows):
    return lax.all_to_all(rows, "task", split_axis=1, concat_axis=0, tiled=True)


def below(rows, length):
    return jnp.pad(rows, ((0, length - rows.shape[0]), (0, 0)))


def above(rows, length):
    return jnp.pad(rows, ((length - rows.shape[0], 0), (0, 0)))


MESH = pl.DeviceIdType.MESH


def dot_of(left, right, dims):
    return lax.dot_general(left, right, (dims, ((), ())), preferred_element_type=F32)


def step_kernel(
    lines,
    x_in, t_in, q_in, k_in, v_in, o_in, split_ref,
    dv_ref, do_ref,
    xf, tg, qs, ks, vw, ow, probs, probs_t, upper, mixq, second, left, acc, half_acc,
    part_0, part_1, part_2, got_0, got_1, got_2, err_1, err_2, err_3, both,
    back, gram_b, cross, cross_got, pairs, value_now, z_mine, a_all, left_all, rows_all,
    x_cols, both_cols, right_a, swap, swap_got,
    load_sem, x_sem, part_sem, part_got, cross_sem, swap_sem,
    a2a_send, a2a_got, g_send, g_line, g_side, g_core,
):
    count = lines * 4
    length, depth = xf.shape
    half = depth // 2
    width = upper.shape[1]
    heads = width // HD
    low, high = length // 4, 3 * length // 4
    piece = depth // count
    chunks = 8
    cut = depth // chunks
    near = chunks // 2

    me = lax.axis_index("task")
    mine = lax.axis_index("tensor")
    core, side, line = lax.rem(me, 2), lax.rem(me // 2, 2), me // 4
    pair = {"tensor": 1 - mine}

    def place(line_at, side_at, core_at):
        return (line_at * 2 + side_at) * 2 + core_at

    def lanes(start, size):
        return pl.ds(pl.multiple_of(start, 128), size)

    own_half = lanes(mine * half, half)
    loads = [
        pltpu.make_async_copy(x_in, xf.at[:, own_half], load_sem.at[0]),
        pltpu.make_async_copy(q_in, qs, load_sem.at[1]),
        pltpu.make_async_copy(k_in, ks, load_sem.at[2]),
        pltpu.make_async_copy(v_in, vw, load_sem.at[3]),
        pltpu.make_async_copy(t_in, tg, load_sem.at[4]),
        pltpu.make_async_copy(o_in, ow, load_sem.at[5]),
    ]
    for load in loads:
        load.start()

    barrier = pltpu.get_barrier_semaphore()
    for step in range(1, count):
        pl.semaphore_signal(
            barrier, inc=1, device_id={"task": lax.rem(me + step, count)}, device_id_type=MESH
        )
    pl.semaphore_signal(barrier, inc=1, device_id=pair, device_id_type=MESH)
    pl.semaphore_wait(barrier, count)

    def remote(src, dst, send, got, peer):
        return pltpu.make_async_remote_copy(
            src_ref=src, dst_ref=dst, send_sem=send, recv_sem=got, device_id=peer, device_id_type=MESH
        )

    def x_copy(k, owner):
        part = xf.at[:, lanes(owner * half + k * cut, cut)]
        return remote(part, part, x_sem.at[near], x_sem.at[k], pair)

    loads[0].wait()
    for k in range(near):
        x_copy(k, mine).start()

    def a2a_copy(number, src, dst, rows, step):
        peer = lax.rem(me + step, count)
        return remote(
            src.at[rows, lanes(peer * piece, piece)],
            dst.at[me, rows],
            a2a_send.at[number],
            a2a_got.at[number],
            {"task": peer},
        )

    def a2a_start(number, src, dst, rows, first=1, last=count):
        def one(step, carry):
            a2a_copy(number, src, dst, rows, step).start()
            return carry
        lax.fori_loop(first, last, one, 0)

    def a2a_wait(number, dst, rows):
        arrived = dst.at[pl.ds(0, count - 1), rows]
        remote(arrived, arrived, a2a_send.at[number], a2a_got.at[number], {"task": lax.rem(me + 1, count)}).wait()

    all_rows = pl.ds(0, length)

    def x_spread(owner, first, last):
        def one(index, carry):
            step = lax.rem(owner * (count // 2) + index + count - me, count)
            @pl.when(step > 0)
            def _():
                a2a_copy(0, xf, x_cols, all_rows, step).start()
            return carry
        lax.fori_loop(first, last, one, 0)

    x_spread(mine, 0, count // 2)

    def gather_copy(number, array, slot, kind, source, got, peer):
        block = array.at[slot] if number < 3 else array.at[slot, pl.ds(high, length - high)]
        if number == 0:
            block = array.at[slot, pl.ds(0, high)]
        return remote(block, block, g_send.at[number, 0 if kind < 2 else 1], got, {"task": peer})

    up_peer, down_peer = me + 4, me - 4
    side_peer, core_peer = place(line, 1 - side, core), place(line, side, 1 - core)

    def pass_on(number, array, source):
        slot = place(source, side, core)
        @pl.when(jnp.logical_and(source <= line, line < lines - 1))
        def _():
            gather_copy(number, array, slot, 0, source, g_line.at[number, source], up_peer).start()
        @pl.when(jnp.logical_and(source >= line, line > 0))
        def _():
            gather_copy(number, array, slot, 1, source, g_line.at[number, source], down_peer).start()
        gather_copy(number, array, slot, 2, source, g_side.at[number, source], side_peer).start()
        gather_copy(number, array, slot, 3, source, g_core.at[number, source, 0], core_peer).start()

    def gather_start(number, array):
        pass_on(number, array, line)

    def at_distance(away, take):
        if away == 0:
            take(line)
            return
        @pl.when(line >= away)
        def _():
            take(line - away)
        @pl.when(line + away < lines)
        def _():
            take(line + away)

    def gather_line(number, array, away):
        def take(source):
            slot = place(source, side, core)
            gather_copy(number, array, slot, 2, source, g_line.at[number, source], side_peer).wait_recv()
            pass_on(number, array, source)
        at_distance(away, take)

    def gather_side(number, array, away):
        def take(source):
            slot = place(source, 1 - side, core)
            gather_copy(number, array, slot, 4, source, g_side.at[number, source], core_peer).wait_recv()
            gather_copy(number, array, slot, 4, source, g_core.at[number, source, 1], core_peer).start()
        at_distance(away, take)

    def gather_sides(number, array):
        for away in range(lines):
            gather_side(number, array, away)

    def gather_core(number, array, source, over):
        slot = place(source, side if over == 0 else 1 - side, 1 - core)
        gather_copy(number, array, slot, 3, source, g_core.at[number, source, over], core_peer).wait_recv()

    def gather_finish(number, array):
        for source in range(lines):
            for over in range(2):
                gather_core(number, array, source, over)

    def gather_sent(number, array):
        def sent(blocks, which):
            rows = (pl.ds(0, high), all_rows, all_rows, pl.ds(high, length - high))[number]
            if number == 1:
                rows = pl.ds(0, high)
            group = array.at[pl.ds(0, blocks), rows]
            remote(group, group, g_send.at[number, which], g_core.at[number, 0, 0], {"task": core_peer}).wait_send()
        for at in range(lines):
            ups = at + 1 if at < lines - 1 else 0
            downs = lines - at if at > 0 else 0
            @pl.when(line == at)
            def _():
                sent(ups + downs, 0)
        sent(3 * lines, 1)

    def head(h):
        return slice(h * HD, (h + 1) * HD)

    row = lax.broadcasted_iota(jnp.int32, (length, length), 0)
    col = lax.broadcasted_iota(jnp.int32, (length, length), 1)
    causal = row >= col
    loads[1].wait()
    loads[2].wait()
    root = jnp.sqrt(F32(HD))
    for h in range(heads):
        scores = dot_of(qs[:, head(h)], ks[:, head(h)], ((1,), (1,))) / root
        scores = jnp.where(causal, scores, F32(-1e30))
        scores = scores - jnp.max(scores, axis=-1, keepdims=True)
        expo = jnp.exp(scores)
        prob = expo / jnp.sum(expo, axis=-1, keepdims=True)
        probs[:, head(h)] = prob.astype(BF)
        probs_t[:, head(h)] = prob.T.astype(BF)

    err_1[high:, :] = jnp.zeros((length - high, depth), BF)
    err_2[:low, :] = jnp.zeros((low, depth), BF)
    err_3[high:, :] = jnp.zeros((length - high, depth), BF)
    position = lax.broadcasted_iota(jnp.int32, (length, 1), 0)
    split = jnp.full((length, 1), split_ref[0], jnp.int32)
    is_support = position < split
    support = is_support.astype(F32)
    count_s = split.astype(F32)
    weight_s = support / count_s
    weight_q = (1.0 - support) / (F32(length) - count_s)

    loads[3].wait()

    def take(k, owner, first):
        at = lanes(owner * half + k * cut, cut)
        x_part = xf[:, at]
        new = dot_of(x_part, vw[pl.ds(pl.multiple_of(owner * half + k * cut, 128), cut), :], ((1,), (0,)))
        gram = dot_of(x_part, x_part, ((1,), (1,)))
        if first:
            acc[...] = new
            half_acc[...] = gram
        else:
            acc[...] += new
            half_acc[...] += gram

    take(0, mine, True)
    def own_take(k, carry):
        take(k, mine, False)
        return carry
    lax.fori_loop(1, near, own_take, 0)
    def other_take(k, carry):
        x_copy(k, 1 - mine).wait_recv()
        x_spread(1 - mine, 2 * k, 2 * k + 2)
        take(k, 1 - mine, False)
        return carry
    lax.fori_loop(0, near, other_take, 0)

    gram_raw = half_acc[...]
    diagonal = jnp.where(row == col, gram_raw, F32(0.0))
    scale_row = lax.rsqrt(jnp.sum(diagonal, axis=1, keepdims=True) / F32(depth) + 1e-05)
    scale_col = lax.rsqrt(jnp.sum(diagonal, axis=0, keepdims=True) / F32(depth) + 1e-05)
    gram_b[...] = (gram_raw * scale_row * scale_col).astype(BF)
    upper[...] = (acc[...] * scale_row).astype(BF)

    a_mine = a_all.at[me]
    for h in range(heads):
        mixed = dot_of(probs[:, head(h)], upper[:, head(h)], ((1,), (0,)))
        z_mine[:, head(h)] = mixed[:high].astype(BF)
    a_mine[:high, :] = (weight_s[:high] * z_mine[...].astype(F32)).astype(BF)
    gather_start(0, a_all)
    loads[4].wait()
    loads[5].wait()

    def part_copy(number, send, got, k, owner):
        at = lanes(lax.rem(owner * near + k, chunks) * cut, cut)
        return remote(send.at[:, at], got.at[:, at], part_sem.at[number], part_got.at[number, k], pair)

    def own_columns(k):
        return lanes(lax.rem(mine * near + k, chunks) * cut, cut)

    def other_columns(k):
        return lanes(lax.rem((1 - mine) * near + k, chunks) * cut, cut)

    def offset(k, rows):
        there = lanes(k * cut, cut)
        return xf[rows, own_columns(k)].astype(F32) - tg[rows, there].astype(F32)

    def send_parts(number, value, rows, send, got, with_offset):
        def one(k, near_half):
            at = own_columns(k)
            part = value(at)
            if near_half and with_offset:
                part = part + offset(k, rows)
            send[:, at] = part.astype(BF)
            part_copy(number, send, got, k, mine).start()
        def first(k, carry):
            one(k, True)
            return carry
        def later(k, carry):
            one(k, False)
            return carry
        lax.fori_loop(0, near, first, 0)
        lax.fori_loop(near, chunks, later, 0)

    def take_parts(number, send, got, rows, weight, error, also, first=0, last=chunks):
        def one(k, carry):
            at = other_columns(k)
            part_copy(number, send, got, k, 1 - mine).wait_recv()
            total = send[:, at].astype(F32) + got[:, at].astype(F32)
            error[rows, at] = (weight[rows] * total).astype(BF)
            part = error[:, at]
            acc[...] += dot_of(part, ow[:, at], ((1,), (1,)))
            also(at, part)
            return carry
        lax.fori_loop(first, last, one, 0)

    support_rows, query_rows = slice(0, high), slice(low, length)
    nothing = lambda at, part: None

    def value_0(at):
        return dot_of(z_mine[...], ow[:, at], ((1,), (0,)))

    early_rows, middle_rows, late_rows = pl.ds(0, low), pl.ds(low, high - low), pl.ds(high, length - high)
    acc[...] = jnp.zeros_like(acc)
    send_parts(0, value_0, support_rows, part_0, got_0, True)
    take_parts(0, part_0, got_0, support_rows, weight_s, err_1, nothing, 0, 6)
    gather_line(0, a_all, 1)
    take_parts(0, part_0, got_0, support_rows, weight_s, err_1, nothing, 6, chunks)
    a2a_start(1, err_1, both_cols, early_rows)

    back[...] = acc[...].astype(BF)
    for h in range(heads):
        up = dot_of(probs_t[:, head(h)], back[:, head(h)], ((1,), (0,))).astype(BF)
        new = (upper[:, head(h)].astype(F32) - step_rate * dot_of(gram_b[...], up, ((1,), (0,)))).astype(BF)
        mixq[:, head(h)] = dot_of(probs[:, head(h)], new, ((1,), (0,))).astype(BF)
    cross[:, high:] = jnp.zeros((length, length - high), BF)
    product = -step_rate * dot_of(mixq[...], z_mine[...], ((1,), (1,)))
    cross[:, :high] = jnp.where(is_support, F32(0.0), product).astype(BF)
    cross_copy = remote(cross, cross_got, cross_sem.at[0], cross_sem.at[1], pair)
    cross_copy.start()

    def value_1(at):
        part = dot_of(mixq[...], ow[:, at], ((1,), (0,))) + dot_of(cross[:, :high], err_1[:high, at], ((1,), (0,)))
        return part[low:]

    half_acc[...] = jnp.zeros_like(half_acc)
    acc[...] = jnp.zeros_like(acc)

    def pairs_of(at, part):
        half_acc[...] += dot_of(part, err_1[:, at], ((1,), (1,)))

    send_parts(1, value_1, query_rows, part_1, got_1, True)
    gather_line(0, a_all, 2)
    cross_copy.wait_recv()
    cross_sum = (cross[...].astype(F32) + cross_got[...].astype(F32)).astype(BF)
    left[...] = (mixq[...].astype(F32) + dot_of(cross_sum[:, :high], a_mine[:high], ((1,), (0,)))).astype(BF)
    a_mine[high:, :] = left[high:, :]
    gather_start(3, a_all)
    take_parts(1, part_1, got_1, query_rows, weight_q, err_2, pairs_of, 0, 3)
    for away in range(3, lines):
        gather_line(0, a_all, away)
    take_parts(1, part_1, got_1, query_rows, weight_q, err_2, pairs_of, 3, 5)
    gather_line(3, a_all, 1)
    take_parts(1, part_1, got_1, query_rows, weight_q, err_2, pairs_of, 5, 7)
    gather_sides(0, a_all)
    take_parts(1, part_1, got_1, query_rows, weight_q, err_2, pairs_of, 7, chunks)
    gather_line(3, a_all, 2)

    pairs[...] = (-step_rate * half_acc[...]).astype(BF)
    back[...] = (acc[...] + dot_of(pairs[:, :high], z_mine[...], ((1,), (0,)))).astype(BF)
    left_mine = left_all.at[me]
    for h in range(heads):
        up = dot_of(probs_t[:, head(h)], back[:, head(h)], ((1,), (0,)))
        value_now[:, head(h)] = up
        flow = (-step_rate * dot_of(gram_b[...], up.astype(BF), ((1,), (0,)))).astype(BF)
        again = dot_of(probs[:, head(h)], flow, ((1,), (0,))).astype(BF)
        second[:, head(h)] = again
        left_mine[:, head(h)] = jnp.where(is_support, again, left[:, head(h)])[:high]

    def value_2(at):
        part = dot_of(second[...], ow[:, at], ((1,), (0,))) + dot_of(cross[...], err_2[:, at], ((0,), (0,)))
        return part[:high]

    acc[...] = jnp.zeros_like(acc)
    gather_start(1, left_all)
    send_parts(2, value_2, support_rows, part_2, got_2, False)

    def join(k, carry):
        at = own_columns(k)
        both[:, at] = jnp.where(is_support, err_1[:, at], err_2[:, at])
        return carry
    lax.fori_loop(0, chunks, join, 0)
    def both_start(first, last):
        a2a_start(2, both, both_cols, middle_rows, first, last)
        a2a_start(3, both, right_a, late_rows, first, last)

    both_start(1, 5)
    take_parts(2, part_2, got_2, support_rows, weight_s, err_3, nothing, 0, 1)
    for away in range(3, lines):
        gather_line(3, a_all, away)
    take_parts(2, part_2, got_2, support_rows, weight_s, err_3, nothing, 1, 2)
    gather_line(1, left_all, 1)
    both_start(5, 10)
    take_parts(2, part_2, got_2, support_rows, weight_s, err_3, nothing, 2, 4)
    gather_sides(3, a_all)
    take_parts(2, part_2, got_2, support_rows, weight_s, err_3, nothing, 4, 6)
    gather_line(1, left_all, 2)
    both_start(10, count)
    take_parts(2, part_2, got_2, support_rows, weight_s, err_3, nothing, 6, chunks)

    back[...] = (acc[...] + dot_of(pairs[...], mixq[...], ((0,), (0,)))).astype(BF)
    rows_mine = rows_all.at[me]
    for h in range(heads):
        late = dot_of(probs_t[:, head(h)], back[:, head(h)], ((1,), (0,)))
        rows_mine[:, head(h)] = ((value_now[:, head(h)] + late) * scale_row).astype(BF)
    gather_start(2, rows_all)
    for away in range(3, lines):
        gather_line(1, left_all, away)
    gather_side(1, left_all, 0)
    gather_side(1, left_all, 1)

    x_cols[me] = xf[:, lanes(me * piece, piece)]
    both_cols[me] = both[:high, lanes(me * piece, piece)]
    right_a[me, late_rows] = both[high:, lanes(me * piece, piece)]

    def swap_copy(slot):
        return remote(swap.at[slot], swap_got.at[slot], swap_sem.at[count], swap_sem.at[slot], pair)

    def swap_one(slot):
        swap[slot] = dot_of(left_all[slot], ow[:, lanes(me * piece, piece)], ((1,), (0,))).astype(BF)
        swap_copy(slot).start()

    def swap_line(side_at, core_at):
        def one(source, carry):
            swap_one(place(source, side_at, core_at))
            return carry
        lax.fori_loop(0, lines, one, 0)

    swap_line(side, core)
    gather_side(1, left_all, 2)
    for away in range(3, lines):
        gather_side(1, left_all, away)
    gather_line(2, rows_all, 1)
    swap_line(1 - side, core)
    gather_finish(1, left_all)
    swap_line(side, 1 - core)
    swap_line(1 - side, 1 - core)
    gather_line(2, rows_all, 2)
    a2a_wait(0, x_cols, all_rows)
    a2a_wait(1, both_cols, early_rows)
    a2a_wait(2, both_cols, middle_rows)

    tile = 256

    def early(i, carry):
        at = lanes(i * tile, tile)
        do_ref[at, :] = dot_of(
            left_all[:, :, at].reshape(count * high, tile), both_cols[...].reshape(count * high, piece), ((0,), (0,))
        )
        return carry
    lax.fori_loop(0, width // tile, early, 0)
    for away in range(3, lines):
        gather_line(2, rows_all, away)
    a2a_wait(3, right_a, late_rows)
    gather_finish(0, a_all)
    gather_finish(3, a_all)

    def add_pair(source, side_at):
        both_cores = pl.ds(place(source, side_at, 0), 2)
        return dot_of(
            x_cols[both_cores].reshape(2 * length, piece), rows_all[both_cores].reshape(2 * length, width), ((0,), (0,))
        )

    gather_core(2, rows_all, line, 0)
    dv_ref[...] = add_pair(line, side)

    def column(source):
        gather_core(2, rows_all, source, 0)
        dv_ref[...] += add_pair(source, side)

    def across(source):
        gather_core(2, rows_all, source, 1)
        dv_ref[...] += add_pair(source, 1 - side)

    gather_side(2, rows_all, 0)
    for away in range(1, lines):
        at_distance(away, column)
    gather_side(2, rows_all, 1)
    at_distance(0, across)

    def swapped(slot, carry):
        swap_copy(slot).wait_recv()
        right_a[slot, :high] = (swap[slot].astype(F32) + swap_got[slot].astype(F32)).astype(BF)
        return carry
    lax.fori_loop(0, count, swapped, 0)

    def late_part(i, carry):
        at = lanes(i * tile, tile)
        do_ref[at, :] += dot_of(
            a_all[:, :, at].reshape(count * length, tile), right_a[...].reshape(count * length, piece), ((0,), (0,))
        )
        return carry
    lax.fori_loop(0, width // tile, late_part, 0)
    at_distance(1, across)
    gather_side(2, rows_all, 2)
    at_distance(2, across)
    for away in range(3, lines):
        gather_side(2, rows_all, away)
        at_distance(away, across)

    cross_copy.wait_send()
    remote(tg, tg, x_sem.at[near], x_sem.at[0], pair).wait_send()
    for number, (send, got) in enumerate(((part_0, got_0), (part_1, got_1), (part_2, got_2))):
        remote(send, got, part_sem.at[number], part_got.at[number, 0], pair).wait_send()
    remote(swap, swap_got, swap_sem.at[count], swap_sem.at[0], pair).wait_send()
    for number, array in enumerate((a_all, left_all, rows_all, a_all)):
        gather_sent(number, array)


def one_kernel(inputs, targets, queries, key_rows, value_weight, output_weight, splits):
    count = lax.axis_size("task")
    lines = count // 4
    length, half = inputs.shape
    depth = 2 * half
    width = queries.shape[1]
    high = 3 * length // 4
    piece = depth // count
    vm = pltpu.VMEM
    dma = pltpu.SemaphoreType.DMA
    anywhere = pl.BlockSpec(memory_space=pl.ANY)
    chunks = 8
    return pl.pallas_call(
        functools.partial(step_kernel, lines),
        out_shape=(
            pltpu.VMEM((piece, width), F32),
            pltpu.VMEM((width, piece), F32),
        ),
        in_specs=[anywhere] * 6 + [pl.BlockSpec(memory_space=pltpu.SMEM)],
        out_specs=(pl.BlockSpec(memory_space=pltpu.VMEM), pl.BlockSpec(memory_space=pltpu.VMEM)),
        scratch_shapes=[
            vm((length, depth), BF),
            vm((length, half), BF),
            vm((length, width), BF),
            vm((length, width), BF),
            vm((depth, width), BF),
            vm((width, depth), BF),
        ]
        + [vm((length, width), BF)] * 6
        + [vm((length, width), F32), vm((length, length), F32)]
        + [vm((high, depth), BF)] * 6
        + [vm((length, depth), BF)] * 4
        + [vm((length, width), BF)]
        + [vm((length, length), BF)] * 4
        + [
            vm((length, width), F32),
            vm((high, width), BF),
            vm((count, length, width), BF),
            vm((count, high, width), BF),
            vm((count, length, width), BF),
            vm((count, length, piece), BF),
            vm((count, high, piece), BF),
            vm((count, length, piece), BF),
            vm((count, high, piece), BF),
            vm((count, high, piece), BF),
            dma((6,)),
            dma((chunks // 2 + 1,)),
            dma((3,)),
            dma((3, chunks)),
            dma((2,)),
            dma((count + 1,)),
            dma((4,)),
            dma((4,)),
            dma((4, 2)),
            dma((4, lines)),
            dma((4, lines)),
            dma((4, lines, 2)),
        ],
        compiler_params=pltpu.CompilerParams(
            collective_id=1, has_side_effects=True, vmem_limit_bytes=60 * 2**20
        ),
    )(inputs, targets, queries, key_rows, value_weight, output_weight, splits)


def make_device(tensor_count):
    def per_device(inputs, targets, queries, key_rows, value_weight, output_weight, splits):
        length = inputs.shape[0]
        low, high = length // 4, 3 * length // 4
        heads = queries.shape[1] // HD
        index = lax.axis_index("tensor")
        normed = normed_rows(full_rows(inputs, tensor_count, index))
        offset_here = inputs.astype(F32) - targets.astype(F32)
        offset = jnp.concatenate(
            [jnp.where(index == block, offset_here, F32(0.0)) for block in range(tensor_count)],
            axis=1,
        )
        probs = attention_probs(queries, key_rows, heads)
        probs_s = probs[:, :high, :high]
        probs_q = probs[:, low:, :]
        split = splits[0]
        count_s = split.astype(F32)
        position = jnp.arange(length)
        support = (position < split).astype(F32)[:, None]
        weight_s = (support / count_s)[:high]
        weight_q = ((1.0 - support) / (F32(length) - count_s))[low:]

        upper = mm(normed, value_weight).astype(BF)
        mixed_s = mix(probs_s, upper[:high]).astype(BF)
        gram = mm_nt(normed, normed).astype(BF)
        mixed_s_all = gather_tokens(mixed_s)
        part_0 = (mm(mixed_s, output_weight) + offset[:high]).astype(BF)
        part_0, normed_sent = lax.optimization_barrier((part_0, normed))
        normed_cols = my_columns(normed_sent)
        error_1 = (weight_s * group_sum(part_0, tensor_count)).astype(BF)

        back_u = mix_back(probs_s, mm_nt(error_1, output_weight).astype(BF)).astype(BF)
        upper_1 = (upper.astype(F32) - step_rate * mm(gram[:, :high], back_u)).astype(BF)
        mixed_q = mix(probs_q, upper_1).astype(BF)
        cross = (-step_rate * mm_nt(mixed_q, mixed_s)).astype(BF)
        part_1 = mm(mixed_q, output_weight) + mm(cross, error_1)
        part_1 = (part_1 + offset[low:]).astype(BF)
        error_2 = (weight_q * group_sum(part_1, tensor_count)).astype(BF)

        errors = (-step_rate * mm_nt(error_2, error_1)).astype(BF)
        back_z1 = (mm_nt(error_2, output_weight) + mm(errors, mixed_s)).astype(BF)
        back_u1 = mix_back(probs_q, back_z1)
        back_u1_b = back_u1.astype(BF)
        back_gram = (-step_rate * mm(gram[:high], back_u1_b)).astype(BF)
        second = mix(probs_s, back_gram).astype(BF)
        error_back = (mm(second, output_weight) + mm_tn(cross, error_2)).astype(BF)
        is_support = (position < split)[:, None]
        left = jnp.where(is_support, below(second, length), above(mixed_q, length))
        errors_both = jnp.where(is_support, below(error_1, length), above(error_2, length))
        error_back, normed_cols, errors_both, left = lax.optimization_barrier(
            (error_back, normed_cols, errors_both, left)
        )
        both_cols = my_columns(errors_both)
        left, mixed_s_all = lax.optimization_barrier((left, mixed_s_all))
        left_all = gather_tokens(left)
        error_sum = group_sum(error_back, tensor_count)
        error_3 = (weight_s * error_sum).astype(BF)
        error_3_cols = my_columns(error_3)

        back_z0 = (mm_nt(error_3, output_weight) + mm_tn(errors, mixed_q)).astype(BF)
        late = mix_back(probs_s, back_z0)
        value_rows = (back_u1 + jnp.pad(late, ((0, length - high), (0, 0)))).astype(BF)
        value_rows_all = gather_by_copies(value_rows, 1)
        total_output = (
            mm_tn(left_all, both_cols)
            + mm_tn(mixed_s_all, error_3_cols)
        )
        total_value = mm_tn(normed_cols, value_rows_all)
        return (total_value, total_output)

    return per_device


def solution(mesh):
    whole_step = mesh.shape["tensor"] == 2 and mesh.shape["task"] % 4 == 0
    return jax.shard_map(
        one_kernel if whole_step else make_device(mesh.shape["tensor"]),
        mesh=mesh,
        in_specs=(
            P("task", "tensor"),
            P("task", "tensor"),
            P("task", "tensor"),
            P("task", "tensor"),
            P(None, "tensor"),
            P("tensor", None),
            P("task"),
        ),
        out_specs=(P("task", "tensor"), P("tensor", "task")),
        check_vma=False,
    )
```

```python
import functools

import jax
import jax.numpy as jnp
from jax import lax
from jax.experimental import pallas as pl
from jax.experimental.pallas import tpu as pltpu
from jax.sharding import PartitionSpec as P

HD = 128
BF = jnp.bfloat16
F32 = jnp.float32

step_rate = 0.25


def normed_rows(inputs):
    values = inputs.astype(F32)
    scale = lax.rsqrt(jnp.mean(values * values, axis=-1, keepdims=True) + 1e-05)
    return (values * scale).astype(BF)


def attention_probs(queries, key_rows, heads):
    length = queries.shape[0]
    query_h = queries.reshape(length, heads, -1)
    key_h = key_rows.reshape(length, heads, -1)
    scores = jnp.einsum("ihd,jhd->hij", query_h, key_h, preferred_element_type=F32)
    scores = scores / jnp.sqrt(F32(query_h.shape[2]))
    position = jnp.arange(length)
    causal = position[:, None] >= position[None, :]
    scores = jnp.where(causal[None], scores, F32(-1e30))
    scores = scores - jnp.max(scores, axis=-1, keepdims=True)
    expo = jnp.exp(scores)
    return (expo / jnp.sum(expo, axis=-1, keepdims=True)).astype(BF)


def mm(left, right):
    return jnp.dot(left, right, preferred_element_type=F32)


def mm_nt(left, right):
    return lax.dot_general(left, right, (((1,), (1,)), ((), ())), preferred_element_type=F32)


def mm_tn(left, right):
    return lax.dot_general(left, right, (((0,), (0,)), ((), ())), preferred_element_type=F32)


def mix(probs, rows):
    heads = probs.shape[0]
    split = rows.reshape(rows.shape[0], heads, -1)
    out = jnp.einsum("hij,jhd->ihd", probs, split, preferred_element_type=F32)
    return out.reshape(out.shape[0], -1)


def mix_back(probs, rows):
    heads = probs.shape[0]
    split = rows.reshape(rows.shape[0], heads, -1)
    out = jnp.einsum("hij,ihd->jhd", probs, split, preferred_element_type=F32)
    return out.reshape(out.shape[0], -1)


def group_sum(term, count):
    term = term.astype(BF)
    if count == 1:
        return term.astype(F32)
    if count == 2:
        other = lax.ppermute(term, "tensor", ((0, 1), (1, 0)))
        return term.astype(F32) + other.astype(F32)
    share = lax.psum_scatter(term, "tensor", scatter_dimension=1, tiled=True)
    return lax.all_gather(share, "tensor", axis=1, tiled=True).astype(F32)


def full_rows(inputs, count, index):
    if count != 2:
        return lax.all_gather(inputs, "tensor", axis=1, tiled=True)
    other = lax.ppermute(inputs, "tensor", ((0, 1), (1, 0)))
    low = jnp.where(index == 0, inputs, other)
    high = jnp.where(index == 0, other, inputs)
    return jnp.concatenate([low, high], axis=1)


def gather_kernel(lines, src_ref, out_ref, own_sem, send_sem, line_sem, side_sem, core_sem):
    me = lax.axis_index("task")
    core, side, line = lax.rem(me, 2), lax.rem(me // 2, 2), me // 4

    def place(back, over_side, over_core):
        line_from = lax.rem(line + lines - back, lines)
        side_from = 1 - side if over_side else side
        core_from = 1 - core if over_core else core
        return (line_from * 2 + side_from) * 2 + core_from

    side_peer, core_peer = place(0, True, False), place(0, False, True)
    peers = [place(lines - step, False, False) for step in range(1, lines)] + [side_peer, core_peer]
    barrier = pltpu.get_barrier_semaphore()
    for peer in peers:
        pl.semaphore_signal(
            barrier, inc=1, device_id={"task": peer}, device_id_type=pl.DeviceIdType.MESH
        )
    pl.semaphore_wait(barrier, len(peers))

    started = []

    def send(source, slot, arrival, peer):
        copy = pltpu.make_async_remote_copy(
            src_ref=source,
            dst_ref=out_ref.at[slot],
            send_sem=send_sem.at[len(started)],
            recv_sem=arrival,
            device_id={"task": peer},
            device_id_type=pl.DeviceIdType.MESH,
        )
        copy.start()
        started.append(copy)

    def arrived(slot, arrival, peer):
        pltpu.make_async_remote_copy(
            src_ref=out_ref.at[slot],
            dst_ref=out_ref.at[slot],
            send_sem=send_sem.at[0],
            recv_sem=arrival,
            device_id={"task": peer},
            device_id_type=pl.DeviceIdType.MESH,
        ).wait_recv()

    for step in sorted(range(1, lines), key=lambda step: -min(step, lines - step)):
        send(src_ref, me, line_sem.at[step], peers[step - 1])
    send(src_ref, me, side_sem.at[0], side_peer)
    send(src_ref, me, core_sem.at[0, 0], core_peer)
    own = pltpu.make_async_copy(src_ref, out_ref.at[me], own_sem)
    own.start()
    order = sorted(range(1, lines), key=lambda step: min(step, lines - step))
    for step in order:
        slot = place(step, False, False)
        arrived(slot, line_sem.at[step], side_peer)
        send(out_ref.at[slot], slot, side_sem.at[step], side_peer)
        send(out_ref.at[slot], slot, core_sem.at[step, 0], core_peer)
    for step in [0] + order:
        slot = place(step, True, False)
        arrived(slot, side_sem.at[step], side_peer)
        send(out_ref.at[slot], slot, core_sem.at[step, 1], core_peer)
    for step in [0] + order:
        for over in range(2):
            arrived(place(step, over == 1, True), core_sem.at[step, over], core_peer)
    own.wait()
    for copy in started:
        copy.wait_send()


def gather_by_copies(rows, number):
    count = lax.axis_size("task")
    if count % 4:
        return gather_tokens(rows)
    lines = count // 4
    sends = (lines + 1) + 2 * (lines - 1) + lines
    gathered = pl.pallas_call(
        functools.partial(gather_kernel, lines),
        out_shape=jax.ShapeDtypeStruct((count,) + rows.shape, rows.dtype),
        in_specs=[pl.BlockSpec(memory_space=pltpu.VMEM)],
        out_specs=pl.BlockSpec(memory_space=pltpu.VMEM),
        scratch_shapes=[
            pltpu.SemaphoreType.DMA,
            pltpu.SemaphoreType.DMA((sends,)),
            pltpu.SemaphoreType.DMA((lines,)),
            pltpu.SemaphoreType.DMA((lines,)),
            pltpu.SemaphoreType.DMA((lines, 2)),
        ],
        compiler_params=pltpu.CompilerParams(collective_id=number, has_side_effects=True),
        cost_estimate=pl.CostEstimate(
            flops=0, bytes_accessed=16 * rows.size * rows.dtype.itemsize * count, transcendentals=0
        ),
    )(rows)
    return gathered.reshape(count * rows.shape[0], rows.shape[1])


def gather_tokens(rows):
    return lax.all_gather(rows, "task", axis=0, tiled=True)


def my_columns(rows):
    return lax.all_to_all(rows, "task", split_axis=1, concat_axis=0, tiled=True)


def below(rows, length):
    return jnp.pad(rows, ((0, length - rows.shape[0]), (0, 0)))


def above(rows, length):
    return jnp.pad(rows, ((length - rows.shape[0], 0), (0, 0)))


MESH = pl.DeviceIdType.MESH


def dot_of(left, right, dims):
    return lax.dot_general(left, right, (dims, ((), ())), preferred_element_type=F32)


def step_kernel(
    lines,
    x_in, t_in, q_in, k_in, v_in, o_in, split_ref,
    dv_ref, do_ref,
    xf, tg, qs, ks, vw, ow, probs, probs_t, upper, mixq, second, left, acc, half_acc,
    part_0, part_1, part_2, got_0, got_1, got_2, err_1, err_2, err_3, both,
    back, gram_b, cross, cross_got, pairs, value_now, z_mine, a_all, left_all, rows_all,
    x_cols, both_cols, right_a, swap, swap_got,
    load_sem, x_sem, part_sem, part_got, cross_sem, swap_sem,
    a2a_send, a2a_got, g_send, g_line, g_side, g_core,
):
    count = lines * 4
    length, depth = xf.shape
    half = depth // 2
    width = upper.shape[1]
    heads = width // HD
    low, high = length // 4, 3 * length // 4
    piece = depth // count
    chunks = 8
    cut = depth // chunks
    near = chunks // 2

    me = lax.axis_index("task")
    mine = lax.axis_index("tensor")
    core, side, line = lax.rem(me, 2), lax.rem(me // 2, 2), me // 4
    pair = {"tensor": 1 - mine}

    def place(line_at, side_at, core_at):
        return (line_at * 2 + side_at) * 2 + core_at

    def lanes(start, size):
        return pl.ds(pl.multiple_of(start, 128), size)

    own_half = lanes(mine * half, half)
    loads = [
        pltpu.make_async_copy(x_in, xf.at[:, own_half], load_sem.at[0]),
        pltpu.make_async_copy(q_in, qs, load_sem.at[1]),
        pltpu.make_async_copy(k_in, ks, load_sem.at[2]),
        pltpu.make_async_copy(v_in, vw, load_sem.at[3]),
        pltpu.make_async_copy(t_in, tg, load_sem.at[4]),
        pltpu.make_async_copy(o_in, ow, load_sem.at[5]),
    ]
    for load in loads:
        load.start()

    barrier = pltpu.get_barrier_semaphore()
    for step in range(1, count):
        pl.semaphore_signal(
            barrier, inc=1, device_id={"task": lax.rem(me + step, count)}, device_id_type=MESH
        )
    pl.semaphore_signal(barrier, inc=1, device_id=pair, device_id_type=MESH)
    pl.semaphore_wait(barrier, count)

    def remote(src, dst, send, got, peer):
        return pltpu.make_async_remote_copy(
            src_ref=src, dst_ref=dst, send_sem=send, recv_sem=got, device_id=peer, device_id_type=MESH
        )

    def x_copy(k, owner):
        part = xf.at[:, lanes(owner * half + k * cut, cut)]
        return remote(part, part, x_sem.at[near], x_sem.at[k], pair)

    loads[0].wait()
    for k in range(near):
        x_copy(k, mine).start()

    def a2a_copy(number, src, dst, rows, step):
        peer = lax.rem(me + step, count)
        return remote(
            src.at[rows, lanes(peer * piece, piece)],
            dst.at[me, rows],
            a2a_send.at[number],
            a2a_got.at[number],
            {"task": peer},
        )

    def a2a_start(number, src, dst, rows, first=1, last=count):
        def one(step, carry):
            a2a_copy(number, src, dst, rows, step).start()
            return carry
        lax.fori_loop(first, last, one, 0)

    def a2a_wait(number, dst, rows):
        arrived = dst.at[pl.ds(0, count - 1), rows]
        remote(arrived, arrived, a2a_send.at[number], a2a_got.at[number], {"task": lax.rem(me + 1, count)}).wait()

    all_rows = pl.ds(0, length)

    def x_spread(owner, first, last):
        def one(index, carry):
            step = lax.rem(owner * (count // 2) + index + count - me, count)
            @pl.when(step > 0)
            def _():
                a2a_copy(0, xf, x_cols, all_rows, step).start()
            return carry
        lax.fori_loop(first, last, one, 0)

    x_spread(mine, 0, count // 2)

    part_rows = (pl.ds(0, high), pl.ds(0, high), all_rows, pl.ds(high, length - high), all_rows)
    part_lanes = (pl.ds(0, width),) * 2 + (pl.ds(0, width // 2), pl.ds(0, width), pl.ds(width // 2, width // 2))

    def gather_copy(number, array, slot, kind, source, got, peer):
        block = array.at[slot, part_rows[number], part_lanes[number]]
        return remote(block, block, g_send.at[number, 0 if kind < 2 else 1], got, {"task": peer})

    def from_end(number, source, away):
        if number in (1, 4) and lines > 2 and away == 2:
            return jnp.logical_or(source == 0, source == lines - 1)
        return None

    def detour(number, away):
        return number == 2 and lines > 2 and away == lines - 1

    up_peer, down_peer = me + 4, me - 4
    side_peer, core_peer = place(line, 1 - side, core), place(line, side, 1 - core)

    def pass_on(number, array, source, away):
        slot = place(source, side, core)
        @pl.when(jnp.logical_and(source <= line, line < lines - 1))
        def _():
            gather_copy(number, array, slot, 0, source, g_line.at[number, source], up_peer).start()
        @pl.when(jnp.logical_and(source >= line, line > 0))
        def _():
            gather_copy(number, array, slot, 1, source, g_line.at[number, source], down_peer).start()
        if not detour(number, away):
            through = from_end(number, source, away)
            @pl.when(True if through is None else jnp.logical_not(through))
            def _():
                gather_copy(number, array, slot, 2, source, g_side.at[number, source], side_peer).start()
        gather_copy(number, array, slot, 3, source, g_core.at[number, source, 0], core_peer).start()

    def gather_start(number, array):
        pass_on(number, array, line, 0)

    def at_distance(away, take):
        if away == 0:
            take(line)
            return
        @pl.when(line >= away)
        def _():
            take(line - away)
        @pl.when(line + away < lines)
        def _():
            take(line + away)

    def gather_line(number, array, away):
        def take(source):
            slot = place(source, side, core)
            gather_copy(number, array, slot, 2, source, g_line.at[number, source], side_peer).wait_recv()
            pass_on(number, array, source, away)
        at_distance(away, take)

    def gather_side(number, array, away):
        def take(source):
            slot = place(source, 1 - side, core)
            gather_copy(number, array, slot, 4, source, g_side.at[number, source], core_peer).wait_recv()
            gather_copy(number, array, slot, 4, source, g_core.at[number, source, 1], core_peer).start()
            through = from_end(number, source, away + 1)
            if detour(number, away + 1) or through is not None:
                through = True if through is None else through
                @pl.when(functools.reduce(jnp.logical_and, (source < line, line < lines - 1, through)))
                def _():
                    gather_copy(number, array, slot, 4, source, g_side.at[number, source], up_peer).start()
                @pl.when(functools.reduce(jnp.logical_and, (source > line, line > 0, through)))
                def _():
                    gather_copy(number, array, slot, 4, source, g_side.at[number, source], down_peer).start()
        at_distance(away, take)

    def gather_sides(number, array):
        for away in range(lines):
            gather_side(number, array, away)

    def gather_core(number, array, source, over):
        slot = place(source, side if over == 0 else 1 - side, 1 - core)
        gather_copy(number, array, slot, 3, source, g_core.at[number, source, over], core_peer).wait_recv()

    def gather_finish(number, array):
        for source in range(lines):
            for over in range(2):
                gather_core(number, array, source, over)

    def gather_sent(number, array):
        def sent(blocks, which):
            group = array.at[pl.ds(0, blocks), part_rows[number], part_lanes[number]]
            remote(group, group, g_send.at[number, which], g_core.at[number, 0, 0], {"task": core_peer}).wait_send()
        for at in range(lines):
            ups = at + 1 if at < lines - 1 else 0
            downs = lines - at if at > 0 else 0
            others = 3 * lines
            if detour(number, lines - 1):
                ends = (at == 0) + (at == lines - 1)
                inner = (at == lines - 2) + (at == 1)
                others += inner - ends
            if number in (1, 4) and lines > 2:
                others += (at == 1) + (at == lines - 2) - (at == 2) - (at == lines - 3)
            @pl.when(line == at)
            def _():
                sent(ups + downs, 0)
                sent(others, 1)

    def head(h):
        return slice(h * HD, (h + 1) * HD)

    row = lax.broadcasted_iota(jnp.int32, (length, length), 0)
    col = lax.broadcasted_iota(jnp.int32, (length, length), 1)
    causal = row >= col
    loads[1].wait()
    loads[2].wait()
    root = jnp.sqrt(F32(HD))
    for h in range(heads):
        scores = dot_of(qs[:, head(h)], ks[:, head(h)], ((1,), (1,))) / root
        scores = jnp.where(causal, scores, F32(-1e30))
        scores = scores - jnp.max(scores, axis=-1, keepdims=True)
        expo = jnp.exp(scores)
        prob = expo / jnp.sum(expo, axis=-1, keepdims=True)
        probs[:, head(h)] = prob.astype(BF)
        probs_t[:, head(h)] = prob.T.astype(BF)

    err_1[high:, :] = jnp.zeros((length - high, depth), BF)
    err_2[:low, :] = jnp.zeros((low, depth), BF)
    err_3[high:, :] = jnp.zeros((length - high, depth), BF)
    position = lax.broadcasted_iota(jnp.int32, (length, 1), 0)
    split = jnp.full((length, 1), split_ref[0], jnp.int32)
    is_support = position < split
    support = is_support.astype(F32)
    count_s = split.astype(F32)
    weight_s = support / count_s
    weight_q = (1.0 - support) / (F32(length) - count_s)

    loads[3].wait()

    def take(k, owner, first):
        at = lanes(owner * half + k * cut, cut)
        x_part = xf[:, at]
        new = dot_of(x_part, vw[pl.ds(pl.multiple_of(owner * half + k * cut, 128), cut), :], ((1,), (0,)))
        gram = dot_of(x_part, x_part, ((1,), (1,)))
        if first:
            acc[...] = new
            half_acc[...] = gram
        else:
            acc[...] += new
            half_acc[...] += gram

    take(0, mine, True)
    def own_take(k, carry):
        take(k, mine, False)
        return carry
    lax.fori_loop(1, near, own_take, 0)
    def other_take(k, carry):
        x_copy(k, 1 - mine).wait_recv()
        x_spread(1 - mine, 2 * k, 2 * k + 2)
        take(k, 1 - mine, False)
        return carry
    lax.fori_loop(0, near, other_take, 0)

    gram_raw = half_acc[...]
    diagonal = jnp.where(row == col, gram_raw, F32(0.0))
    scale_row = lax.rsqrt(jnp.sum(diagonal, axis=1, keepdims=True) / F32(depth) + 1e-05)
    scale_col = lax.rsqrt(jnp.sum(diagonal, axis=0, keepdims=True) / F32(depth) + 1e-05)
    gram_b[...] = (gram_raw * scale_row * scale_col).astype(BF)
    upper[...] = (acc[...] * scale_row).astype(BF)

    a_mine = a_all.at[me]
    for h in range(heads):
        mixed = dot_of(probs[:, head(h)], upper[:, head(h)], ((1,), (0,)))
        z_mine[:, head(h)] = mixed[:high].astype(BF)
    a_mine[:high, :] = (weight_s[:high] * z_mine[...].astype(F32)).astype(BF)
    gather_start(0, a_all)
    loads[4].wait()
    loads[5].wait()

    def part_copy(number, send, got, k, owner):
        at = lanes(lax.rem(owner * near + k, chunks) * cut, cut)
        return remote(send.at[:, at], got.at[:, at], part_sem.at[number], part_got.at[number, k], pair)

    def own_columns(k):
        return lanes(lax.rem(mine * near + k, chunks) * cut, cut)

    def other_columns(k):
        return lanes(lax.rem((1 - mine) * near + k, chunks) * cut, cut)

    def offset(k, rows):
        there = lanes(k * cut, cut)
        return xf[rows, own_columns(k)].astype(F32) - tg[rows, there].astype(F32)

    def send_parts(number, value, rows, send, got, with_offset):
        def one(k, near_half):
            at = own_columns(k)
            part = value(at)
            if near_half and with_offset:
                part = part + offset(k, rows)
            send[:, at] = part.astype(BF)
            part_copy(number, send, got, k, mine).start()
        def first(k, carry):
            one(k, True)
            return carry
        def later(k, carry):
            one(k, False)
            return carry
        lax.fori_loop(0, near, first, 0)
        lax.fori_loop(near, chunks, later, 0)

    def take_parts(number, send, got, rows, weight, error, also, first=0, last=chunks):
        def one(k, carry):
            at = other_columns(k)
            part_copy(number, send, got, k, 1 - mine).wait_recv()
            total = send[:, at].astype(F32) + got[:, at].astype(F32)
            error[rows, at] = (weight[rows] * total).astype(BF)
            part = error[:, at]
            acc[...] += dot_of(part, ow[:, at], ((1,), (1,)))
            also(at, part)
            return carry
        lax.fori_loop(first, last, one, 0)

    support_rows, query_rows = slice(0, high), slice(low, length)
    nothing = lambda at, part: None

    def value_0(at):
        return dot_of(z_mine[...], ow[:, at], ((1,), (0,)))

    early_rows, middle_rows, late_rows = pl.ds(0, low), pl.ds(low, high - low), pl.ds(high, length - high)
    acc[...] = jnp.zeros_like(acc)
    send_parts(0, value_0, support_rows, part_0, got_0, True)
    take_parts(0, part_0, got_0, support_rows, weight_s, err_1, nothing, 0, 6)
    gather_line(0, a_all, 1)
    take_parts(0, part_0, got_0, support_rows, weight_s, err_1, nothing, 6, chunks)
    a2a_start(1, err_1, both_cols, early_rows)

    back[...] = acc[...].astype(BF)
    for h in range(heads):
        up = dot_of(probs_t[:, head(h)], back[:, head(h)], ((1,), (0,))).astype(BF)
        new = (upper[:, head(h)].astype(F32) - step_rate * dot_of(gram_b[...], up, ((1,), (0,)))).astype(BF)
        mixq[:, head(h)] = dot_of(probs[:, head(h)], new, ((1,), (0,))).astype(BF)
    cross[:, high:] = jnp.zeros((length, length - high), BF)
    product = -step_rate * dot_of(mixq[...], z_mine[...], ((1,), (1,)))
    cross[:, :high] = jnp.where(is_support, F32(0.0), product).astype(BF)
    cross_copy = remote(cross, cross_got, cross_sem.at[0], cross_sem.at[1], pair)
    cross_copy.start()

    def value_1(at):
        part = dot_of(mixq[...], ow[:, at], ((1,), (0,))) + dot_of(cross[:, :high], err_1[:high, at], ((1,), (0,)))
        return part[low:]

    half_acc[...] = jnp.zeros_like(half_acc)
    acc[...] = jnp.zeros_like(acc)

    def pairs_of(at, part):
        half_acc[...] += dot_of(part, err_1[:, at], ((1,), (1,)))

    send_parts(1, value_1, query_rows, part_1, got_1, True)
    gather_line(0, a_all, 2)
    cross_copy.wait_recv()
    cross_sum = (cross[...].astype(F32) + cross_got[...].astype(F32)).astype(BF)
    left[...] = (mixq[...].astype(F32) + dot_of(cross_sum[:, :high], a_mine[:high], ((1,), (0,)))).astype(BF)
    a_mine[high:, :] = left[high:, :]
    gather_start(3, a_all)
    take_parts(1, part_1, got_1, query_rows, weight_q, err_2, pairs_of, 0, 3)
    for away in range(3, lines):
        gather_line(0, a_all, away)
    take_parts(1, part_1, got_1, query_rows, weight_q, err_2, pairs_of, 3, 5)
    gather_line(3, a_all, 1)
    take_parts(1, part_1, got_1, query_rows, weight_q, err_2, pairs_of, 5, 7)
    gather_sides(0, a_all)
    take_parts(1, part_1, got_1, query_rows, weight_q, err_2, pairs_of, 7, chunks)
    gather_line(3, a_all, 2)

    pairs[...] = (-step_rate * half_acc[...]).astype(BF)
    back[...] = (acc[...] + dot_of(pairs[:, :high], z_mine[...], ((1,), (0,)))).astype(BF)
    left_mine = left_all.at[me]
    for h in range(heads):
        up = dot_of(probs_t[:, head(h)], back[:, head(h)], ((1,), (0,)))
        value_now[:, head(h)] = up
        flow = (-step_rate * dot_of(gram_b[...], up.astype(BF), ((1,), (0,)))).astype(BF)
        again = dot_of(probs[:, head(h)], flow, ((1,), (0,))).astype(BF)
        second[:, head(h)] = again
        left_mine[:, head(h)] = jnp.where(is_support, again, left[:, head(h)])[:high]

    def value_2(at):
        part = dot_of(second[...], ow[:, at], ((1,), (0,))) + dot_of(cross[...], err_2[:, at], ((0,), (0,)))
        return part[:high]

    acc[...] = jnp.zeros_like(acc)
    gather_start(1, left_all)
    send_parts(2, value_2, support_rows, part_2, got_2, False)

    def join(k, carry):
        at = own_columns(k)
        both[:, at] = jnp.where(is_support, err_1[:, at], err_2[:, at])
        return carry
    lax.fori_loop(0, chunks, join, 0)
    keeper = core == mine

    def both_start(first, last):
        def one(index, carry):
            step = 2 * index + lax.rem(core + mine, 2)
            @pl.when(step > 0)
            def _():
                a2a_copy(2, both, both_cols, middle_rows, step).start()
                a2a_copy(3, both, right_a, late_rows, step).start()
            return carry
        lax.fori_loop(first, last, one, 0)

    def both_moved(number, array, rows, slots):
        group = array.at[pl.ds(0, slots), rows]
        return remote(group, group, a2a_send.at[number], a2a_got.at[number], pair)

    both_arrays = ((2, both_cols, middle_rows), (3, right_a, late_rows))

    def both_forward():
        @pl.when(keeper)
        def _():
            both_cols[me, middle_rows] = both[middle_rows, lanes(me * piece, piece)]
            right_a[me, late_rows] = both[late_rows, lanes(me * piece, piece)]
            for number, array, rows in both_arrays:
                both_moved(number, array, rows, count - 1).wait_recv()
                both_moved(number + 2, array, rows, count).start()

    def both_ready():
        @pl.when(jnp.logical_not(keeper))
        def _():
            for number, array, rows in both_arrays:
                both_moved(number + 2, array, rows, count).wait_recv()

    def both_sent():
        @pl.when(keeper)
        def _():
            for number, array, rows in both_arrays:
                both_moved(number, array, rows, count // 2 - 1).wait_send()
                both_moved(number + 2, array, rows, count).wait_send()
        @pl.when(jnp.logical_not(keeper))
        def _():
            for number, array, rows in both_arrays:
                both_moved(number, array, rows, count // 2).wait_send()

    def swap_copy(slot):
        return remote(swap.at[slot], swap_got.at[slot], swap_sem.at[count], swap_sem.at[slot], pair)

    def swap_one(slot):
        swap[slot] = dot_of(left_all[slot], ow[:, lanes(me * piece, piece)], ((1,), (0,))).astype(BF)
        swap_copy(slot).start()

    def swap_own(away, over_side):
        at_distance(away, lambda source: swap_one(place(source, 1 - side if over_side else side, core)))

    def swap_core(away, over):
        def one(source):
            gather_core(1, left_all, source, over)
            swap_one(place(source, 1 - side if over else side, 1 - core))
        at_distance(away, one)

    def take_2(first, last):
        take_parts(2, part_2, got_2, support_rows, weight_s, err_3, nothing, first, last)

    both_start(0, 3)
    take_2(0, 1)
    for away in range(3, lines):
        gather_line(3, a_all, away)
    swap_own(0, False)
    take_2(1, 2)
    gather_line(1, left_all, 1)
    both_start(3, 6)
    swap_own(1, False)
    take_2(2, 3)
    gather_side(1, left_all, 0)
    swap_own(0, True)
    take_2(3, 4)
    gather_sides(3, a_all)
    both_start(6, count // 2)
    swap_core(0, 0)
    swap_core(1, 0)
    take_2(4, 7)
    gather_line(1, left_all, 2)
    swap_own(2, False)
    take_2(7, chunks)

    back[...] = (acc[...] + dot_of(pairs[...], mixq[...], ((0,), (0,)))).astype(BF)
    rows_mine = rows_all.at[me]
    for h in range(heads):
        late = dot_of(probs_t[:, head(h)], back[:, head(h)], ((1,), (0,)))
        rows_mine[:, head(h)] = ((value_now[:, head(h)] + late) * scale_row).astype(BF)
    gather_start(2, rows_all)
    gather_start(4, rows_all)
    gather_side(1, left_all, 1)
    swap_own(1, True)
    swap_core(0, 1)
    swap_core(2, 0)
    both_forward()
    for away in range(3, lines):
        gather_line(1, left_all, away)
        swap_own(away, False)
    swap_core(1, 1)

    x_cols[me] = xf[:, lanes(me * piece, piece)]
    both_cols[me, early_rows] = both[early_rows, lanes(me * piece, piece)]

    def add_pair(number, source, side_at):
        both_cores = pl.ds(place(source, side_at, 0), 2)
        return dot_of(
            x_cols[both_cores].reshape(2 * length, piece),
            rows_all[both_cores, :, part_lanes[number]].reshape(2 * length, width // 2),
            ((0,), (0,)),
        )

    def column(number):
        def one(source):
            gather_core(number, rows_all, source, 0)
            dv_ref[:, part_lanes[number]] += add_pair(number, source, side)
        return one

    def across(number):
        def one(source):
            gather_core(number, rows_all, source, 1)
            dv_ref[:, part_lanes[number]] += add_pair(number, source, 1 - side)
        return one

    a2a_wait(0, x_cols, all_rows)
    gather_line(2, rows_all, 1)
    for number in (2, 4):
        gather_core(number, rows_all, line, 0)
        dv_ref[:, part_lanes[number]] = add_pair(number, line, side)
    gather_side(1, left_all, 2)
    swap_own(2, True)
    gather_line(4, rows_all, 1)
    gather_side(2, rows_all, 0)
    gather_side(4, rows_all, 0)
    at_distance(1, column(2))
    swap_core(2, 1)
    for away in range(3, lines):
        swap_core(away, 0)
    gather_line(2, rows_all, 2)
    at_distance(1, column(4))
    for away in range(3, lines):
        gather_side(1, left_all, away)
        swap_own(away, True)
    gather_line(4, rows_all, 2)
    at_distance(0, across(2))
    gather_side(2, rows_all, 1)
    at_distance(0, across(4))
    for away in range(3, lines):
        swap_core(away, 1)
    a2a_wait(1, both_cols, early_rows)
    both_ready()

    tile = 256

    def early(i, carry):
        at = lanes(i * tile, tile)
        do_ref[at, :] = dot_of(
            left_all[:, :, at].reshape(count * high, tile), both_cols[...].reshape(count * high, piece), ((0,), (0,))
        )
        return carry
    lax.fori_loop(0, width // tile, early, 0)
    gather_side(4, rows_all, 1)
    at_distance(2, column(2))
    gather_side(2, rows_all, 2)
    for away in range(3, lines):
        gather_line(2, rows_all, away)
    at_distance(2, column(4))
    gather_side(4, rows_all, 2)
    for away in range(3, lines):
        gather_line(4, rows_all, away)
    gather_finish(0, a_all)
    gather_finish(3, a_all)
    for away in range(3, lines):
        for number in (2, 4):
            at_distance(away, column(number))
    for number in (2, 4):
        at_distance(1, across(number))

    def swapped(slot, carry):
        swap_copy(slot).wait_recv()
        right_a[slot, :high] = (swap[slot].astype(F32) + swap_got[slot].astype(F32)).astype(BF)
        return carry
    lax.fori_loop(0, count, swapped, 0)

    def late_part(i, carry):
        at = lanes(i * tile, tile)
        do_ref[at, :] += dot_of(
            a_all[:, :, at].reshape(count * length, tile), right_a[...].reshape(count * length, piece), ((0,), (0,))
        )
        return carry
    lax.fori_loop(0, width // tile, late_part, 0)
    for number in (2, 4):
        at_distance(2, across(number))
    for away in range(3, lines):
        gather_side(2, rows_all, away)
        gather_side(4, rows_all, away)
        at_distance(away, across(2))
        at_distance(away, across(4))

    cross_copy.wait_send()
    both_sent()
    remote(tg, tg, x_sem.at[near], x_sem.at[0], pair).wait_send()
    for number, (send, got) in enumerate(((part_0, got_0), (part_1, got_1), (part_2, got_2))):
        remote(send, got, part_sem.at[number], part_got.at[number, 0], pair).wait_send()
    remote(swap, swap_got, swap_sem.at[count], swap_sem.at[0], pair).wait_send()
    for number, array in enumerate((a_all, left_all, rows_all, a_all, rows_all)):
        gather_sent(number, array)


def one_kernel(inputs, targets, queries, key_rows, value_weight, output_weight, splits):
    count = lax.axis_size("task")
    lines = count // 4
    length, half = inputs.shape
    depth = 2 * half
    width = queries.shape[1]
    high = 3 * length // 4
    piece = depth // count
    vm = pltpu.VMEM
    dma = pltpu.SemaphoreType.DMA
    anywhere = pl.BlockSpec(memory_space=pl.ANY)
    chunks = 8
    return pl.pallas_call(
        functools.partial(step_kernel, lines),
        out_shape=(
            pltpu.VMEM((piece, width), F32),
            pltpu.VMEM((width, piece), F32),
        ),
        in_specs=[anywhere] * 6 + [pl.BlockSpec(memory_space=pltpu.SMEM)],
        out_specs=(pl.BlockSpec(memory_space=pltpu.VMEM), pl.BlockSpec(memory_space=pltpu.VMEM)),
        scratch_shapes=[
            vm((length, depth), BF),
            vm((length, half), BF),
            vm((length, width), BF),
            vm((length, width), BF),
            vm((depth, width), BF),
            vm((width, depth), BF),
        ]
        + [vm((length, width), BF)] * 6
        + [vm((length, width), F32), vm((length, length), F32)]
        + [vm((high, depth), BF)] * 6
        + [vm((length, depth), BF)] * 4
        + [vm((length, width), BF)]
        + [vm((length, length), BF)] * 4
        + [
            vm((length, width), F32),
            vm((high, width), BF),
            vm((count, length, width), BF),
            vm((count, high, width), BF),
            vm((count, length, width), BF),
            vm((count, length, piece), BF),
            vm((count, high, piece), BF),
            vm((count, length, piece), BF),
            vm((count, high, piece), BF),
            vm((count, high, piece), BF),
            dma((6,)),
            dma((chunks // 2 + 1,)),
            dma((3,)),
            dma((3, chunks)),
            dma((2,)),
            dma((count + 1,)),
            dma((6,)),
            dma((6,)),
            dma((5, 2)),
            dma((5, lines)),
            dma((5, lines)),
            dma((5, lines, 2)),
        ],
        compiler_params=pltpu.CompilerParams(
            collective_id=1, has_side_effects=True, vmem_limit_bytes=60 * 2**20
        ),
    )(inputs, targets, queries, key_rows, value_weight, output_weight, splits)


def make_device(tensor_count):
    def per_device(inputs, targets, queries, key_rows, value_weight, output_weight, splits):
        length = inputs.shape[0]
        low, high = length // 4, 3 * length // 4
        heads = queries.shape[1] // HD
        index = lax.axis_index("tensor")
        normed = normed_rows(full_rows(inputs, tensor_count, index))
        offset_here = inputs.astype(F32) - targets.astype(F32)
        offset = jnp.concatenate(
            [jnp.where(index == block, offset_here, F32(0.0)) for block in range(tensor_count)],
            axis=1,
        )
        probs = attention_probs(queries, key_rows, heads)
        probs_s = probs[:, :high, :high]
        probs_q = probs[:, low:, :]
        split = splits[0]
        count_s = split.astype(F32)
        position = jnp.arange(length)
        support = (position < split).astype(F32)[:, None]
        weight_s = (support / count_s)[:high]
        weight_q = ((1.0 - support) / (F32(length) - count_s))[low:]

        upper = mm(normed, value_weight).astype(BF)
        mixed_s = mix(probs_s, upper[:high]).astype(BF)
        gram = mm_nt(normed, normed).astype(BF)
        mixed_s_all = gather_tokens(mixed_s)
        part_0 = (mm(mixed_s, output_weight) + offset[:high]).astype(BF)
        part_0, normed_sent = lax.optimization_barrier((part_0, normed))
        normed_cols = my_columns(normed_sent)
        error_1 = (weight_s * group_sum(part_0, tensor_count)).astype(BF)

        back_u = mix_back(probs_s, mm_nt(error_1, output_weight).astype(BF)).astype(BF)
        upper_1 = (upper.astype(F32) - step_rate * mm(gram[:, :high], back_u)).astype(BF)
        mixed_q = mix(probs_q, upper_1).astype(BF)
        cross = (-step_rate * mm_nt(mixed_q, mixed_s)).astype(BF)
        part_1 = mm(mixed_q, output_weight) + mm(cross, error_1)
        part_1 = (part_1 + offset[low:]).astype(BF)
        error_2 = (weight_q * group_sum(part_1, tensor_count)).astype(BF)

        errors = (-step_rate * mm_nt(error_2, error_1)).astype(BF)
        back_z1 = (mm_nt(error_2, output_weight) + mm(errors, mixed_s)).astype(BF)
        back_u1 = mix_back(probs_q, back_z1)
        back_u1_b = back_u1.astype(BF)
        back_gram = (-step_rate * mm(gram[:high], back_u1_b)).astype(BF)
        second = mix(probs_s, back_gram).astype(BF)
        error_back = (mm(second, output_weight) + mm_tn(cross, error_2)).astype(BF)
        is_support = (position < split)[:, None]
        left = jnp.where(is_support, below(second, length), above(mixed_q, length))
        errors_both = jnp.where(is_support, below(error_1, length), above(error_2, length))
        error_back, normed_cols, errors_both, left = lax.optimization_barrier(
            (error_back, normed_cols, errors_both, left)
        )
        both_cols = my_columns(errors_both)
        left, mixed_s_all = lax.optimization_barrier((left, mixed_s_all))
        left_all = gather_tokens(left)
        error_sum = group_sum(error_back, tensor_count)
        error_3 = (weight_s * error_sum).astype(BF)
        error_3_cols = my_columns(error_3)

        back_z0 = (mm_nt(error_3, output_weight) + mm_tn(errors, mixed_q)).astype(BF)
        late = mix_back(probs_s, back_z0)
        value_rows = (back_u1 + jnp.pad(late, ((0, length - high), (0, 0)))).astype(BF)
        value_rows_all = gather_by_copies(value_rows, 1)
        total_output = (
            mm_tn(left_all, both_cols)
            + mm_tn(mixed_s_all, error_3_cols)
        )
        total_value = mm_tn(normed_cols, value_rows_all)
        return (total_value, total_output)

    return per_device


def solution(mesh):
    whole_step = mesh.shape["tensor"] == 2 and mesh.shape["task"] % 4 == 0
    return jax.shard_map(
        one_kernel if whole_step else make_device(mesh.shape["tensor"]),
        mesh=mesh,
        in_specs=(
            P("task", "tensor"),
            P("task", "tensor"),
            P("task", "tensor"),
            P("task", "tensor"),
            P(None, "tensor"),
            P("tensor", None),
            P("task"),
        ),
        out_specs=(P("task", "tensor"), P("tensor", "task")),
        check_vma=False,
    )
```

```python
import functools

import jax
import jax.numpy as jnp
from jax import lax
from jax.experimental import pallas as pl
from jax.experimental.pallas import tpu as pltpu
from jax.sharding import PartitionSpec as P

HD = 128
BF = jnp.bfloat16
F32 = jnp.float32

step_rate = 0.25


def normed_rows(inputs):
    values = inputs.astype(F32)
    scale = lax.rsqrt(jnp.mean(values * values, axis=-1, keepdims=True) + 1e-05)
    return (values * scale).astype(BF)


def attention_probs(queries, key_rows, heads):
    length = queries.shape[0]
    query_h = queries.reshape(length, heads, -1)
    key_h = key_rows.reshape(length, heads, -1)
    scores = jnp.einsum("ihd,jhd->hij", query_h, key_h, preferred_element_type=F32)
    scores = scores / jnp.sqrt(F32(query_h.shape[2]))
    position = jnp.arange(length)
    causal = position[:, None] >= position[None, :]
    scores = jnp.where(causal[None], scores, F32(-1e30))
    scores = scores - jnp.max(scores, axis=-1, keepdims=True)
    expo = jnp.exp(scores)
    return (expo / jnp.sum(expo, axis=-1, keepdims=True)).astype(BF)


def mm(left, right):
    return jnp.dot(left, right, preferred_element_type=F32)


def mm_nt(left, right):
    return lax.dot_general(left, right, (((1,), (1,)), ((), ())), preferred_element_type=F32)


def mm_tn(left, right):
    return lax.dot_general(left, right, (((0,), (0,)), ((), ())), preferred_element_type=F32)


def mix(probs, rows):
    heads = probs.shape[0]
    split = rows.reshape(rows.shape[0], heads, -1)
    out = jnp.einsum("hij,jhd->ihd", probs, split, preferred_element_type=F32)
    return out.reshape(out.shape[0], -1)


def mix_back(probs, rows):
    heads = probs.shape[0]
    split = rows.reshape(rows.shape[0], heads, -1)
    out = jnp.einsum("hij,ihd->jhd", probs, split, preferred_element_type=F32)
    return out.reshape(out.shape[0], -1)


def group_sum(term, count):
    term = term.astype(BF)
    if count == 1:
        return term.astype(F32)
    if count == 2:
        other = lax.ppermute(term, "tensor", ((0, 1), (1, 0)))
        return term.astype(F32) + other.astype(F32)
    share = lax.psum_scatter(term, "tensor", scatter_dimension=1, tiled=True)
    return lax.all_gather(share, "tensor", axis=1, tiled=True).astype(F32)


def full_rows(inputs, count, index):
    if count != 2:
        return lax.all_gather(inputs, "tensor", axis=1, tiled=True)
    other = lax.ppermute(inputs, "tensor", ((0, 1), (1, 0)))
    low = jnp.where(index == 0, inputs, other)
    high = jnp.where(index == 0, other, inputs)
    return jnp.concatenate([low, high], axis=1)


def gather_kernel(lines, src_ref, out_ref, own_sem, send_sem, line_sem, side_sem, core_sem):
    me = lax.axis_index("task")
    core, side, line = lax.rem(me, 2), lax.rem(me // 2, 2), me // 4

    def place(back, over_side, over_core):
        line_from = lax.rem(line + lines - back, lines)
        side_from = 1 - side if over_side else side
        core_from = 1 - core if over_core else core
        return (line_from * 2 + side_from) * 2 + core_from

    side_peer, core_peer = place(0, True, False), place(0, False, True)
    peers = [place(lines - step, False, False) for step in range(1, lines)] + [side_peer, core_peer]
    barrier = pltpu.get_barrier_semaphore()
    for peer in peers:
        pl.semaphore_signal(
            barrier, inc=1, device_id={"task": peer}, device_id_type=pl.DeviceIdType.MESH
        )
    pl.semaphore_wait(barrier, len(peers))

    started = []

    def send(source, slot, arrival, peer):
        copy = pltpu.make_async_remote_copy(
            src_ref=source,
            dst_ref=out_ref.at[slot],
            send_sem=send_sem.at[len(started)],
            recv_sem=arrival,
            device_id={"task": peer},
            device_id_type=pl.DeviceIdType.MESH,
        )
        copy.start()
        started.append(copy)

    def arrived(slot, arrival, peer):
        pltpu.make_async_remote_copy(
            src_ref=out_ref.at[slot],
            dst_ref=out_ref.at[slot],
            send_sem=send_sem.at[0],
            recv_sem=arrival,
            device_id={"task": peer},
            device_id_type=pl.DeviceIdType.MESH,
        ).wait_recv()

    for step in sorted(range(1, lines), key=lambda step: -min(step, lines - step)):
        send(src_ref, me, line_sem.at[step], peers[step - 1])
    send(src_ref, me, side_sem.at[0], side_peer)
    send(src_ref, me, core_sem.at[0, 0], core_peer)
    own = pltpu.make_async_copy(src_ref, out_ref.at[me], own_sem)
    own.start()
    order = sorted(range(1, lines), key=lambda step: min(step, lines - step))
    for step in order:
        slot = place(step, False, False)
        arrived(slot, line_sem.at[step], side_peer)
        send(out_ref.at[slot], slot, side_sem.at[step], side_peer)
        send(out_ref.at[slot], slot, core_sem.at[step, 0], core_peer)
    for step in [0] + order:
        slot = place(step, True, False)
        arrived(slot, side_sem.at[step], side_peer)
        send(out_ref.at[slot], slot, core_sem.at[step, 1], core_peer)
    for step in [0] + order:
        for over in range(2):
            arrived(place(step, over == 1, True), core_sem.at[step, over], core_peer)
    own.wait()
    for copy in started:
        copy.wait_send()


def gather_by_copies(rows, number):
    count = lax.axis_size("task")
    if count % 4:
        return gather_tokens(rows)
    lines = count // 4
    sends = (lines + 1) + 2 * (lines - 1) + lines
    gathered = pl.pallas_call(
        functools.partial(gather_kernel, lines),
        out_shape=jax.ShapeDtypeStruct((count,) + rows.shape, rows.dtype),
        in_specs=[pl.BlockSpec(memory_space=pltpu.VMEM)],
        out_specs=pl.BlockSpec(memory_space=pltpu.VMEM),
        scratch_shapes=[
            pltpu.SemaphoreType.DMA,
            pltpu.SemaphoreType.DMA((sends,)),
            pltpu.SemaphoreType.DMA((lines,)),
            pltpu.SemaphoreType.DMA((lines,)),
            pltpu.SemaphoreType.DMA((lines, 2)),
        ],
        compiler_params=pltpu.CompilerParams(collective_id=number, has_side_effects=True),
        cost_estimate=pl.CostEstimate(
            flops=0, bytes_accessed=16 * rows.size * rows.dtype.itemsize * count, transcendentals=0
        ),
    )(rows)
    return gathered.reshape(count * rows.shape[0], rows.shape[1])


def gather_tokens(rows):
    return lax.all_gather(rows, "task", axis=0, tiled=True)


def my_columns(rows):
    return lax.all_to_all(rows, "task", split_axis=1, concat_axis=0, tiled=True)


def below(rows, length):
    return jnp.pad(rows, ((0, length - rows.shape[0]), (0, 0)))


def above(rows, length):
    return jnp.pad(rows, ((length - rows.shape[0], 0), (0, 0)))


MESH = pl.DeviceIdType.MESH


def dot_of(left, right, dims):
    return lax.dot_general(left, right, (dims, ((), ())), preferred_element_type=F32)


def step_kernel(
    lines,
    x_in, t_in, q_in, k_in, v_in, o_in, split_ref,
    dv_ref, do_ref,
    xf, tg, qs, ks, vw, ow, probs, probs_t, upper, mixq, second, left, chain, mixed_all, acc, half_acc,
    part_0, part_1, part_2, got_0, got_1, got_2, err_1, err_2, err_3, both,
    back, gram_b, cross, cross_got, pairs, value_now, z_mine, a_all, left_all, rows_all,
    x_cols, both_cols, right_a, swap, swap_got,
    load_sem, x_sem, part_sem, part_got, cross_sem, swap_sem,
    a2a_send, a2a_got, g_send, g_line, g_side, g_core,
):
    count = lines * 4
    length, depth = xf.shape
    half = depth // 2
    width = upper.shape[1]
    heads = width // HD
    low, high = length // 4, 3 * length // 4
    piece = depth // count
    chunks = 8
    cut = depth // chunks
    near = chunks // 2

    me = lax.axis_index("task")
    mine = lax.axis_index("tensor")
    core, side, line = lax.rem(me, 2), lax.rem(me // 2, 2), me // 4
    pair = {"tensor": 1 - mine}

    def place(line_at, side_at, core_at):
        return (line_at * 2 + side_at) * 2 + core_at

    def lanes(start, size):
        return pl.ds(pl.multiple_of(start, 128), size)

    own_half = lanes(mine * half, half)
    loads = [
        pltpu.make_async_copy(x_in, xf.at[:, own_half], load_sem.at[0]),
        pltpu.make_async_copy(q_in, qs, load_sem.at[1]),
        pltpu.make_async_copy(k_in, ks, load_sem.at[2]),
        pltpu.make_async_copy(v_in, vw, load_sem.at[3]),
        pltpu.make_async_copy(t_in, tg, load_sem.at[4]),
        pltpu.make_async_copy(o_in, ow, load_sem.at[5]),
    ]
    for load in loads:
        load.start()

    barrier = pltpu.get_barrier_semaphore()
    for step in range(1, count):
        pl.semaphore_signal(
            barrier, inc=1, device_id={"task": lax.rem(me + step, count)}, device_id_type=MESH
        )
    pl.semaphore_signal(barrier, inc=1, device_id=pair, device_id_type=MESH)
    pl.semaphore_wait(barrier, count)

    def remote(src, dst, send, got, peer):
        return pltpu.make_async_remote_copy(
            src_ref=src, dst_ref=dst, send_sem=send, recv_sem=got, device_id=peer, device_id_type=MESH
        )

    def x_copy(k, owner):
        part = xf.at[:, lanes(owner * half + k * cut, cut)]
        return remote(part, part, x_sem.at[near], x_sem.at[k], pair)

    loads[0].wait()
    for k in range(near):
        x_copy(k, mine).start()

    def a2a_copy(number, src, dst, rows, step):
        peer = lax.rem(me + step, count)
        return remote(
            src.at[rows, lanes(peer * piece, piece)],
            dst.at[me, rows],
            a2a_send.at[number],
            a2a_got.at[number],
            {"task": peer},
        )

    def a2a_start(number, src, dst, rows, first=1, last=count):
        def one(step, carry):
            a2a_copy(number, src, dst, rows, step).start()
            return carry
        lax.fori_loop(first, last, one, 0)

    def a2a_wait(number, dst, rows):
        arrived = dst.at[pl.ds(0, count - 1), rows]
        remote(arrived, arrived, a2a_send.at[number], a2a_got.at[number], {"task": lax.rem(me + 1, count)}).wait()

    all_rows = pl.ds(0, length)

    def x_spread(owner, first, last):
        def one(index, carry):
            step = lax.rem(owner * (count // 2) + index + count - me, count)
            @pl.when(step > 0)
            def _():
                a2a_copy(0, xf, x_cols, all_rows, step).start()
            return carry
        lax.fori_loop(first, last, one, 0)

    x_spread(mine, 0, count // 2)

    part_rows = (pl.ds(0, high), pl.ds(0, high), all_rows, pl.ds(high, length - high), all_rows)
    part_lanes = (pl.ds(0, width),) * 2 + (pl.ds(0, width // 2), pl.ds(0, width), pl.ds(width // 2, width // 2))

    def gather_copy(number, array, slot, kind, source, got, peer):
        block = array.at[slot, part_rows[number], part_lanes[number]]
        return remote(block, block, g_send.at[number, 0 if kind < 2 else 1], got, {"task": peer})

    def from_end(number, source, away):
        if number in (1, 4) and lines > 2 and away == 2:
            return jnp.logical_or(source == 0, source == lines - 1)
        return None

    def detour(number, away):
        return number == 2 and lines > 2 and away == lines - 1

    up_peer, down_peer = me + 4, me - 4
    side_peer, core_peer = place(line, 1 - side, core), place(line, side, 1 - core)

    def pass_on(number, array, source, away):
        slot = place(source, side, core)
        if not detour(number, away):
            through = from_end(number, source, away)
            @pl.when(True if through is None else jnp.logical_not(through))
            def _():
                gather_copy(number, array, slot, 2, source, g_side.at[number, source], side_peer).start()
        @pl.when(jnp.logical_and(source <= line, line < lines - 1))
        def _():
            gather_copy(number, array, slot, 0, source, g_line.at[number, source], up_peer).start()
        @pl.when(jnp.logical_and(source >= line, line > 0))
        def _():
            gather_copy(number, array, slot, 1, source, g_line.at[number, source], down_peer).start()
        gather_copy(number, array, slot, 3, source, g_core.at[number, source, 0], core_peer).start()

    def gather_start(number, array):
        pass_on(number, array, line, 0)

    def at_distance(away, take):
        if away == 0:
            take(line)
            return
        @pl.when(line >= away)
        def _():
            take(line - away)
        @pl.when(line + away < lines)
        def _():
            take(line + away)

    def gather_line(number, array, away):
        def take(source):
            slot = place(source, side, core)
            gather_copy(number, array, slot, 2, source, g_line.at[number, source], side_peer).wait_recv()
            pass_on(number, array, source, away)
        at_distance(away, take)

    def gather_side(number, array, away):
        def take(source):
            slot = place(source, 1 - side, core)
            gather_copy(number, array, slot, 4, source, g_side.at[number, source], core_peer).wait_recv()
            gather_copy(number, array, slot, 4, source, g_core.at[number, source, 1], core_peer).start()
            through = from_end(number, source, away + 1)
            if detour(number, away + 1) or through is not None:
                through = True if through is None else through
                @pl.when(functools.reduce(jnp.logical_and, (source < line, line < lines - 1, through)))
                def _():
                    gather_copy(number, array, slot, 4, source, g_side.at[number, source], up_peer).start()
                @pl.when(functools.reduce(jnp.logical_and, (source > line, line > 0, through)))
                def _():
                    gather_copy(number, array, slot, 4, source, g_side.at[number, source], down_peer).start()
        at_distance(away, take)

    def gather_sides(number, array):
        for away in range(lines):
            gather_side(number, array, away)

    def gather_core(number, array, source, over):
        slot = place(source, side if over == 0 else 1 - side, 1 - core)
        gather_copy(number, array, slot, 3, source, g_core.at[number, source, over], core_peer).wait_recv()

    def gather_finish(number, array):
        for source in range(lines):
            for over in range(2):
                gather_core(number, array, source, over)

    def gather_sent(number, array):
        def sent(blocks, which):
            group = array.at[pl.ds(0, blocks), part_rows[number], part_lanes[number]]
            remote(group, group, g_send.at[number, which], g_core.at[number, 0, 0], {"task": core_peer}).wait_send()
        for at in range(lines):
            ups = at + 1 if at < lines - 1 else 0
            downs = lines - at if at > 0 else 0
            others = 3 * lines
            if detour(number, lines - 1):
                ends = (at == 0) + (at == lines - 1)
                inner = (at == lines - 2) + (at == 1)
                others += inner - ends
            if number in (1, 4) and lines > 2:
                others += (at == 1) + (at == lines - 2) - (at == 2) - (at == lines - 3)
            @pl.when(line == at)
            def _():
                sent(ups + downs, 0)
                sent(others, 1)

    def head(h):
        return slice(h * HD, (h + 1) * HD)

    row = lax.broadcasted_iota(jnp.int32, (length, length), 0)
    col = lax.broadcasted_iota(jnp.int32, (length, length), 1)
    causal = row >= col
    loads[1].wait()
    loads[2].wait()
    root = jnp.sqrt(F32(HD))
    for h in range(heads):
        scores = dot_of(qs[:, head(h)], ks[:, head(h)], ((1,), (1,))) / root
        scores = jnp.where(causal, scores, F32(-1e30))
        scores = scores - jnp.max(scores, axis=-1, keepdims=True)
        expo = jnp.exp(scores)
        prob = expo / jnp.sum(expo, axis=-1, keepdims=True)
        probs[:, head(h)] = prob.astype(BF)
        probs_t[:, head(h)] = prob.T.astype(BF)

    err_1[high:, :] = jnp.zeros((length - high, depth), BF)
    err_2[:low, :] = jnp.zeros((low, depth), BF)
    err_3[high:, :] = jnp.zeros((length - high, depth), BF)
    position = lax.broadcasted_iota(jnp.int32, (length, 1), 0)
    split = jnp.full((length, 1), split_ref[0], jnp.int32)
    is_support = position < split
    support = is_support.astype(F32)
    count_s = split.astype(F32)
    weight_s = support / count_s
    weight_q = (1.0 - support) / (F32(length) - count_s)

    loads[3].wait()

    def take(k, owner, first):
        at = lanes(owner * half + k * cut, cut)
        x_part = xf[:, at]
        new = dot_of(x_part, vw[pl.ds(pl.multiple_of(owner * half + k * cut, 128), cut), :], ((1,), (0,)))
        gram = dot_of(x_part, x_part, ((1,), (1,)))
        if first:
            acc[...] = new
            half_acc[...] = gram
        else:
            acc[...] += new
            half_acc[...] += gram

    take(0, mine, True)
    def own_take(k, carry):
        take(k, mine, False)
        return carry
    lax.fori_loop(1, near, own_take, 0)
    def other_take(k, carry):
        x_copy(k, 1 - mine).wait_recv()
        x_spread(1 - mine, 2 * k, 2 * k + 2)
        take(k, 1 - mine, False)
        return carry
    lax.fori_loop(0, near, other_take, 0)

    gram_raw = half_acc[...]
    diagonal = jnp.where(row == col, gram_raw, F32(0.0))
    scale_row = lax.rsqrt(jnp.sum(diagonal, axis=1, keepdims=True) / F32(depth) + 1e-05)
    scale_col = lax.rsqrt(jnp.sum(diagonal, axis=0, keepdims=True) / F32(depth) + 1e-05)
    gram_b[...] = (gram_raw * scale_row * scale_col).astype(BF)
    upper[...] = (acc[...] * scale_row).astype(BF)

    a_mine = a_all.at[me]
    for h in range(heads):
        mixed = dot_of(probs[:, head(h)], upper[:, head(h)], ((1,), (0,)))
        mixed_all[:, head(h)] = mixed
        z_mine[:, head(h)] = mixed[:high].astype(BF)
    a_mine[:high, :] = (weight_s[:high] * z_mine[...].astype(F32)).astype(BF)
    gather_start(0, a_all)
    loads[4].wait()
    loads[5].wait()

    def part_copy(number, send, got, k, owner):
        at = lanes(lax.rem(owner * near + k, chunks) * cut, cut)
        return remote(send.at[:, at], got.at[:, at], part_sem.at[number], part_got.at[number, k], pair)

    def own_columns(k):
        return lanes(lax.rem(mine * near + k, chunks) * cut, cut)

    def other_columns(k):
        return lanes(lax.rem((1 - mine) * near + k, chunks) * cut, cut)

    def offset(k, rows):
        there = lanes(k * cut, cut)
        return xf[rows, own_columns(k)].astype(F32) - tg[rows, there].astype(F32)

    def send_parts(number, value, rows, send, got, with_offset):
        def one(k, near_half):
            at = own_columns(k)
            part = value(at)
            if near_half and with_offset:
                part = part + offset(k, rows)
            send[:, at] = part.astype(BF)
            part_copy(number, send, got, k, mine).start()
        def first(k, carry):
            one(k, True)
            return carry
        def later(k, carry):
            one(k, False)
            return carry
        lax.fori_loop(0, near, first, 0)
        lax.fori_loop(near, chunks, later, 0)

    def take_parts(number, send, got, rows, weight, error, also, first=0, last=chunks):
        def one(k, carry):
            at = other_columns(k)
            part_copy(number, send, got, k, 1 - mine).wait_recv()
            total = send[:, at].astype(F32) + got[:, at].astype(F32)
            error[rows, at] = (weight[rows] * total).astype(BF)
            part = error[:, at]
            acc[...] += dot_of(part, ow[:, at], ((1,), (1,)))
            also(at, part)
            return carry
        lax.fori_loop(first, last, one, 0)

    support_rows, query_rows = slice(0, high), slice(low, length)
    nothing = lambda at, part: None

    def value_0(at):
        return dot_of(z_mine[...], ow[:, at], ((1,), (0,)))

    early_rows, middle_rows, late_rows = pl.ds(0, low), pl.ds(low, high - low), pl.ds(high, length - high)
    acc[...] = jnp.zeros_like(acc)
    send_parts(0, value_0, support_rows, part_0, got_0, True)
    for h in range(heads):
        middle = dot_of(probs[:, head(h)], gram_b[...], ((1,), (0,))).astype(BF)
        chain[:, head(h)] = (-step_rate * dot_of(middle, probs_t[:, head(h)], ((1,), (0,)))).astype(BF)
    take_parts(0, part_0, got_0, support_rows, weight_s, err_1, nothing, 0, 6)
    gather_line(0, a_all, 1)
    take_parts(0, part_0, got_0, support_rows, weight_s, err_1, nothing, 6, chunks)
    a2a_start(1, err_1, both_cols, early_rows)

    back[...] = acc[...].astype(BF)
    for h in range(heads):
        moved = dot_of(chain[:, head(h)], back[:, head(h)], ((1,), (0,)))
        mixq[:, head(h)] = (mixed_all[:, head(h)] + moved).astype(BF)
    cross[:, high:] = jnp.zeros((length, length - high), BF)
    product = -step_rate * dot_of(mixq[...], z_mine[...], ((1,), (1,)))
    cross[:, :high] = jnp.where(is_support, F32(0.0), product).astype(BF)
    cross_copy = remote(cross, cross_got, cross_sem.at[0], cross_sem.at[1], pair)
    cross_copy.start()

    def value_1(at):
        part = dot_of(mixq[...], ow[:, at], ((1,), (0,))) + dot_of(cross[:, :high], err_1[:high, at], ((1,), (0,)))
        return part[low:]

    half_acc[...] = jnp.zeros_like(half_acc)
    acc[...] = jnp.zeros_like(acc)

    def pairs_of(at, part):
        half_acc[...] += dot_of(part, err_1[:, at], ((1,), (1,)))

    send_parts(1, value_1, query_rows, part_1, got_1, True)
    gather_line(0, a_all, 2)
    cross_copy.wait_recv()
    cross_sum = (cross[...].astype(F32) + cross_got[...].astype(F32)).astype(BF)
    left[...] = (mixq[...].astype(F32) + dot_of(cross_sum[:, :high], a_mine[:high], ((1,), (0,)))).astype(BF)
    a_mine[high:, :] = left[high:, :]
    gather_start(3, a_all)
    take_parts(1, part_1, got_1, query_rows, weight_q, err_2, pairs_of, 0, 3)
    for away in range(3, lines):
        gather_line(0, a_all, away)
    take_parts(1, part_1, got_1, query_rows, weight_q, err_2, pairs_of, 3, 5)
    gather_line(3, a_all, 1)
    take_parts(1, part_1, got_1, query_rows, weight_q, err_2, pairs_of, 5, 7)
    gather_sides(0, a_all)
    take_parts(1, part_1, got_1, query_rows, weight_q, err_2, pairs_of, 7, chunks)
    gather_line(3, a_all, 2)

    pairs[...] = (-step_rate * half_acc[...]).astype(BF)
    back[...] = (acc[...] + dot_of(pairs[:, :high], z_mine[...], ((1,), (0,)))).astype(BF)
    left_mine = left_all.at[me]
    for h in range(heads):
        again = dot_of(chain[:, head(h)], back[:, head(h)], ((1,), (0,))).astype(BF)
        second[:, head(h)] = again
        left_mine[:, head(h)] = jnp.where(is_support, again, left[:, head(h)])[:high]

    def value_2(at):
        part = dot_of(second[...], ow[:, at], ((1,), (0,))) + dot_of(cross[...], err_2[:, at], ((0,), (0,)))
        return part[:high]

    acc[...] = jnp.zeros_like(acc)
    gather_start(1, left_all)
    send_parts(2, value_2, support_rows, part_2, got_2, False)

    for h in range(heads):
        value_now[:, head(h)] = dot_of(probs_t[:, head(h)], back[:, head(h)], ((1,), (0,)))
    def join(k, carry):
        at = own_columns(k)
        both[:, at] = jnp.where(is_support, err_1[:, at], err_2[:, at])
        return carry
    lax.fori_loop(0, chunks, join, 0)
    keeper = core == mine

    def both_start(first, last):
        def one(index, carry):
            step = 2 * index + lax.rem(core + mine, 2)
            @pl.when(step > 0)
            def _():
                a2a_copy(2, both, both_cols, middle_rows, step).start()
                a2a_copy(3, both, right_a, late_rows, step).start()
            return carry
        lax.fori_loop(first, last, one, 0)

    def both_moved(number, array, rows, slots):
        group = array.at[pl.ds(0, slots), rows]
        return remote(group, group, a2a_send.at[number], a2a_got.at[number], pair)

    both_arrays = ((2, both_cols, middle_rows), (3, right_a, late_rows))

    def both_forward():
        @pl.when(keeper)
        def _():
            both_cols[me, middle_rows] = both[middle_rows, lanes(me * piece, piece)]
            right_a[me, late_rows] = both[late_rows, lanes(me * piece, piece)]
            for number, array, rows in both_arrays:
                both_moved(number, array, rows, count - 1).wait_recv()
                both_moved(number + 2, array, rows, count).start()

    def both_ready():
        @pl.when(jnp.logical_not(keeper))
        def _():
            for number, array, rows in both_arrays:
                both_moved(number + 2, array, rows, count).wait_recv()

    def both_sent():
        @pl.when(keeper)
        def _():
            for number, array, rows in both_arrays:
                both_moved(number, array, rows, count // 2 - 1).wait_send()
                both_moved(number + 2, array, rows, count).wait_send()
        @pl.when(jnp.logical_not(keeper))
        def _():
            for number, array, rows in both_arrays:
                both_moved(number, array, rows, count // 2).wait_send()

    def swap_copy(slot):
        return remote(swap.at[slot], swap_got.at[slot], swap_sem.at[count], swap_sem.at[slot], pair)

    def swap_one(slot):
        swap[slot] = dot_of(left_all[slot], ow[:, lanes(me * piece, piece)], ((1,), (0,))).astype(BF)
        swap_copy(slot).start()

    def swap_own(away, over_side):
        at_distance(away, lambda source: swap_one(place(source, 1 - side if over_side else side, core)))

    def swap_core(away, over):
        def one(source):
            gather_core(1, left_all, source, over)
            swap_one(place(source, 1 - side if over else side, 1 - core))
        at_distance(away, one)

    def take_2(first, last):
        take_parts(2, part_2, got_2, support_rows, weight_s, err_3, nothing, first, last)

    both_start(0, count // 2)
    take_2(0, 1)
    for away in range(3, lines):
        gather_line(3, a_all, away)
    swap_own(0, False)
    take_2(1, 2)
    gather_line(1, left_all, 1)
    swap_own(1, False)
    take_2(2, 3)
    gather_side(1, left_all, 0)
    swap_own(0, True)
    take_2(3, 4)
    gather_sides(3, a_all)
    swap_core(0, 0)
    swap_core(1, 0)
    take_2(4, 5)
    gather_line(1, left_all, 2)
    swap_own(2, False)
    take_2(5, 7)
    gather_side(1, left_all, 1)
    swap_own(1, True)
    take_2(7, chunks)

    back[...] = (acc[...] + dot_of(pairs[...], mixq[...], ((0,), (0,)))).astype(BF)
    rows_mine = rows_all.at[me]
    for h in range(heads):
        late = dot_of(probs_t[:, head(h)], back[:, head(h)], ((1,), (0,)))
        rows_mine[:, head(h)] = ((value_now[:, head(h)] + late) * scale_row).astype(BF)
    gather_start(2, rows_all)
    gather_start(4, rows_all)
    swap_core(0, 1)
    swap_core(2, 0)
    both_forward()
    for away in range(3, lines):
        gather_line(1, left_all, away)
        swap_own(away, False)
    swap_core(1, 1)

    x_cols[me] = xf[:, lanes(me * piece, piece)]
    both_cols[me, early_rows] = both[early_rows, lanes(me * piece, piece)]

    def add_pair(number, source, side_at):
        both_cores = pl.ds(place(source, side_at, 0), 2)
        return dot_of(
            x_cols[both_cores].reshape(2 * length, piece),
            rows_all[both_cores, :, part_lanes[number]].reshape(2 * length, width // 2),
            ((0,), (0,)),
        )

    def column(number):
        def one(source):
            gather_core(number, rows_all, source, 0)
            dv_ref[:, part_lanes[number]] += add_pair(number, source, side)
        return one

    def across(number):
        def one(source):
            gather_core(number, rows_all, source, 1)
            dv_ref[:, part_lanes[number]] += add_pair(number, source, 1 - side)
        return one

    a2a_wait(0, x_cols, all_rows)
    gather_line(2, rows_all, 1)
    for number in (2, 4):
        gather_core(number, rows_all, line, 0)
        dv_ref[:, part_lanes[number]] = add_pair(number, line, side)
    gather_side(1, left_all, 2)
    swap_own(2, True)
    gather_line(4, rows_all, 1)
    gather_side(2, rows_all, 0)
    gather_side(4, rows_all, 0)
    at_distance(1, column(2))
    swap_core(2, 1)
    for away in range(3, lines):
        swap_core(away, 0)
    gather_line(2, rows_all, 2)
    at_distance(1, column(4))
    for away in range(3, lines):
        gather_side(1, left_all, away)
        swap_own(away, True)
    gather_line(4, rows_all, 2)
    at_distance(0, across(2))
    gather_side(2, rows_all, 1)
    at_distance(0, across(4))
    for away in range(3, lines):
        swap_core(away, 1)
    a2a_wait(1, both_cols, early_rows)
    both_ready()

    tile = 256

    def early(i, carry):
        at = lanes(i * tile, tile)
        do_ref[at, :] = dot_of(
            left_all[:, :, at].reshape(count * high, tile), both_cols[...].reshape(count * high, piece), ((0,), (0,))
        )
        return carry
    lax.fori_loop(0, width // tile, early, 0)
    gather_side(4, rows_all, 1)
    at_distance(2, column(2))
    gather_side(2, rows_all, 2)
    for away in range(3, lines):
        gather_line(2, rows_all, away)
    at_distance(2, column(4))
    for away in range(3, lines):
        gather_line(4, rows_all, away)
    gather_finish(0, a_all)
    gather_finish(3, a_all)
    for away in range(3, lines):
        for number in (2, 4):
            at_distance(away, column(number))

    def swapped(slot, carry):
        swap_copy(slot).wait_recv()
        right_a[slot, :high] = (swap[slot].astype(F32) + swap_got[slot].astype(F32)).astype(BF)
        return carry
    lax.fori_loop(0, count, swapped, 0)

    def late_part(i, carry):
        at = lanes(i * tile, tile)
        do_ref[at, :] += dot_of(
            a_all[:, :, at].reshape(count * length, tile), right_a[...].reshape(count * length, piece), ((0,), (0,))
        )
        return carry
    lax.fori_loop(0, width // tile, late_part, 0)
    gather_side(4, rows_all, 2)
    for number in (2, 4):
        at_distance(1, across(number))
    for number in (2, 4):
        at_distance(2, across(number))
    for away in range(3, lines):
        gather_side(2, rows_all, away)
        gather_side(4, rows_all, away)
        at_distance(away, across(2))
        at_distance(away, across(4))

    cross_copy.wait_send()
    both_sent()
    remote(tg, tg, x_sem.at[near], x_sem.at[0], pair).wait_send()
    for number, (send, got) in enumerate(((part_0, got_0), (part_1, got_1), (part_2, got_2))):
        remote(send, got, part_sem.at[number], part_got.at[number, 0], pair).wait_send()
    remote(swap, swap_got, swap_sem.at[count], swap_sem.at[0], pair).wait_send()
    for number, array in enumerate((a_all, left_all, rows_all, a_all, rows_all)):
        gather_sent(number, array)


def one_kernel(inputs, targets, queries, key_rows, value_weight, output_weight, splits):
    count = lax.axis_size("task")
    lines = count // 4
    length, half = inputs.shape
    depth = 2 * half
    width = queries.shape[1]
    high = 3 * length // 4
    piece = depth // count
    vm = pltpu.VMEM
    dma = pltpu.SemaphoreType.DMA
    anywhere = pl.BlockSpec(memory_space=pl.ANY)
    chunks = 8
    return pl.pallas_call(
        functools.partial(step_kernel, lines),
        out_shape=(
            pltpu.VMEM((piece, width), F32),
            pltpu.VMEM((width, piece), F32),
        ),
        in_specs=[anywhere] * 6 + [pl.BlockSpec(memory_space=pltpu.SMEM)],
        out_specs=(pl.BlockSpec(memory_space=pltpu.VMEM), pl.BlockSpec(memory_space=pltpu.VMEM)),
        scratch_shapes=[
            vm((length, depth), BF),
            vm((length, half), BF),
            vm((length, width), BF),
            vm((length, width), BF),
            vm((depth, width), BF),
            vm((width, depth), BF),
        ]
        + [vm((length, width), BF)] * 7
        + [vm((length, width), F32)] * 2
        + [vm((length, length), F32)]
        + [vm((high, depth), BF)] * 6
        + [vm((length, depth), BF)] * 4
        + [vm((length, width), BF)]
        + [vm((length, length), BF)] * 4
        + [
            vm((length, width), F32),
            vm((high, width), BF),
            vm((count, length, width), BF),
            vm((count, high, width), BF),
            vm((count, length, width), BF),
            vm((count, length, piece), BF),
            vm((count, high, piece), BF),
            vm((count, length, piece), BF),
            vm((count, high, piece), BF),
            vm((count, high, piece), BF),
            dma((6,)),
            dma((chunks // 2 + 1,)),
            dma((3,)),
            dma((3, chunks)),
            dma((2,)),
            dma((count + 1,)),
            dma((6,)),
            dma((6,)),
            dma((5, 2)),
            dma((5, lines)),
            dma((5, lines)),
            dma((5, lines, 2)),
        ],
        compiler_params=pltpu.CompilerParams(
            collective_id=1, has_side_effects=True, vmem_limit_bytes=60 * 2**20
        ),
    )(inputs, targets, queries, key_rows, value_weight, output_weight, splits)


def make_device(tensor_count):
    def per_device(inputs, targets, queries, key_rows, value_weight, output_weight, splits):
        length = inputs.shape[0]
        low, high = length // 4, 3 * length // 4
        heads = queries.shape[1] // HD
        index = lax.axis_index("tensor")
        normed = normed_rows(full_rows(inputs, tensor_count, index))
        offset_here = inputs.astype(F32) - targets.astype(F32)
        offset = jnp.concatenate(
            [jnp.where(index == block, offset_here, F32(0.0)) for block in range(tensor_count)],
            axis=1,
        )
        probs = attention_probs(queries, key_rows, heads)
        probs_s = probs[:, :high, :high]
        probs_q = probs[:, low:, :]
        split = splits[0]
        count_s = split.astype(F32)
        position = jnp.arange(length)
        support = (position < split).astype(F32)[:, None]
        weight_s = (support / count_s)[:high]
        weight_q = ((1.0 - support) / (F32(length) - count_s))[low:]

        upper = mm(normed, value_weight).astype(BF)
        mixed_s = mix(probs_s, upper[:high]).astype(BF)
        gram = mm_nt(normed, normed).astype(BF)
        mixed_s_all = gather_tokens(mixed_s)
        part_0 = (mm(mixed_s, output_weight) + offset[:high]).astype(BF)
        part_0, normed_sent = lax.optimization_barrier((part_0, normed))
        normed_cols = my_columns(normed_sent)
        error_1 = (weight_s * group_sum(part_0, tensor_count)).astype(BF)

        back_u = mix_back(probs_s, mm_nt(error_1, output_weight).astype(BF)).astype(BF)
        upper_1 = (upper.astype(F32) - step_rate * mm(gram[:, :high], back_u)).astype(BF)
        mixed_q = mix(probs_q, upper_1).astype(BF)
        cross = (-step_rate * mm_nt(mixed_q, mixed_s)).astype(BF)
        part_1 = mm(mixed_q, output_weight) + mm(cross, error_1)
        part_1 = (part_1 + offset[low:]).astype(BF)
        error_2 = (weight_q * group_sum(part_1, tensor_count)).astype(BF)

        errors = (-step_rate * mm_nt(error_2, error_1)).astype(BF)
        back_z1 = (mm_nt(error_2, output_weight) + mm(errors, mixed_s)).astype(BF)
        back_u1 = mix_back(probs_q, back_z1)
        back_u1_b = back_u1.astype(BF)
        back_gram = (-step_rate * mm(gram[:high], back_u1_b)).astype(BF)
        second = mix(probs_s, back_gram).astype(BF)
        error_back = (mm(second, output_weight) + mm_tn(cross, error_2)).astype(BF)
        is_support = (position < split)[:, None]
        left = jnp.where(is_support, below(second, length), above(mixed_q, length))
        errors_both = jnp.where(is_support, below(error_1, length), above(error_2, length))
        error_back, normed_cols, errors_both, left = lax.optimization_barrier(
            (error_back, normed_cols, errors_both, left)
        )
        both_cols = my_columns(errors_both)
        left, mixed_s_all = lax.optimization_barrier((left, mixed_s_all))
        left_all = gather_tokens(left)
        error_sum = group_sum(error_back, tensor_count)
        error_3 = (weight_s * error_sum).astype(BF)
        error_3_cols = my_columns(error_3)

        back_z0 = (mm_nt(error_3, output_weight) + mm_tn(errors, mixed_q)).astype(BF)
        late = mix_back(probs_s, back_z0)
        value_rows = (back_u1 + jnp.pad(late, ((0, length - high), (0, 0)))).astype(BF)
        value_rows_all = gather_by_copies(value_rows, 1)
        total_output = (
            mm_tn(left_all, both_cols)
            + mm_tn(mixed_s_all, error_3_cols)
        )
        total_value = mm_tn(normed_cols, value_rows_all)
        return (total_value, total_output)

    return per_device


def solution(mesh):
    whole_step = mesh.shape["tensor"] == 2 and mesh.shape["task"] % 4 == 0
    return jax.shard_map(
        one_kernel if whole_step else make_device(mesh.shape["tensor"]),
        mesh=mesh,
        in_specs=(
            P("task", "tensor"),
            P("task", "tensor"),
            P("task", "tensor"),
            P("task", "tensor"),
            P(None, "tensor"),
            P("tensor", None),
            P("task"),
        ),
        out_specs=(P("task", "tensor"), P("tensor", "task")),
        check_vma=False,
    )
```

```python
import functools

import jax
import jax.numpy as jnp
from jax import lax
from jax.experimental import pallas as pl
from jax.experimental.pallas import tpu as pltpu
from jax.sharding import PartitionSpec as P

HD = 128
BF = jnp.bfloat16
F32 = jnp.float32

step_rate = 0.25


def normed_rows(inputs):
    values = inputs.astype(F32)
    scale = lax.rsqrt(jnp.mean(values * values, axis=-1, keepdims=True) + 1e-05)
    return (values * scale).astype(BF)


def attention_probs(queries, key_rows, heads):
    length = queries.shape[0]
    query_h = queries.reshape(length, heads, -1)
    key_h = key_rows.reshape(length, heads, -1)
    scores = jnp.einsum("ihd,jhd->hij", query_h, key_h, preferred_element_type=F32)
    scores = scores / jnp.sqrt(F32(query_h.shape[2]))
    position = jnp.arange(length)
    causal = position[:, None] >= position[None, :]
    scores = jnp.where(causal[None], scores, F32(-1e30))
    scores = scores - jnp.max(scores, axis=-1, keepdims=True)
    expo = jnp.exp(scores)
    return (expo / jnp.sum(expo, axis=-1, keepdims=True)).astype(BF)


def mm(left, right):
    return jnp.dot(left, right, preferred_element_type=F32)


def mm_nt(left, right):
    return lax.dot_general(left, right, (((1,), (1,)), ((), ())), preferred_element_type=F32)


def mm_tn(left, right):
    return lax.dot_general(left, right, (((0,), (0,)), ((), ())), preferred_element_type=F32)


def mix(probs, rows):
    heads = probs.shape[0]
    split = rows.reshape(rows.shape[0], heads, -1)
    out = jnp.einsum("hij,jhd->ihd", probs, split, preferred_element_type=F32)
    return out.reshape(out.shape[0], -1)


def mix_back(probs, rows):
    heads = probs.shape[0]
    split = rows.reshape(rows.shape[0], heads, -1)
    out = jnp.einsum("hij,ihd->jhd", probs, split, preferred_element_type=F32)
    return out.reshape(out.shape[0], -1)


def group_sum(term, count):
    term = term.astype(BF)
    if count == 1:
        return term.astype(F32)
    if count == 2:
        other = lax.ppermute(term, "tensor", ((0, 1), (1, 0)))
        return term.astype(F32) + other.astype(F32)
    share = lax.psum_scatter(term, "tensor", scatter_dimension=1, tiled=True)
    return lax.all_gather(share, "tensor", axis=1, tiled=True).astype(F32)


def full_rows(inputs, count, index):
    if count != 2:
        return lax.all_gather(inputs, "tensor", axis=1, tiled=True)
    other = lax.ppermute(inputs, "tensor", ((0, 1), (1, 0)))
    low = jnp.where(index == 0, inputs, other)
    high = jnp.where(index == 0, other, inputs)
    return jnp.concatenate([low, high], axis=1)


def gather_kernel(lines, src_ref, out_ref, own_sem, send_sem, line_sem, side_sem, core_sem):
    me = lax.axis_index("task")
    core, side, line = lax.rem(me, 2), lax.rem(me // 2, 2), me // 4

    def place(back, over_side, over_core):
        line_from = lax.rem(line + lines - back, lines)
        side_from = 1 - side if over_side else side
        core_from = 1 - core if over_core else core
        return (line_from * 2 + side_from) * 2 + core_from

    side_peer, core_peer = place(0, True, False), place(0, False, True)
    peers = [place(lines - step, False, False) for step in range(1, lines)] + [side_peer, core_peer]
    barrier = pltpu.get_barrier_semaphore()
    for peer in peers:
        pl.semaphore_signal(
            barrier, inc=1, device_id={"task": peer}, device_id_type=pl.DeviceIdType.MESH
        )
    pl.semaphore_wait(barrier, len(peers))

    started = []

    def send(source, slot, arrival, peer):
        copy = pltpu.make_async_remote_copy(
            src_ref=source,
            dst_ref=out_ref.at[slot],
            send_sem=send_sem.at[len(started)],
            recv_sem=arrival,
            device_id={"task": peer},
            device_id_type=pl.DeviceIdType.MESH,
        )
        copy.start()
        started.append(copy)

    def arrived(slot, arrival, peer):
        pltpu.make_async_remote_copy(
            src_ref=out_ref.at[slot],
            dst_ref=out_ref.at[slot],
            send_sem=send_sem.at[0],
            recv_sem=arrival,
            device_id={"task": peer},
            device_id_type=pl.DeviceIdType.MESH,
        ).wait_recv()

    for step in sorted(range(1, lines), key=lambda step: -min(step, lines - step)):
        send(src_ref, me, line_sem.at[step], peers[step - 1])
    send(src_ref, me, side_sem.at[0], side_peer)
    send(src_ref, me, core_sem.at[0, 0], core_peer)
    own = pltpu.make_async_copy(src_ref, out_ref.at[me], own_sem)
    own.start()
    order = sorted(range(1, lines), key=lambda step: min(step, lines - step))
    for step in order:
        slot = place(step, False, False)
        arrived(slot, line_sem.at[step], side_peer)
        send(out_ref.at[slot], slot, side_sem.at[step], side_peer)
        send(out_ref.at[slot], slot, core_sem.at[step, 0], core_peer)
    for step in [0] + order:
        slot = place(step, True, False)
        arrived(slot, side_sem.at[step], side_peer)
        send(out_ref.at[slot], slot, core_sem.at[step, 1], core_peer)
    for step in [0] + order:
        for over in range(2):
            arrived(place(step, over == 1, True), core_sem.at[step, over], core_peer)
    own.wait()
    for copy in started:
        copy.wait_send()


def gather_by_copies(rows, number):
    count = lax.axis_size("task")
    if count % 4:
        return gather_tokens(rows)
    lines = count // 4
    sends = (lines + 1) + 2 * (lines - 1) + lines
    gathered = pl.pallas_call(
        functools.partial(gather_kernel, lines),
        out_shape=jax.ShapeDtypeStruct((count,) + rows.shape, rows.dtype),
        in_specs=[pl.BlockSpec(memory_space=pltpu.VMEM)],
        out_specs=pl.BlockSpec(memory_space=pltpu.VMEM),
        scratch_shapes=[
            pltpu.SemaphoreType.DMA,
            pltpu.SemaphoreType.DMA((sends,)),
            pltpu.SemaphoreType.DMA((lines,)),
            pltpu.SemaphoreType.DMA((lines,)),
            pltpu.SemaphoreType.DMA((lines, 2)),
        ],
        compiler_params=pltpu.CompilerParams(collective_id=number, has_side_effects=True),
        cost_estimate=pl.CostEstimate(
            flops=0, bytes_accessed=16 * rows.size * rows.dtype.itemsize * count, transcendentals=0
        ),
    )(rows)
    return gathered.reshape(count * rows.shape[0], rows.shape[1])


def gather_tokens(rows):
    return lax.all_gather(rows, "task", axis=0, tiled=True)


def my_columns(rows):
    return lax.all_to_all(rows, "task", split_axis=1, concat_axis=0, tiled=True)


def below(rows, length):
    return jnp.pad(rows, ((0, length - rows.shape[0]), (0, 0)))


def above(rows, length):
    return jnp.pad(rows, ((length - rows.shape[0], 0), (0, 0)))


MESH = pl.DeviceIdType.MESH


def dot_of(left, right, dims):
    return lax.dot_general(left, right, (dims, ((), ())), preferred_element_type=F32)


def step_kernel(
    lines,
    x_in, t_in, q_in, k_in, v_in, o_in, split_ref,
    dv_ref, do_ref,
    xf, tg, qs, ks, vw, ow, probs, probs_t, upper, mixq, second, left, chain, mixed_all, acc, half_acc,
    part_0, part_1, part_2, got_0, got_1, got_2, err_1, err_2, err_3, both,
    back, gram_b, cross, cross_got, pairs, value_now, z_mine, a_all, left_all, rows_all,
    x_cols, both_cols, right_a, swap, swap_got,
    load_sem, x_sem, part_sem, part_got, cross_sem, swap_sem,
    a2a_send, a2a_got, g_send, g_line, g_side, g_core,
):
    count = lines * 4
    length, depth = xf.shape
    half = depth // 2
    width = upper.shape[1]
    heads = width // HD
    low, high = length // 4, 3 * length // 4
    piece = depth // count
    chunks = 8
    cut = depth // chunks
    near = chunks // 2
    fine = 2 * near
    thin = half // fine

    me = lax.axis_index("task")
    mine = lax.axis_index("tensor")
    core, side, line = lax.rem(me, 2), lax.rem(me // 2, 2), me // 4
    pair = {"tensor": 1 - mine}

    def place(line_at, side_at, core_at):
        return (line_at * 2 + side_at) * 2 + core_at

    def lanes(start, size):
        return pl.ds(pl.multiple_of(start, 128), size)

    own_half = lanes(mine * half, half)
    loads = [
        pltpu.make_async_copy(x_in, xf.at[:, own_half], load_sem.at[0]),
        pltpu.make_async_copy(q_in, qs, load_sem.at[1]),
        pltpu.make_async_copy(k_in, ks, load_sem.at[2]),
        pltpu.make_async_copy(v_in, vw, load_sem.at[3]),
        pltpu.make_async_copy(t_in, tg, load_sem.at[4]),
        pltpu.make_async_copy(o_in, ow, load_sem.at[5]),
    ]
    for load in loads:
        load.start()

    barrier = pltpu.get_barrier_semaphore()
    for step in range(1, count):
        pl.semaphore_signal(
            barrier, inc=1, device_id={"task": lax.rem(me + step, count)}, device_id_type=MESH
        )
    pl.semaphore_signal(barrier, inc=1, device_id=pair, device_id_type=MESH)
    pl.semaphore_wait(barrier, count)

    def remote(src, dst, send, got, peer):
        return pltpu.make_async_remote_copy(
            src_ref=src, dst_ref=dst, send_sem=send, recv_sem=got, device_id=peer, device_id_type=MESH
        )

    def x_copy(k, owner):
        part = xf.at[:, lanes(owner * half + k * thin, thin)]
        return remote(part, part, x_sem.at[fine], x_sem.at[k], pair)

    loads[0].wait()
    for k in range(fine):
        x_copy(k, mine).start()

    def a2a_copy(number, src, dst, rows, step):
        peer = lax.rem(me + step, count)
        return remote(
            src.at[rows, lanes(peer * piece, piece)],
            dst.at[me, rows],
            a2a_send.at[number],
            a2a_got.at[number],
            {"task": peer},
        )

    def a2a_start(number, src, dst, rows, first=1, last=count):
        def one(step, carry):
            a2a_copy(number, src, dst, rows, step).start()
            return carry
        lax.fori_loop(first, last, one, 0)

    def a2a_wait(number, dst, rows):
        arrived = dst.at[pl.ds(0, count - 1), rows]
        remote(arrived, arrived, a2a_send.at[number], a2a_got.at[number], {"task": lax.rem(me + 1, count)}).wait()

    all_rows = pl.ds(0, length)

    def x_spread(owner, first, last):
        def one(index, carry):
            step = lax.rem(owner * (count // 2) + index + count - me, count)
            @pl.when(step > 0)
            def _():
                a2a_copy(0, xf, x_cols, all_rows, step).start()
            return carry
        lax.fori_loop(first, last, one, 0)

    x_spread(mine, 0, count // 2)

    part_rows = (pl.ds(0, high), pl.ds(0, high), all_rows, pl.ds(high, length - high), all_rows)
    part_lanes = (pl.ds(0, width),) * 2 + (pl.ds(0, width // 2), pl.ds(0, width), pl.ds(width // 2, width // 2))

    def gather_copy(number, array, slot, kind, source, got, peer):
        block = array.at[slot, part_rows[number], part_lanes[number]]
        return remote(block, block, g_send.at[number, 0 if kind < 2 else 1], got, {"task": peer})

    def from_end(number, source, away):
        if number in (1, 4) and lines > 2 and away == 2:
            return jnp.logical_or(source == 0, source == lines - 1)
        return None

    def detour(number, away):
        return number == 2 and lines > 2 and away == lines - 1

    up_peer, down_peer = me + 4, me - 4
    side_peer, core_peer = place(line, 1 - side, core), place(line, side, 1 - core)

    def pass_on(number, array, source, away):
        slot = place(source, side, core)
        if not detour(number, away):
            through = from_end(number, source, away)
            @pl.when(True if through is None else jnp.logical_not(through))
            def _():
                gather_copy(number, array, slot, 2, source, g_side.at[number, source], side_peer).start()
        @pl.when(jnp.logical_and(source <= line, line < lines - 1))
        def _():
            gather_copy(number, array, slot, 0, source, g_line.at[number, source], up_peer).start()
        @pl.when(jnp.logical_and(source >= line, line > 0))
        def _():
            gather_copy(number, array, slot, 1, source, g_line.at[number, source], down_peer).start()
        gather_copy(number, array, slot, 3, source, g_core.at[number, source, 0], core_peer).start()

    def gather_start(number, array):
        pass_on(number, array, line, 0)

    def at_distance(away, take):
        if away == 0:
            take(line)
            return
        @pl.when(line >= away)
        def _():
            take(line - away)
        @pl.when(line + away < lines)
        def _():
            take(line + away)

    def gather_line(number, array, away):
        def take(source):
            slot = place(source, side, core)
            gather_copy(number, array, slot, 2, source, g_line.at[number, source], side_peer).wait_recv()
            pass_on(number, array, source, away)
        at_distance(away, take)

    def gather_side(number, array, away):
        def take(source):
            slot = place(source, 1 - side, core)
            gather_copy(number, array, slot, 4, source, g_side.at[number, source], core_peer).wait_recv()
            gather_copy(number, array, slot, 4, source, g_core.at[number, source, 1], core_peer).start()
            through = from_end(number, source, away + 1)
            if detour(number, away + 1) or through is not None:
                through = True if through is None else through
                @pl.when(functools.reduce(jnp.logical_and, (source < line, line < lines - 1, through)))
                def _():
                    gather_copy(number, array, slot, 4, source, g_side.at[number, source], up_peer).start()
                @pl.when(functools.reduce(jnp.logical_and, (source > line, line > 0, through)))
                def _():
                    gather_copy(number, array, slot, 4, source, g_side.at[number, source], down_peer).start()
        at_distance(away, take)

    def gather_sides(number, array):
        for away in range(lines):
            gather_side(number, array, away)

    def gather_core(number, array, source, over):
        slot = place(source, side if over == 0 else 1 - side, 1 - core)
        gather_copy(number, array, slot, 3, source, g_core.at[number, source, over], core_peer).wait_recv()

    def gather_finish(number, array):
        for source in range(lines):
            for over in range(2):
                gather_core(number, array, source, over)

    def gather_sent(number, array):
        def sent(blocks, which):
            group = array.at[pl.ds(0, blocks), part_rows[number], part_lanes[number]]
            remote(group, group, g_send.at[number, which], g_core.at[number, 0, 0], {"task": core_peer}).wait_send()
        for at in range(lines):
            ups = at + 1 if at < lines - 1 else 0
            downs = lines - at if at > 0 else 0
            others = 3 * lines
            if detour(number, lines - 1):
                ends = (at == 0) + (at == lines - 1)
                inner = (at == lines - 2) + (at == 1)
                others += inner - ends
            if number in (1, 4) and lines > 2:
                others += (at == 1) + (at == lines - 2) - (at == 2) - (at == lines - 3)
            @pl.when(line == at)
            def _():
                sent(ups + downs, 0)
                sent(others, 1)

    def head(h):
        return slice(h * HD, (h + 1) * HD)

    row = lax.broadcasted_iota(jnp.int32, (length, length), 0)
    col = lax.broadcasted_iota(jnp.int32, (length, length), 1)
    causal = row >= col
    loads[1].wait()
    loads[2].wait()
    root = jnp.sqrt(F32(HD))
    for h in range(heads):
        scores = dot_of(qs[:, head(h)], ks[:, head(h)], ((1,), (1,))) / root
        scores = jnp.where(causal, scores, F32(-1e30))
        scores = scores - jnp.max(scores, axis=-1, keepdims=True)
        expo = jnp.exp(scores)
        prob = expo / jnp.sum(expo, axis=-1, keepdims=True)
        probs[:, head(h)] = prob.astype(BF)
        probs_t[:, head(h)] = prob.T.astype(BF)

    err_1[high:, :] = jnp.zeros((length - high, depth), BF)
    err_2[:low, :] = jnp.zeros((low, depth), BF)
    err_3[high:, :] = jnp.zeros((length - high, depth), BF)
    position = lax.broadcasted_iota(jnp.int32, (length, 1), 0)
    split = jnp.full((length, 1), split_ref[0], jnp.int32)
    is_support = position < split
    support = is_support.astype(F32)
    count_s = split.astype(F32)
    weight_s = support / count_s
    weight_q = (1.0 - support) / (F32(length) - count_s)

    loads[3].wait()

    def take(k, owner, first):
        at = lanes(owner * half + k * thin, thin)
        x_part = xf[:, at]
        new = dot_of(x_part, vw[pl.ds(pl.multiple_of(owner * half + k * thin, 128), thin), :], ((1,), (0,)))
        gram = dot_of(x_part, x_part, ((1,), (1,)))
        if first:
            acc[...] = new
            half_acc[...] = gram
        else:
            acc[...] += new
            half_acc[...] += gram

    take(0, mine, True)
    def own_take(k, carry):
        take(k, mine, False)
        return carry
    lax.fori_loop(1, fine, own_take, 0)
    def other_take(k, carry):
        x_copy(k, 1 - mine).wait_recv()
        each = count // 2 // fine
        x_spread(1 - mine, each * k, each * (k + 1))
        take(k, 1 - mine, False)
        return carry
    lax.fori_loop(0, fine, other_take, 0)

    gram_raw = half_acc[...]
    diagonal = jnp.where(row == col, gram_raw, F32(0.0))
    scale_row = lax.rsqrt(jnp.sum(diagonal, axis=1, keepdims=True) / F32(depth) + 1e-05)
    scale_col = lax.rsqrt(jnp.sum(diagonal, axis=0, keepdims=True) / F32(depth) + 1e-05)
    gram_b[...] = (gram_raw * scale_row * scale_col).astype(BF)
    upper[...] = (acc[...] * scale_row).astype(BF)

    a_mine = a_all.at[me]
    for h in range(heads):
        mixed = dot_of(probs[:, head(h)], upper[:, head(h)], ((1,), (0,)))
        mixed_all[:, head(h)] = mixed
        z_mine[:, head(h)] = mixed[:high].astype(BF)
    a_mine[:high, :] = (weight_s[:high] * z_mine[...].astype(F32)).astype(BF)
    gather_start(0, a_all)
    loads[4].wait()
    loads[5].wait()

    def part_copy(number, send, got, k, owner):
        at = lanes(lax.rem(owner * near + k, chunks) * cut, cut)
        return remote(send.at[:, at], got.at[:, at], part_sem.at[number], part_got.at[number, k], pair)

    def own_columns(k):
        return lanes(lax.rem(mine * near + k, chunks) * cut, cut)

    def other_columns(k):
        return lanes(lax.rem((1 - mine) * near + k, chunks) * cut, cut)

    def offset(k, rows):
        there = lanes(k * cut, cut)
        return xf[rows, own_columns(k)].astype(F32) - tg[rows, there].astype(F32)

    def send_parts(number, value, rows, send, got, with_offset):
        def one(k, near_half):
            at = own_columns(k)
            part = value(at)
            if near_half and with_offset:
                part = part + offset(k, rows)
            send[:, at] = part.astype(BF)
            part_copy(number, send, got, k, mine).start()
        def first(k, carry):
            one(k, True)
            return carry
        def later(k, carry):
            one(k, False)
            return carry
        lax.fori_loop(0, near, first, 0)
        lax.fori_loop(near, chunks, later, 0)

    def take_parts(number, send, got, rows, weight, error, also, first=0, last=chunks):
        def one(k, carry):
            at = other_columns(k)
            part_copy(number, send, got, k, 1 - mine).wait_recv()
            total = send[:, at].astype(F32) + got[:, at].astype(F32)
            error[rows, at] = (weight[rows] * total).astype(BF)
            part = error[:, at]
            acc[...] += dot_of(part, ow[:, at], ((1,), (1,)))
            also(at, part)
            return carry
        lax.fori_loop(first, last, one, 0)

    support_rows, query_rows = slice(0, high), slice(low, length)
    nothing = lambda at, part: None

    def value_0(at):
        return dot_of(z_mine[...], ow[:, at], ((1,), (0,)))

    early_rows, middle_rows, late_rows = pl.ds(0, low), pl.ds(low, high - low), pl.ds(high, length - high)
    acc[...] = jnp.zeros_like(acc)
    send_parts(0, value_0, support_rows, part_0, got_0, True)
    for h in range(heads):
        middle = dot_of(probs[:, head(h)], gram_b[...], ((1,), (0,))).astype(BF)
        chain[:, head(h)] = (-step_rate * dot_of(middle, probs_t[:, head(h)], ((1,), (0,)))).astype(BF)
    take_parts(0, part_0, got_0, support_rows, weight_s, err_1, nothing, 0, 6)
    gather_line(0, a_all, 1)
    take_parts(0, part_0, got_0, support_rows, weight_s, err_1, nothing, 6, chunks)
    a2a_start(1, err_1, both_cols, early_rows)

    back[...] = acc[...].astype(BF)
    for h in range(heads):
        moved = dot_of(chain[:, head(h)], back[:, head(h)], ((1,), (0,)))
        mixq[:, head(h)] = (mixed_all[:, head(h)] + moved).astype(BF)
    cross[:, high:] = jnp.zeros((length, length - high), BF)
    product = -step_rate * dot_of(mixq[...], z_mine[...], ((1,), (1,)))
    cross[:, :high] = jnp.where(is_support, F32(0.0), product).astype(BF)
    cross_copy = remote(cross, cross_got, cross_sem.at[0], cross_sem.at[1], pair)
    cross_copy.start()

    def value_1(at):
        part = dot_of(mixq[...], ow[:, at], ((1,), (0,))) + dot_of(cross[:, :high], err_1[:high, at], ((1,), (0,)))
        return part[low:]

    half_acc[...] = jnp.zeros_like(half_acc)
    acc[...] = jnp.zeros_like(acc)

    def pairs_of(at, part):
        half_acc[...] += dot_of(part, err_1[:, at], ((1,), (1,)))

    send_parts(1, value_1, query_rows, part_1, got_1, True)
    gather_line(0, a_all, 2)
    cross_copy.wait_recv()
    cross_sum = (cross[...].astype(F32) + cross_got[...].astype(F32)).astype(BF)
    left[...] = (mixq[...].astype(F32) + dot_of(cross_sum[:, :high], a_mine[:high], ((1,), (0,)))).astype(BF)
    a_mine[high:, :] = left[high:, :]
    gather_start(3, a_all)
    take_parts(1, part_1, got_1, query_rows, weight_q, err_2, pairs_of, 0, 3)
    for away in range(3, lines):
        gather_line(0, a_all, away)
    take_parts(1, part_1, got_1, query_rows, weight_q, err_2, pairs_of, 3, 5)
    gather_line(3, a_all, 1)
    take_parts(1, part_1, got_1, query_rows, weight_q, err_2, pairs_of, 5, 7)
    gather_sides(0, a_all)
    take_parts(1, part_1, got_1, query_rows, weight_q, err_2, pairs_of, 7, chunks)
    gather_line(3, a_all, 2)

    pairs[...] = (-step_rate * half_acc[...]).astype(BF)
    back[...] = (acc[...] + dot_of(pairs[:, :high], z_mine[...], ((1,), (0,)))).astype(BF)
    left_mine = left_all.at[me]
    for h in range(heads):
        again = dot_of(chain[:, head(h)], back[:, head(h)], ((1,), (0,))).astype(BF)
        second[:, head(h)] = again
        left_mine[:, head(h)] = jnp.where(is_support, again, left[:, head(h)])[:high]

    def value_2(at):
        part = dot_of(second[...], ow[:, at], ((1,), (0,))) + dot_of(cross[...], err_2[:, at], ((0,), (0,)))
        return part[:high]

    acc[...] = jnp.zeros_like(acc)
    gather_start(1, left_all)
    send_parts(2, value_2, support_rows, part_2, got_2, False)

    for h in range(heads):
        value_now[:, head(h)] = dot_of(probs_t[:, head(h)], back[:, head(h)], ((1,), (0,)))
    def join(k, carry):
        at = own_columns(k)
        both[:, at] = jnp.where(is_support, err_1[:, at], err_2[:, at])
        return carry
    lax.fori_loop(0, chunks, join, 0)
    keeper = core == mine

    def both_start(first, last):
        def one(index, carry):
            step = 2 * index + lax.rem(core + mine, 2)
            @pl.when(step > 0)
            def _():
                a2a_copy(2, both, both_cols, middle_rows, step).start()
                a2a_copy(3, both, right_a, late_rows, step).start()
            return carry
        lax.fori_loop(first, last, one, 0)

    def both_moved(number, array, rows, slots):
        group = array.at[pl.ds(0, slots), rows]
        return remote(group, group, a2a_send.at[number], a2a_got.at[number], pair)

    both_arrays = ((2, both_cols, middle_rows), (3, right_a, late_rows))

    def both_forward():
        @pl.when(keeper)
        def _():
            both_cols[me, middle_rows] = both[middle_rows, lanes(me * piece, piece)]
            right_a[me, late_rows] = both[late_rows, lanes(me * piece, piece)]
            for number, array, rows in both_arrays:
                both_moved(number, array, rows, count - 1).wait_recv()
                both_moved(number + 2, array, rows, count).start()

    def both_ready():
        @pl.when(jnp.logical_not(keeper))
        def _():
            for number, array, rows in both_arrays:
                both_moved(number + 2, array, rows, count).wait_recv()

    def both_sent():
        @pl.when(keeper)
        def _():
            for number, array, rows in both_arrays:
                both_moved(number, array, rows, count // 2 - 1).wait_send()
                both_moved(number + 2, array, rows, count).wait_send()
        @pl.when(jnp.logical_not(keeper))
        def _():
            for number, array, rows in both_arrays:
                both_moved(number, array, rows, count // 2).wait_send()

    def swap_copy(slot):
        return remote(swap.at[slot], swap_got.at[slot], swap_sem.at[0], swap_sem.at[1], pair)

    def swap_one(slot):
        swap[slot] = dot_of(left_all[slot], ow[:, lanes(me * piece, piece)], ((1,), (0,))).astype(BF)
        swap_copy(slot).start()

    def swap_own(away, over_side):
        at_distance(away, lambda source: swap_one(place(source, 1 - side if over_side else side, core)))

    def swap_core(away, over):
        def one(source):
            gather_core(1, left_all, source, over)
            swap_one(place(source, 1 - side if over else side, 1 - core))
        at_distance(away, one)

    def take_2(first, last):
        take_parts(2, part_2, got_2, support_rows, weight_s, err_3, nothing, first, last)

    both_start(0, count // 2)
    take_2(0, 1)
    for away in range(3, lines):
        gather_line(3, a_all, away)
    swap_own(0, False)
    take_2(1, 2)
    gather_line(1, left_all, 1)
    swap_own(1, False)
    take_2(2, 3)
    gather_side(1, left_all, 0)
    swap_own(0, True)
    take_2(3, 4)
    gather_sides(3, a_all)
    swap_core(0, 0)
    swap_core(1, 0)
    take_2(4, 5)
    gather_line(1, left_all, 2)
    swap_own(2, False)
    take_2(5, 7)
    gather_side(1, left_all, 1)
    swap_own(1, True)
    take_2(7, chunks)

    back[...] = (acc[...] + dot_of(pairs[...], mixq[...], ((0,), (0,)))).astype(BF)
    rows_mine = rows_all.at[me]
    for h in range(heads):
        late = dot_of(probs_t[:, head(h)], back[:, head(h)], ((1,), (0,)))
        rows_mine[:, head(h)] = ((value_now[:, head(h)] + late) * scale_row).astype(BF)
    gather_start(2, rows_all)
    gather_start(4, rows_all)
    swap_core(0, 1)
    swap_core(2, 0)
    both_forward()
    for away in range(3, lines):
        gather_line(1, left_all, away)
        swap_own(away, False)
    swap_core(1, 1)

    x_cols[me] = xf[:, lanes(me * piece, piece)]
    both_cols[me, early_rows] = both[early_rows, lanes(me * piece, piece)]

    def add_pair(number, source, side_at):
        both_cores = pl.ds(place(source, side_at, 0), 2)
        return dot_of(
            x_cols[both_cores].reshape(2 * length, piece),
            rows_all[both_cores, :, part_lanes[number]].reshape(2 * length, width // 2),
            ((0,), (0,)),
        )

    def column(number):
        def one(source):
            gather_core(number, rows_all, source, 0)
            dv_ref[:, part_lanes[number]] += add_pair(number, source, side)
        return one

    def across(number):
        def one(source):
            gather_core(number, rows_all, source, 1)
            dv_ref[:, part_lanes[number]] += add_pair(number, source, 1 - side)
        return one

    a2a_wait(0, x_cols, all_rows)
    gather_line(2, rows_all, 1)
    for number in (2, 4):
        gather_core(number, rows_all, line, 0)
        dv_ref[:, part_lanes[number]] = add_pair(number, line, side)
    gather_side(1, left_all, 2)
    swap_own(2, True)
    gather_line(4, rows_all, 1)
    gather_side(2, rows_all, 0)
    gather_side(4, rows_all, 0)
    at_distance(1, column(2))
    swap_core(2, 1)
    for away in range(3, lines):
        swap_core(away, 0)
    gather_line(2, rows_all, 2)
    at_distance(1, column(4))
    for away in range(3, lines):
        gather_side(1, left_all, away)
        swap_own(away, True)
    gather_line(4, rows_all, 2)
    at_distance(0, across(2))
    gather_side(2, rows_all, 1)
    at_distance(0, across(4))
    for away in range(3, lines):
        swap_core(away, 1)
    a2a_wait(1, both_cols, early_rows)
    both_ready()

    tile = 256

    def early(i, carry):
        at = lanes(i * tile, tile)
        do_ref[at, :] = dot_of(
            left_all[:, :, at].reshape(count * high, tile), both_cols[...].reshape(count * high, piece), ((0,), (0,))
        )
        return carry
    lax.fori_loop(0, width // tile, early, 0)
    gather_side(4, rows_all, 1)
    at_distance(2, column(2))
    gather_side(2, rows_all, 2)
    for away in range(3, lines):
        gather_line(2, rows_all, away)
    at_distance(2, column(4))
    for away in range(3, lines):
        gather_line(4, rows_all, away)
    gather_finish(0, a_all)
    gather_finish(3, a_all)
    for away in range(3, lines):
        for number in (2, 4):
            at_distance(away, column(number))

    swaps = remote(swap, swap_got, swap_sem.at[0], swap_sem.at[1], pair)
    swaps.wait_recv()

    def swapped(slot, carry):
        right_a[slot, :high] = (swap[slot].astype(F32) + swap_got[slot].astype(F32)).astype(BF)
        return carry
    lax.fori_loop(0, count, swapped, 0)

    def late_part(i, carry):
        at = lanes(i * tile, tile)
        do_ref[at, :] += dot_of(
            a_all[:, :, at].reshape(count * length, tile), right_a[...].reshape(count * length, piece), ((0,), (0,))
        )
        return carry
    lax.fori_loop(0, width // tile, late_part, 0)
    gather_side(4, rows_all, 2)
    for number in (2, 4):
        at_distance(1, across(number))
    for number in (2, 4):
        at_distance(2, across(number))
    for away in range(3, lines):
        gather_side(2, rows_all, away)
        gather_side(4, rows_all, away)
        at_distance(away, across(2))
        at_distance(away, across(4))

    cross_copy.wait_send()
    both_sent()
    remote(tg, tg, x_sem.at[fine], x_sem.at[0], pair).wait_send()
    for number, (send, got) in enumerate(((part_0, got_0), (part_1, got_1), (part_2, got_2))):
        remote(send, got, part_sem.at[number], part_got.at[number, 0], pair).wait_send()
    swaps.wait_send()
    for number, array in enumerate((a_all, left_all, rows_all, a_all, rows_all)):
        gather_sent(number, array)


def one_kernel(inputs, targets, queries, key_rows, value_weight, output_weight, splits):
    count = lax.axis_size("task")
    lines = count // 4
    length, half = inputs.shape
    depth = 2 * half
    width = queries.shape[1]
    high = 3 * length // 4
    piece = depth // count
    vm = pltpu.VMEM
    dma = pltpu.SemaphoreType.DMA
    anywhere = pl.BlockSpec(memory_space=pl.ANY)
    chunks = 8
    return pl.pallas_call(
        functools.partial(step_kernel, lines),
        out_shape=(
            pltpu.VMEM((piece, width), F32),
            pltpu.VMEM((width, piece), F32),
        ),
        in_specs=[anywhere] * 6 + [pl.BlockSpec(memory_space=pltpu.SMEM)],
        out_specs=(pl.BlockSpec(memory_space=pltpu.VMEM), pl.BlockSpec(memory_space=pltpu.VMEM)),
        scratch_shapes=[
            vm((length, depth), BF),
            vm((length, half), BF),
            vm((length, width), BF),
            vm((length, width), BF),
            vm((depth, width), BF),
            vm((width, depth), BF),
        ]
        + [vm((length, width), BF)] * 7
        + [vm((length, width), F32)] * 2
        + [vm((length, length), F32)]
        + [vm((high, depth), BF)] * 6
        + [vm((length, depth), BF)] * 4
        + [vm((length, width), BF)]
        + [vm((length, length), BF)] * 4
        + [
            vm((length, width), F32),
            vm((high, width), BF),
            vm((count, length, width), BF),
            vm((count, high, width), BF),
            vm((count, length, width), BF),
            vm((count, length, piece), BF),
            vm((count, high, piece), BF),
            vm((count, length, piece), BF),
            vm((count, high, piece), BF),
            vm((count, high, piece), BF),
            dma((6,)),
            dma((chunks + 1,)),
            dma((3,)),
            dma((3, chunks)),
            dma((2,)),
            dma((2,)),
            dma((6,)),
            dma((6,)),
            dma((5, 2)),
            dma((5, lines)),
            dma((5, lines)),
            dma((5, lines, 2)),
        ],
        compiler_params=pltpu.CompilerParams(
            collective_id=1, has_side_effects=True, vmem_limit_bytes=60 * 2**20
        ),
    )(inputs, targets, queries, key_rows, value_weight, output_weight, splits)


def make_device(tensor_count):
    def per_device(inputs, targets, queries, key_rows, value_weight, output_weight, splits):
        length = inputs.shape[0]
        low, high = length // 4, 3 * length // 4
        heads = queries.shape[1] // HD
        index = lax.axis_index("tensor")
        normed = normed_rows(full_rows(inputs, tensor_count, index))
        offset_here = inputs.astype(F32) - targets.astype(F32)
        offset = jnp.concatenate(
            [jnp.where(index == block, offset_here, F32(0.0)) for block in range(tensor_count)],
            axis=1,
        )
        probs = attention_probs(queries, key_rows, heads)
        probs_s = probs[:, :high, :high]
        probs_q = probs[:, low:, :]
        split = splits[0]
        count_s = split.astype(F32)
        position = jnp.arange(length)
        support = (position < split).astype(F32)[:, None]
        weight_s = (support / count_s)[:high]
        weight_q = ((1.0 - support) / (F32(length) - count_s))[low:]

        upper = mm(normed, value_weight).astype(BF)
        mixed_s = mix(probs_s, upper[:high]).astype(BF)
        gram = mm_nt(normed, normed).astype(BF)
        mixed_s_all = gather_tokens(mixed_s)
        part_0 = (mm(mixed_s, output_weight) + offset[:high]).astype(BF)
        part_0, normed_sent = lax.optimization_barrier((part_0, normed))
        normed_cols = my_columns(normed_sent)
        error_1 = (weight_s * group_sum(part_0, tensor_count)).astype(BF)

        back_u = mix_back(probs_s, mm_nt(error_1, output_weight).astype(BF)).astype(BF)
        upper_1 = (upper.astype(F32) - step_rate * mm(gram[:, :high], back_u)).astype(BF)
        mixed_q = mix(probs_q, upper_1).astype(BF)
        cross = (-step_rate * mm_nt(mixed_q, mixed_s)).astype(BF)
        part_1 = mm(mixed_q, output_weight) + mm(cross, error_1)
        part_1 = (part_1 + offset[low:]).astype(BF)
        error_2 = (weight_q * group_sum(part_1, tensor_count)).astype(BF)

        errors = (-step_rate * mm_nt(error_2, error_1)).astype(BF)
        back_z1 = (mm_nt(error_2, output_weight) + mm(errors, mixed_s)).astype(BF)
        back_u1 = mix_back(probs_q, back_z1)
        back_u1_b = back_u1.astype(BF)
        back_gram = (-step_rate * mm(gram[:high], back_u1_b)).astype(BF)
        second = mix(probs_s, back_gram).astype(BF)
        error_back = (mm(second, output_weight) + mm_tn(cross, error_2)).astype(BF)
        is_support = (position < split)[:, None]
        left = jnp.where(is_support, below(second, length), above(mixed_q, length))
        errors_both = jnp.where(is_support, below(error_1, length), above(error_2, length))
        error_back, normed_cols, errors_both, left = lax.optimization_barrier(
            (error_back, normed_cols, errors_both, left)
        )
        both_cols = my_columns(errors_both)
        left, mixed_s_all = lax.optimization_barrier((left, mixed_s_all))
        left_all = gather_tokens(left)
        error_sum = group_sum(error_back, tensor_count)
        error_3 = (weight_s * error_sum).astype(BF)
        error_3_cols = my_columns(error_3)

        back_z0 = (mm_nt(error_3, output_weight) + mm_tn(errors, mixed_q)).astype(BF)
        late = mix_back(probs_s, back_z0)
        value_rows = (back_u1 + jnp.pad(late, ((0, length - high), (0, 0)))).astype(BF)
        value_rows_all = gather_by_copies(value_rows, 1)
        total_output = (
            mm_tn(left_all, both_cols)
            + mm_tn(mixed_s_all, error_3_cols)
        )
        total_value = mm_tn(normed_cols, value_rows_all)
        return (total_value, total_output)

    return per_device


def solution(mesh):
    whole_step = mesh.shape["tensor"] == 2 and mesh.shape["task"] % 16 == 0
    return jax.shard_map(
        one_kernel if whole_step else make_device(mesh.shape["tensor"]),
        mesh=mesh,
        in_specs=(
            P("task", "tensor"),
            P("task", "tensor"),
            P("task", "tensor"),
            P("task", "tensor"),
            P(None, "tensor"),
            P("tensor", None),
            P("task"),
        ),
        out_specs=(P("task", "tensor"), P("tensor", "task")),
        check_vma=False,
    )
```
